32 devices in a mesh: dom: 8 (over y, x, core), sub: 4 (over z).
Axes of the slice: x: 2, y: 2, z: 4, core: 2. Of those that a mesh axis runs over, the one named last changes fastest.
Arguments:
- displacement: float32 [3, 43200], P(None, ('dom', 'sub')), may hold values from -0.01 to 0.01
- velocity: float32 [3, 43200], P(None, ('dom', 'sub')), may hold values from -3 to 3
- energy: float32 [27, 1536], P(None, ('dom', 'sub')), may hold values from 0.5 to 18, as said below
- mass_density: float32 [125, 1536], P(None, ('dom', 'sub')), may hold values from 0.5 to 4
- live_mask: int32 [1536], P(('dom', 'sub')), may hold values from 0 to 1, as said below
- time_step: float32 [], replicated, may hold values from 0.004 to 0.008
Outputs:
- new_velocity: float32 [3, 43200], P(None, ('dom', 'sub'))
- energy_rate: float32 [27, 1536], P(None, ('dom', 'sub'))
- mesh_velocity: float32 [3, 43200], P(None, ('dom', 'sub'))
The draws below stay inside these ranges and needn't reach their ends.
Inputs may be any that keep to these rules, and one draw needn't show every extreme that they name: `energy`: internal energies are positive. `live_mask`: at most 36 element slots of one device are live, and some device has exactly 36.
All inputs are finite; a program needn't handle non-finite values.
Results may differ from the reference program's by a relative error of at most 0.0003.
Values sent between devices are 32-bit elements; how exact they have to be, the bound alone decides.
A program may use at most 64 MiB of HBM per device.

```python
import math
import jax
import jax.numpy as jnp
import numpy as np
from jax import lax

EX = 1
EY = 8
EZ = 6
QUAD_POINTS = 125
CG_ITERS = 2
RELAX_PASSES = 2
GX = 8
GZ = 24
ELEMS = 1536
NODES = 43200
N_DOM = 8
N_SUB = 4


def draw_energy(key, part):
    devices = N_DOM * N_SUB
    per_device = EX * EY * EZ
    key_base = jax.random.fold_in(key, 11)
    base_values = jnp.exp(jax.random.uniform(key_base, (27, devices, per_device), jnp.float32, math.log(0.5), math.log(2.0)))
    ramp = 1.0 + 2.0 * jnp.arange(devices, dtype=jnp.float32) / max(devices - 1, 1)
    scaled = base_values * ramp[None, :, None]
    return scaled.reshape(27, devices * per_device)


def draw_live_mask(key, part):
    devices = N_DOM * N_SUB
    per_device = EX * EY * EZ
    largest = 3 * per_device // 4
    fewest = max(per_device // 4, 1)
    key_count = jax.random.fold_in(key, 21)
    key_pick = jax.random.fold_in(key, 22)
    key_order = jax.random.fold_in(key, 23)
    counts = jax.random.randint(key_count, (devices,), fewest, largest + 1)
    chosen = jax.random.randint(key_pick, (), 0, devices)
    counts = jnp.where(jnp.arange(devices) == chosen, largest, counts)
    scores = jax.random.randint(key_order, (devices, per_device), 0, 1 << 18)
    scores = scores * per_device + jnp.arange(per_device, dtype=jnp.int32)[None, :]
    ranking = jnp.argsort(jnp.argsort(scores, axis=1, stable=True), axis=1, stable=True)
    live_values = (ranking < counts[:, None]).astype(jnp.int32)
    return live_values.reshape(devices * per_device)


def block_levels(key, dims, split, low, high):
    level = 1.0
    for axis_at, shards_of in split:
        steps = jax.random.uniform(jax.random.fold_in(jax.random.fold_in(key, 6), axis_at), (shards_of,), jnp.float32, low / len(split), high / len(split))
        level = level * jnp.repeat(jnp.exp(steps), dims[axis_at] // shards_of).reshape((-1,) + (1,) * (len(dims) - 1 - axis_at))
    return level


def scatter_about(key, dims, scale, most, cuts=(), kind=jnp.bfloat16):
    gain = block_levels(key, dims, cuts, -0.22, 0.18) if cuts else 1.0
    values = jax.random.normal(key, dims, jnp.float32) * scale * gain
    return jnp.minimum(jnp.maximum(values, -most), most).astype(kind)


def setup_inputs(seed: int = 0) -> dict:
    arg_keys = jax.random.split(jax.random.key(seed), 7)
    return {
        "displacement": jnp.clip(jax.random.uniform(arg_keys[0], (3, NODES), jnp.float32, -0.01, 0.01) * block_levels(arg_keys[0], (3, NODES), ((1, 32),), -0.4, 0.0), -0.01, 0.01),
        "velocity": scatter_about(arg_keys[1], (3, NODES), 0.5, 3.0, ((1, 32),), jnp.float32),
        "energy": draw_energy(jax.random.fold_in(arg_keys[6], 71), 0),
        "mass_density": jnp.clip(jnp.exp(math.log(4.0) - 2.0794415 * jax.random.uniform(arg_keys[3], (QUAD_POINTS, ELEMS), jnp.float32) ** block_levels(arg_keys[3], (QUAD_POINTS, ELEMS), ((1, 32),), -0.2, 0.2)), 0.5, 4.0),
        "live_mask": draw_live_mask(jax.random.fold_in(arg_keys[6], 71), 0),
        "time_step": jnp.clip(jax.random.uniform(arg_keys[5], (), jnp.float32, 0.004, 0.008), 0.004, 0.008),
    }


highest = lax.Precision.HIGHEST
adiabatic = 5.0 / 3.0
viscosity = 0.3
mesh_step = 0.01

def outer_triple(first, second, third):
    product = first[:, None, None, :, None, None] * second[None, :, None, None, :, None] * third[None, None, :, None, None, :]
    return product.reshape(first.shape[0] * second.shape[0] * third.shape[0], first.shape[1] * second.shape[1] * third.shape[1])

def basis_tables():
    root_term = math.sqrt(10.0 / 7.0)
    gauss_roots = np.array([-math.sqrt(5.0 + 2.0 * root_term) / 3.0, -math.sqrt(5.0 - 2.0 * root_term) / 3.0, 0.0, math.sqrt(5.0 - 2.0 * root_term) / 3.0, math.sqrt(5.0 + 2.0 * root_term) / 3.0])
    outer_weight = (322.0 - 13.0 * math.sqrt(70.0)) / 900.0
    middle_weight = (322.0 + 13.0 * math.sqrt(70.0)) / 900.0
    weights = np.array([outer_weight, middle_weight, 128.0 / 225.0, middle_weight, outer_weight]) / 2.0
    points = (1.0 + gauss_roots) / 2.0
    lobatto = [0.0, (1.0 - 1.0 / math.sqrt(5.0)) / 2.0, (1.0 + 1.0 / math.sqrt(5.0)) / 2.0, 1.0]
    values = np.ones((5, 4))
    slopes = np.zeros((5, 4))
    for node_index in range(4):
        for other_index in range(4):
            if other_index != node_index:
                values[:, node_index] *= (points - lobatto[other_index]) / (lobatto[node_index] - lobatto[other_index])
        for other_index in range(4):
            if other_index != node_index:
                factor_term = np.ones(5) / (lobatto[node_index] - lobatto[other_index])
                for third_index in range(4):
                    if third_index != node_index and third_index != other_index:
                        factor_term = factor_term * (points - lobatto[third_index]) / (lobatto[node_index] - lobatto[third_index])
                slopes[:, node_index] += factor_term
    bernstein = np.stack([(1.0 - points) ** 2, 2.0 * points * (1.0 - points), points ** 2], axis=1)
    vel_basis = outer_triple(values, values, values)
    grad_table = np.concatenate([outer_triple(slopes, values, values), outer_triple(values, slopes, values), outer_triple(values, values, slopes)], axis=0)
    energy_basis = outer_triple(bernstein, bernstein, bernstein)
    quad_weight = (weights[:, None, None] * weights[None, :, None] * weights[None, None, :]).reshape(125)
    tables = (jnp.asarray(vel_basis, jnp.float32), jnp.asarray(grad_table, jnp.float32), jnp.asarray(energy_basis, jnp.float32), jnp.asarray(quad_weight, jnp.float32))
    return (tables, lobatto)

def product_dot(left, right):
    return jnp.dot(left, right, precision=highest, preferred_element_type=jnp.float32)

def nodal_gradient(grad_table, nodal_values):
    element_count = nodal_values.shape[1] // 3
    shaped = product_dot(grad_table, nodal_values).reshape(3, 125, 3, element_count)
    return [[shaped[direction, :, component, :] for direction in range(3)] for component in range(3)]

def cofactors(matrix):
    return [[matrix[(row_index + 1) % 3][(col_index + 1) % 3] * matrix[(row_index + 2) % 3][(col_index + 2) % 3] - matrix[(row_index + 1) % 3][(col_index + 2) % 3] * matrix[(row_index + 2) % 3][(col_index + 1) % 3] for col_index in range(3)] for row_index in range(3)]

def project(grad_table, fields):
    element_count = fields[0][0].shape[1]
    stacked = jnp.stack([jnp.stack([fields[component][direction] for component in range(3)], axis=1) for direction in range(3)], axis=0)
    return product_dot(grad_table.T, stacked.reshape(375, 3 * element_count))

def lagrange_rates(coords, speeds, energy, mass_density, live_values, tables):
    vel_basis, grad_table, energy_basis, quad_weight = tables
    jacobian = nodal_gradient(grad_table, coords)
    velocity_grad = nodal_gradient(grad_table, speeds)
    cofactor = cofactors(jacobian)
    volume = jacobian[0][0] * cofactor[0][0] + jacobian[0][1] * cofactor[0][1] + jacobian[0][2] * cofactor[0][2]
    density = mass_density / volume
    pressure = (adiabatic - 1.0) * density * product_dot(energy_basis, energy)
    spatial = [[(velocity_grad[component][0] * cofactor[direction][0] + velocity_grad[component][1] * cofactor[direction][1] + velocity_grad[component][2] * cofactor[direction][2]) / volume for direction in range(3)] for component in range(3)]
    stress = [[viscosity * density * (spatial[component][direction] + spatial[direction][component]) - (pressure if component == direction else 0.0) for direction in range(3)] for component in range(3)]
    weight = quad_weight[:, None] * live_values[None, :]
    flux_terms = [[weight * (stress[component][0] * cofactor[0][direction] + stress[component][1] * cofactor[1][direction] + stress[component][2] * cofactor[2][direction]) for direction in range(3)] for component in range(3)]
    node_force = -project(grad_table, flux_terms)
    power_density = stress[0][0] * spatial[0][0]
    for component in range(3):
        for direction in range(3):
            if component + direction > 0:
                power_density = power_density + stress[component][direction] * spatial[component][direction]
    power_density = weight * volume * power_density
    lumped = product_dot(energy_basis.T, quad_weight[:, None] * mass_density)
    return (node_force, product_dot(energy_basis.T, power_density) / lumped)

def mass_apply(nodal_values, mass_weight, vel_basis):
    element_count = mass_weight.shape[1]
    at_points = product_dot(vel_basis, nodal_values).reshape(125, 3, element_count) * mass_weight[:, None, :]
    return product_dot(vel_basis.T, at_points.reshape(125, 3 * element_count))

def shape_gradient(coords, live_values, tables):
    vel_basis, grad_table, energy_basis, quad_weight = tables
    jacobian = nodal_gradient(grad_table, coords)
    cofactor = cofactors(jacobian)
    volume = jacobian[0][0] * cofactor[0][0] + jacobian[0][1] * cofactor[0][1] + jacobian[0][2] * cofactor[0][2]
    norm_sq = jacobian[0][0] * jacobian[0][0]
    for component in range(3):
        for direction in range(3):
            if component + direction > 0:
                norm_sq = norm_sq + jacobian[component][direction] * jacobian[component][direction]
    ratio_term = norm_sq / volume
    weight = quad_weight[:, None] * live_values[None, :] * volume ** (-2.0 / 3.0)
    fields = [[weight * (2.0 / 3.0 * jacobian[component][direction] - 2.0 / 9.0 * ratio_term * cofactor[component][direction]) for direction in range(3)] for component in range(3)]
    return project(grad_table, fields)

def correlation_take(grid, axis_place):
    rotated = jnp.moveaxis(grid, axis_place, -1)
    block_count = (rotated.shape[-1] - 1) // 3
    main_part = rotated[..., :3 * block_count].reshape(rotated.shape[:-1] + (block_count, 3))
    edge_part = rotated[..., 3::3][..., None]
    return jnp.concatenate([main_part, edge_part], axis=-1)

def correlation_add(pieces):
    block_count = pieces.shape[-2]
    block_width = pieces.shape[-1] - 1
    leading = pieces.shape[:-2]
    main_part = pieces[..., :block_width].reshape(leading + (block_count * block_width,))
    main_part = jnp.pad(main_part, [(0, 0)] * len(leading) + [(0, 1)])
    edge_part = jnp.pad(pieces[..., block_width:], [(0, 0)] * (len(leading) + 1) + [(0, block_width - 1)])
    edge_part = edge_part.reshape(leading + (block_count * block_width,))
    edge_part = jnp.pad(edge_part, [(0, 0)] * len(leading) + [(block_width, 0)])[..., :block_count * block_width + 1]
    return main_part + edge_part

def to_elements(grid):
    pieces = correlation_take(grid, 1)
    pieces = correlation_take(pieces, 1)
    pieces = correlation_take(pieces, 1)
    pieces = pieces.transpose(2, 4, 6, 0, 1, 3, 5)
    return pieces.reshape(64, 3 * EX * EY * EZ)

def to_grid(nodal_values):
    pieces = nodal_values.reshape(4, 4, 4, 3, EX, EY, EZ).transpose(3, 4, 0, 5, 1, 6, 2)
    pieces = correlation_add(pieces)
    pieces = correlation_add(jnp.moveaxis(pieces, (3, 4), (4, 5)))
    pieces = correlation_add(jnp.moveaxis(pieces, (1, 2), (3, 4)))
    return pieces.transpose(0, 3, 2, 1)

def lattice_axis(start_at, extent, lobatto):
    number = start_at + lax.iota(jnp.int32, extent)
    remainder = number % 3
    offset = jnp.where(remainder == 1, lobatto[1], jnp.where(remainder == 2, lobatto[2], 0.0))
    return (number // 3).astype(jnp.float32) + offset

def lattice_grid(start_x, start_z, extent_x, extent_y, extent_z, lobatto):
    along_x = lattice_axis(start_x, extent_x, lobatto)
    along_y = lattice_axis(0, extent_y, lobatto)
    along_z = lattice_axis(start_z, extent_z, lobatto)
    grid_shape = (extent_x, extent_y, extent_z)
    return jnp.stack([jnp.broadcast_to(along_x[:, None, None], grid_shape), jnp.broadcast_to(along_y[None, :, None], grid_shape), jnp.broadcast_to(along_z[None, None, :], grid_shape)])

def full_grid(owned_values):
    channels = owned_values.shape[0]
    blocks = owned_values.reshape(channels, N_DOM, N_SUB, 3 * EX, 3 * EY + 1, 3 * EZ)
    whole = blocks.transpose(0, 1, 3, 4, 2, 5).reshape(channels, 3 * GX, 3 * EY + 1, 3 * GZ)
    return jnp.pad(whole, ((0, 0), (1, 0), (0, 0), (1, 0)))

def device_window(full_values, device):
    dom_place = (device // N_SUB).astype(jnp.int32)
    sub_place = (device % N_SUB).astype(jnp.int32)
    starts = (jnp.int32(0), dom_place * (3 * EX), jnp.int32(0), sub_place * (3 * EZ))
    return lax.dynamic_slice(full_values, starts, (full_values.shape[0], 3 * EX + 1, 3 * EY + 1, 3 * EZ + 1))

def owned_sum(stack):
    channels = stack.shape[1]
    grids = stack.reshape(N_DOM, N_SUB, channels, 3 * EX + 1, 3 * EY + 1, 3 * EZ + 1)
    along_x = correlation_add(grids.transpose(2, 4, 1, 5, 0, 3))
    along_z = correlation_add(along_x.transpose(0, 4, 1, 2, 3))
    interior = along_z[:, 1:, :, 1:]
    blocks = interior.reshape(channels, N_DOM, 3 * EX, 3 * EY + 1, N_SUB, 3 * EZ).transpose(0, 1, 4, 2, 3, 5)
    return blocks.reshape(channels, -1)

def reference(displacement, velocity, energy, mass_density, live_mask, time_step):
    tables, lobatto = basis_tables()
    vel_basis, grad_table, energy_basis, quad_weight = tables
    element_count = EX * EY * EZ
    devices = N_DOM * N_SUB
    device_ids = jnp.arange(devices, dtype=jnp.int32)
    live_values = live_mask.astype(jnp.float32)
    lattice = lattice_grid(0, 0, 3 * GX + 1, 3 * EY + 1, 3 * GZ + 1, lobatto)

    def local_block(element_data, device):
        return lax.dynamic_slice_in_dim(element_data, (device * element_count).astype(jnp.int32), element_count, axis=element_data.ndim - 1)
    full_disp = lattice + full_grid(displacement)
    full_vel = full_grid(velocity)

    def force_block(device):
        coords = to_elements(device_window(full_disp, device))
        speeds = to_elements(device_window(full_vel, device))
        node_force, rate_values = lagrange_rates(coords, speeds, local_block(energy, device), local_block(mass_density, device), local_block(live_values, device), tables)
        return (to_grid(node_force), rate_values)
    forces, rates = lax.map(force_block, device_ids)
    energy_rate = rates.transpose(1, 0, 2).reshape(27, devices * element_count)
    node_force = owned_sum(forces)

    def mass_operator(vector):
        full_values = full_grid(vector)

        def mass_block(device):
            mass_weight = quad_weight[:, None] * local_block(mass_density, device) * local_block(live_values, device)[None, :]
            return to_grid(mass_apply(to_elements(device_window(full_values, device)), mass_weight, vel_basis))
        return owned_sum(lax.map(mass_block, device_ids))
    solution = jnp.zeros_like(node_force)
    residual = node_force
    direction = node_force
    norm_now = jnp.sum(residual * residual)
    for iteration in range(CG_ITERS):
        mass_image = mass_operator(direction)
        step_length = norm_now / jnp.sum(direction * mass_image)
        solution = solution + step_length * direction
        residual = residual - step_length * mass_image
        if iteration + 1 < CG_ITERS:
            norm_next = jnp.sum(residual * residual)
            direction = residual + norm_next / norm_now * direction
            norm_now = norm_next
    new_velocity = velocity + time_step * solution
    moved_disp = displacement + time_step * new_velocity

    def shape_pass(current):
        full_values = lattice + full_grid(current)

        def shape_block(device):
            coords = to_elements(device_window(full_values, device))
            return to_grid(shape_gradient(coords, local_block(live_values, device), tables))
        return owned_sum(lax.map(shape_block, device_ids))
    gradient_sum = jnp.zeros_like(moved_disp)
    for relax_pass in range(RELAX_PASSES):
        gradient = shape_pass(moved_disp)
        gradient_sum = gradient_sum + gradient
        moved_disp = moved_disp - mesh_step * gradient
    mesh_velocity = new_velocity - mesh_step / time_step * gradient_sum
    return (new_velocity, energy_rate, mesh_velocity)
```

```python
import functools
import math

import jax
import jax.numpy as jnp
import numpy as np
from jax import lax
from jax.experimental import pallas as pl
from jax.experimental.pallas import tpu as pltpu
from jax.sharding import PartitionSpec as P

EX = 1
EY = 8
EZ = 6
ELEMS = EX * EY * EZ
HALF = 64

adiabatic = 5.0 / 3.0
viscosity = 0.3
mesh_step = 0.01
MESH = pl.DeviceIdType.MESH
STEPS = [(dx, dz) for dx in (-1, 0, 1) for dz in (-1, 0, 1) if (dx, dz) != (0, 0)]


def one_dimension():
    root_term = math.sqrt(10.0 / 7.0)
    outer_root = math.sqrt(5.0 + 2.0 * root_term) / 3.0
    inner_root = math.sqrt(5.0 - 2.0 * root_term) / 3.0
    gauss_roots = np.array([-outer_root, -inner_root, 0.0, inner_root, outer_root])
    outer_weight = (322.0 - 13.0 * math.sqrt(70.0)) / 900.0
    middle_weight = (322.0 + 13.0 * math.sqrt(70.0)) / 900.0
    weights = (
        np.array([outer_weight, middle_weight, 128.0 / 225.0, middle_weight, outer_weight]) / 2.0
    )
    points = (1.0 + gauss_roots) / 2.0
    lobatto = [0.0, (1.0 - 1.0 / math.sqrt(5.0)) / 2.0, (1.0 + 1.0 / math.sqrt(5.0)) / 2.0, 1.0]
    values = np.ones((5, 4))
    slopes = np.zeros((5, 4))
    for node in range(4):
        for other in range(4):
            if other != node:
                values[:, node] *= (points - lobatto[other]) / (lobatto[node] - lobatto[other])
                term = np.ones(5) / (lobatto[node] - lobatto[other])
                for third in range(4):
                    if third != node and third != other:
                        term = term * (points - lobatto[third]) / (lobatto[node] - lobatto[third])
                slopes[:, node] += term
    bernstein = np.stack([(1.0 - points) ** 2, 2.0 * points * (1.0 - points), points**2], axis=1)
    return values, slopes, bernstein, weights


def outer_triple(first, second, third):
    product = np.einsum("ia,jb,kc->ijkabc", first, second, third)
    return product.reshape(125, -1)


def halves(table, rows):
    padded = np.concatenate([table, np.repeat(table[-1:], 3, axis=0)], axis=0)
    padded = np.pad(padded, [(0, 0), (0, rows - table.shape[1])])
    return np.concatenate([padded[:64], padded[64:]], axis=1)


@functools.lru_cache(None)
def tables():
    values, slopes, bernstein, weights = one_dimension()
    basis = halves(outer_triple(values, values, values), 64)
    grad = np.concatenate(
        [
            halves(outer_triple(slopes, values, values), 64),
            halves(outer_triple(values, slopes, values), 64),
            halves(outer_triple(values, values, slopes), 64),
        ],
        axis=0,
    )
    energy = halves(outer_triple(bernstein, bernstein, bernstein), 32)
    forward = np.concatenate([grad, basis], axis=0)
    backward = np.zeros((128, 384))
    backward[:, :192] = grad.T
    backward[:, 256:320] = basis.T
    energy_pair = np.concatenate([energy, energy.T], axis=1)
    weight = np.einsum("i,j,k->ijk", weights, weights, weights).reshape(125)
    weight = np.pad(weight, (0, 3))
    spread_weight = np.zeros((64, 128))
    spread_weight[:, :ELEMS] = weight[:64, None]
    spread_weight[:, 64 : 64 + ELEMS] = weight[64:, None]
    planes_y, planes_z = 3 * EY + 1, 3 * EZ
    pick = np.zeros((planes_y * planes_z, 16 * HALF), np.float32)
    for b in range(4):
        for c in range(4):
            for q in range(EY):
                for r in range(EZ):
                    z = 3 * r + c - 1
                    if z >= 0:
                        lane = (4 * b + c) * HALF + q * EZ + r
                        pick[(3 * q + b) * planes_z + z, lane] = 1.0
    return [np.asarray(t, np.float32) for t in (forward, backward, energy_pair, spread_weight)] + [
        pick
    ]


def dot(left, right):
    left_high, left_low = split_two(left)
    right_high, right_low = split_two(right)
    product = functools.partial(jnp.dot, preferred_element_type=jnp.float32)
    return (
        product(left_low, right_high) + product(left_high, right_low)
    ) + product(left_high, right_high)


def split_two(value):
    high = value.astype(jnp.bfloat16)
    return high, (value - high.astype(jnp.float32)).astype(jnp.bfloat16)


def cofactors(m):
    return [
        [
            m[(i + 1) % 3][(j + 1) % 3] * m[(i + 2) % 3][(j + 2) % 3]
            - m[(i + 1) % 3][(j + 2) % 3] * m[(i + 2) % 3][(j + 1) % 3]
            for j in range(3)
        ]
        for i in range(3)
    ]


def turn(value, rows, lanes):
    if rows:
        value = pltpu.roll(value, rows % value.shape[0], 0)
    if lanes % value.shape[1]:
        value = pltpu.roll(value, lanes % value.shape[1], 1)
    return value


def split_three(value):
    high = value.astype(jnp.bfloat16).astype(jnp.float32)
    rest = value - high
    middle = rest.astype(jnp.bfloat16).astype(jnp.float32)
    return jnp.concatenate([high, middle, rest - middle], axis=0).astype(jnp.bfloat16)


def kernel(
    n_dom,
    n_sub,
    disp_in_hbm,
    vel_in_hbm,
    energy_in_hbm,
    density_in_hbm,
    live_in_hbm,
    step_in_hbm,
    forward_hbm,
    backward_hbm,
    energy_pair_hbm,
    quad_weight_hbm,
    pick_hbm,
    new_vel_out,
    rate_out,
    mesh_vel_out,
    flat,
    wide,
    first,
    local,
    state,
    out_nodes,
    out_wide,
    density_pad,
    energy_pad,
    live_pad,
    packs,
    x_first,
    x_got,
    z_got,
    d_got,
    sum_dom,
    sum_sub,
    send_sems,
    recv_sems,
    dom_send,
    dom_recv,
    sub_send,
    sub_recv,
    disp_in,
    vel_in,
    energy_in,
    density_in,
    live_in,
    step_in,
    forward,
    backward,
    energy_pair,
    quad_weight,
    pick,
    in_sems,
):
    dom = lax.axis_index("dom")
    sub = lax.axis_index("sub")
    plane = (3 * EY + 1) * 3 * EZ

    def inside(dx, dz):
        ok = None
        for step, place, size in ((dx, dom, n_dom), (dz, sub, n_sub)):
            if step:
                here = (place > 0) if step < 0 else (place < size - 1)
                ok = here if ok is None else jnp.logical_and(ok, here)
        return ok

    held = [
        (disp_in_hbm, disp_in),
        (vel_in_hbm, vel_in),
        (pick_hbm, pick),
        (forward_hbm, forward),
        (backward_hbm, backward),
        (density_in_hbm, density_in),
        (energy_in_hbm, energy_in),
        (live_in_hbm, live_in),
        (energy_pair_hbm, energy_pair),
        (quad_weight_hbm, quad_weight),
        (step_in_hbm, step_in),
    ]
    loads = [
        pltpu.make_async_copy(source, target, in_sems.at[number])
        for number, (source, target) in enumerate(held)
    ]
    for load in loads:
        load.start()

    x_first[...] = jnp.zeros_like(x_first)
    x_got[...] = jnp.zeros_like(x_got)
    z_got[...] = jnp.zeros_like(z_got)
    d_got[...] = jnp.zeros_like(d_got)

    barrier = pltpu.get_barrier_semaphore()
    one_phase = n_dom * n_sub <= 64
    if one_phase:
        devices = n_dom * n_sub
        count = devices - 1

        @pl.loop(1, devices, unroll=True)
        def _(i):
            t = lax.rem(dom * n_sub + sub + i, devices)
            pl.semaphore_signal(
                barrier,
                inc=1,
                device_id=(t // n_sub, lax.rem(t, n_sub)),
                device_id_type=MESH,
            )

    else:
        count = (n_dom - 1) + (n_sub - 1)
        for dx, dz in STEPS:
            if dx and dz:
                ok = inside(dx, dz)
                count = count + ok.astype(jnp.int32)

                @pl.when(ok)
                def _():
                    pl.semaphore_signal(
                        barrier, inc=1, device_id=(dom + dx, sub + dz), device_id_type=MESH
                    )

        @pl.loop(1, n_dom)
        def _(i):
            pl.semaphore_signal(
                barrier, inc=1, device_id=(lax.rem(dom + i, n_dom), sub), device_id_type=MESH
            )

        @pl.loop(1, n_sub)
        def _(i):
            pl.semaphore_signal(
                barrier, inc=1, device_id=(dom, lax.rem(sub + i, n_sub)), device_id_type=MESH
            )

    first[...] = jnp.zeros_like(first)
    density_pad[...] = jnp.zeros_like(density_pad)
    energy_pad[...] = jnp.zeros_like(energy_pad)
    live_pad[...] = jnp.zeros_like(live_pad)
    flat[...] = jnp.zeros_like(flat)
    out_wide[...] = jnp.zeros_like(out_wide)

    lane = lax.broadcasted_iota(jnp.int32, (64, 128), 1)
    row = lax.broadcasted_iota(jnp.int32, (64, 128), 0)
    q_of, r_of = lane // EZ, lane % EZ
    a_of, b_of, c_of = row // 16, (row // 4) % 4, row % 4
    valid = lane < ELEMS
    triple = lambda x: jnp.concatenate([x, x, x], axis=0)
    y_up = triple((b_of == 3) & (q_of < EY - 1) & valid)
    y_down = triple((b_of == 0) & (q_of > 0) & valid)
    z_up = triple((c_of == 3) & (r_of < EZ - 1) & valid)
    z_down = triple((c_of == 0) & (r_of > 0) & valid)
    off_wall = jnp.where(
        valid
        & jnp.logical_or(a_of > 0, dom > 0)
        & jnp.logical_or(jnp.logical_or(c_of > 0, r_of > 0), sub > 0),
        1.0,
        0.0,
    )
    off_wall = triple(off_wall)
    owned = jnp.where(
        valid & (a_of > 0) & (c_of > 0) & ((b_of < 3) | (q_of == EY - 1)), 1.0, 0.0
    )
    owned = triple(owned)
    lane16, row16 = lane[:16], row[:16]
    r16 = jnp.where(lane16 < ELEMS, lane16 % EZ, EZ)

    for load in loads[:3]:
        load.wait()
    flat[0:3, :] = disp_in[...]
    flat[3:6, :] = vel_in[...]
    stacked = jnp.concatenate([flat[:, plane * x : plane * (x + 1)] for x in range(3)], axis=0)
    picked = jnp.dot(split_three(stacked), pick[...], preferred_element_type=jnp.float32)
    wide[...] = picked[0:24] + picked[24:48] + picked[48:72]
    for x in range(3):
        for pair in range(8):
            got = wide[8 * x : 8 * x + 8, 128 * pair : 128 * pair + 128]
            other = turn(got, 0, 64)
            at = 16 * (x + 1) + 2 * pair
            keep = lane[:8] < 64
            first[pl.ds(at, 8, stride=64), :] = jnp.where(keep, got, 0.0)
            first[pl.ds(at + 1, 8, stride=64), :] = jnp.where(keep, other, 0.0)

    pl.semaphore_wait(barrier, count)

    def faces(source, fields, place, shifts):
        packed = jnp.zeros((16, 128), jnp.float32)
        for k in range(fields):
            face = source[pl.ds(64 * k + place, 16, stride=4), :]
            if place == 3:
                packed = jnp.where(r16 == EZ - 1 - k, turn(face, 0, -k), packed)
            else:
                packed = jnp.where(r16 == k, turn(face, 0, k), packed)
        return packed

    waits = []

    def exchange_start(rnd, source, fields, x_target, ups, downs):
        if ups:
            packs[rnd, 1] = faces(source, fields, 3, None)
        if downs:
            packs[rnd, 0] = faces(source, fields, 0, None)
        started = []
        for number, (dx, dz) in enumerate(STEPS):
            lead = dz if dz else dx
            going = (dx, dz)
            up = all(s >= 0 for s in going)
            down = all(s <= 0 for s in going)
            if not ((ups and downs) or (ups and up) or (downs and down)):
                continue
            target = (dom + dx, sub + dz)
            jobs = []
            if dz == 0:
                base = 48 if dx > 0 else 0
                slot = 0 if dx > 0 else 1
                jobs.append(
                    (
                        source_blocks(source, fields, base),
                        x_target(slot),
                    )
                )
            elif dx == 0:
                side = 1 if dz > 0 else 0
                jobs.append((packs.at[rnd, side], z_got.at[rnd, 1 - side]))
            else:
                side = 1 if dz > 0 else 0
                half = 8 if dx > 0 else 0
                slot = (0 if dx > 0 else 1) + 2 * (1 - side)
                jobs.append((packs.at[rnd, side, pl.ds(half, 8)], d_got.at[rnd, slot]))
            src, dst = jobs[0]
            copy = pltpu.make_async_remote_copy(
                src_ref=src,
                dst_ref=dst,
                send_sem=send_sems.at[rnd, number],
                recv_sem=recv_sems.at[rnd, number],
                device_id=target,
                device_id_type=MESH,
            )

            @pl.when(inside(dx, dz))
            def _():
                copy.start()

            started.append((copy, (dx, dz)))
        return started

    def source_blocks(source, fields, base):
        blocks = source.reshape(source.shape[0] // 64, 64, 128)
        return blocks.at[pl.ds(0, fields), pl.ds(base, 16)]

    def exchange_wait(started):
        for copy, (dx, dz) in started:

            @pl.when(inside(-dx, -dz))
            def _():
                copy.wait_recv()

        waits.extend(started)

    def exchange_add(rnd, source, target, fields, x_from, ups, downs):
        if target is not source:
            target[...] = source[...]
        top = lax.broadcasted_iota(jnp.int32, (8, 128), 0) < 4
        for came, side, place in ((ups, 0, 0), (downs, 1, 3)):
            if not came:
                continue
            face = z_got[rnd, side]
            low = jnp.where(top, turn(d_got[rnd, 2 * side], 4, 0), 0.0)
            high = jnp.where(top, 0.0, turn(d_got[rnd, 2 * side + 1], 4, 0))
            face = face + jnp.concatenate([low, high], axis=0)
            for k in range(fields):
                if place == 0:
                    part = jnp.where(r16 == 0, turn(face, 0, k - (EZ - 1)), 0.0)
                else:
                    part = jnp.where(r16 == EZ - 1, turn(face, 0, EZ - 1 - k), 0.0)
                at = pl.ds(64 * k + place, 16, stride=4)
                target[at, :] = target[at, :] + part
        for k in range(fields):
            if ups:
                target[64 * k : 64 * k + 16, :] += x_from(0)[k]
            if downs:
                target[64 * k + 48 : 64 * k + 64, :] += x_from(1)[k]

    started = exchange_start(0, first, 6, lambda slot: x_first, True, False)

    for load in loads[3:]:
        load.wait()
    step = step_in[0, 0]
    density_pad[0:ELEMS, 0:125] = density_in[...]
    energy_pad[0:27, 0:ELEMS] = energy_in[...]
    live_pad[0:1, 0:ELEMS] = live_in[...].astype(jnp.float32)
    live = live_pad[0:1, :]
    live = live + turn(live, 0, 64)
    by_point = jnp.transpose(density_pad[...])
    mass_density = by_point[0:64] + turn(by_point[64:128], 0, 64)
    weight = quad_weight[...]
    live_weight = weight * live
    mass_weight = live_weight * mass_density
    energy_pad_v = energy_pad[...]
    at_points = dot(
        energy_pair[:, 0:64], jnp.concatenate([energy_pad_v, turn(energy_pad_v, 0, 64)], axis=0)
    )

    def paired(v):
        return jnp.concatenate(
            [
                jnp.concatenate([v[64 * k : 64 * k + 64], turn(v[64 * k : 64 * k + 64], 0, 64)], 0)
                for k in range(v.shape[0] // 64)
            ],
            axis=1,
        )

    def folded(product):
        half = product.shape[0] // 2
        out = []
        for k in range(product.shape[1] // 128):
            part = product[:, 128 * k : 128 * k + 128]
            out.append(part[:half] + turn(part[half:], 0, 64))
        return out

    def gradient(v):
        shaped = dot(forward[0:192, :], paired(v))
        return [
            [shaped[64 * m : 64 * m + 64, 128 * c : 128 * c + 128] for m in range(3)]
            for c in range(3)
        ]

    def jacobian_of(v):
        jacobian = gradient(v)
        for c in range(3):
            jacobian[c][c] = jacobian[c][c] + 1.0
        return jacobian

    def project(fields):
        right = jnp.concatenate(
            [jnp.concatenate([fields[c][m] for c in range(3)], axis=1) for m in range(3)], axis=0
        )
        return share(jnp.concatenate(folded(dot(backward[:, 0:192], right)), axis=0))

    def share(v):
        v = v * jnp.where(triple(valid), 1.0, 0.0)
        v = v + jnp.where(y_up, turn(v, 12, -EZ), 0.0) + jnp.where(y_down, turn(v, -12, EZ), 0.0)
        v = v + jnp.where(z_up, turn(v, 3, -1), 0.0) + jnp.where(z_down, turn(v, -3, 1), 0.0)
        return v

    def interpolate(v):
        return dot(forward[192:256, :], paired(v))

    def volume_of(jacobian, cofactor):
        return (
            jacobian[0][0] * cofactor[0][0]
            + jacobian[0][1] * cofactor[0][1]
            + jacobian[0][2] * cofactor[0][2]
        )

    def begin(rnd, v, ups=True, downs=True):
        source = local.at[rnd - 1]
        source[...] = v
        return exchange_start(rnd, source, 3, lambda slot: x_got.at[rnd - 1, slot], ups, downs)

    def finish(rnd, started, ups=True, downs=True):
        exchange_wait(started)
        source = local.at[rnd - 1]
        exchange_add(
            rnd, source, state, 3, lambda slot: x_got.at[rnd - 1, slot], ups, downs
        )
        return state[...] * off_wall

    exchange_wait(started)
    out_nodes[...] = first[0:384, :]
    exchange_add(0, out_nodes, out_nodes, 6, lambda slot: x_first, True, False)
    displacement = out_nodes[0:192, :]
    velocity = out_nodes[192:384, :]

    jacobian = jacobian_of(displacement)
    velocity_grad = gradient(velocity)
    cofactor = cofactors(jacobian)
    volume = volume_of(jacobian, cofactor)
    inverse = 1.0 / volume
    density = mass_density * inverse
    pressure = (adiabatic - 1.0) * density * at_points
    spatial = [
        [
            (
                velocity_grad[c][0] * cofactor[m][0]
                + velocity_grad[c][1] * cofactor[m][1]
                + velocity_grad[c][2] * cofactor[m][2]
            )
            * inverse
            for m in range(3)
        ]
        for c in range(3)
    ]
    viscous = viscosity * density
    stress = [[None] * 3 for _ in range(3)]
    for c in range(3):
        for m in range(c, 3):
            value = viscous * (spatial[c][m] + spatial[m][c])
            stress[c][m] = stress[m][c] = value - pressure if c == m else value
    flux = [
        [
            -live_weight
            * (
                stress[c][0] * cofactor[0][m]
                + stress[c][1] * cofactor[1][m]
                + stress[c][2] * cofactor[2][m]
            )
            for m in range(3)
        ]
        for c in range(3)
    ]
    started = begin(1, project(flux))
    power = stress[0][0] * spatial[0][0]
    for c in range(3):
        for m in range(3):
            if c + m > 0:
                power = power + stress[c][m] * spatial[c][m]
    power = live_weight * volume * power
    sums = folded(
        dot(energy_pair[:, 64:128], jnp.concatenate([power, weight * mass_density], axis=1))
    )
    rate_out[...] = (sums[0] / sums[1])[0:27, 0:ELEMS]
    force = finish(1, started)

    wide_mass = jnp.concatenate([mass_weight] * 3, axis=1)
    values = interpolate(force)
    weighted = wide_mass * values
    image = share(jnp.concatenate(folded(dot(backward[:, 256:320], weighted)), axis=0))
    started = begin(2, image)

    def total(x):
        return jnp.sum(jnp.sum(x, axis=0, keepdims=True), axis=1, keepdims=True)

    norm_part = total(force * force * owned)
    product_part = total(weighted * values)
    image = finish(2, started)
    image_norm_part = total(image * image * owned)
    values = interpolate(image)
    image_product_part = total(wide_mass * values * values)

    lane1 = lane[0:1]
    packed = jnp.where(
        lane1 == 0,
        norm_part,
        jnp.where(
            lane1 == 1,
            product_part,
            jnp.where(lane1 == 2, image_norm_part, image_product_part),
        ),
    )

    late = []

    def all_sum(value, slots, size, place, target, sends, recvs):
        slots[0] = value

        def copy_of(i):
            return pltpu.make_async_remote_copy(
                src_ref=slots.at[0],
                dst_ref=slots.at[i],
                send_sem=sends.at[i],
                recv_sem=recvs.at[i],
                device_id=target(lax.rem(place + i, size)),
                device_id_type=MESH,
            )

        @pl.loop(1, size, unroll=True)
        def _(i):
            copy_of(i).start()

        @pl.loop(1, size, unroll=True)
        def _(i):
            copy_of(i).wait_recv()

        out = jnp.sum(slots[...], axis=0)

        late.append((copy_of, size))
        return out

    if one_phase:
        packed = all_sum(
            packed,
            sum_dom,
            n_dom * n_sub,
            dom * n_sub + sub,
            lambda t: (t // n_sub, lax.rem(t, n_sub)),
            dom_send,
            dom_recv,
        )
    else:
        packed = all_sum(packed, sum_dom, n_dom, dom, lambda t: (t, sub), dom_send, dom_recv)
        packed = all_sum(packed, sum_sub, n_sub, sub, lambda t: (dom, t), sub_send, sub_recv)
    rr, rw, ww, wmw = (
        jnp.sum(jnp.where(lane1 == k, packed, 0.0), axis=1, keepdims=True) for k in range(4)
    )
    first_length = rr / rw
    next_norm = first_length * (first_length * ww) - rr
    conjugacy = next_norm / rr
    residual_image = rw - first_length * ww
    residual_product = rw - 2.0 * first_length * ww + first_length * first_length * wmw
    bend = residual_product + 2.0 * conjugacy * residual_image + conjugacy * conjugacy * rw
    second_length = next_norm / bend
    on_force = first_length + second_length * (1.0 + conjugacy)
    on_image = second_length * first_length
    new_velocity = velocity + step * (on_force * force - on_image * image)
    moved = displacement + step * new_velocity

    def shape(v):
        jacobian = jacobian_of(v)
        cofactor = cofactors(jacobian)
        volume = volume_of(jacobian, cofactor)
        norm_sq = None
        for c in range(3):
            for m in range(3):
                square = jacobian[c][m] * jacobian[c][m]
                norm_sq = square if norm_sq is None else norm_sq + square
        scale = live_weight * jnp.exp(jnp.log(volume) * (-2.0 / 3.0))
        along = scale * (2.0 / 3.0)
        across = scale * (2.0 / 9.0) * (norm_sq / volume)
        return project(
            [
                [along * jacobian[c][m] - across * cofactor[c][m] for m in range(3)]
                for c in range(3)
            ]
        )

    started = begin(3, shape(moved))
    slope = finish(3, started)
    started = begin(4, shape(moved - mesh_step * slope), False, True)
    last = finish(4, started, False, True)
    mesh_velocity = new_velocity - (mesh_step / step) * (slope + last)

    out_nodes[0:192, :] = new_velocity * owned
    out_nodes[192:384, :] = mesh_velocity * owned
    for x in range(3):
        for pair in range(8):
            at = 16 * (x + 1) + 2 * pair
            even = out_nodes[pl.ds(at, 6, stride=64), :]
            odd = out_nodes[pl.ds(at + 1, 6, stride=64), :]
            out_wide[8 * x : 8 * x + 6, 128 * pair : 128 * pair + 128] = even + turn(odd, 0, 64)
    back = lax.dot_general(
        split_three(out_wide[...]),
        pick[...],
        (((1,), (1,)), ((), ())),
        preferred_element_type=jnp.float32,
    )
    back = back[0:24] + back[24:48] + back[48:72]
    for x in range(3):
        new_vel_out[:, plane * x : plane * (x + 1)] = back[8 * x : 8 * x + 3]
        mesh_vel_out[:, plane * x : plane * (x + 1)] = back[8 * x + 3 : 8 * x + 6]

    for copy_of, size in late:

        @pl.loop(1, size, unroll=True)
        def _(i, copy_of=copy_of):
            copy_of(i).wait_send()

    for copy, (dx, dz) in waits:

        @pl.when(inside(dx, dz))
        def _():
            copy.wait_send()


def hand_on(*refs):
    copies = [
        pltpu.make_async_copy(refs[k], refs[3 + k], refs[6].at[k]) for k in range(3)
    ]
    for copy in copies:
        copy.start()
    for copy in copies:
        copy.wait()


def body(n_dom, n_sub, displacement, velocity, energy, mass_density, live_mask, time_step):
    forward, backward, energy_pair, quad_weight, pick = tables()
    vmem = pl.BlockSpec(memory_space=pltpu.VMEM)
    anywhere = pl.BlockSpec(memory_space=pl.ANY)
    f32 = jnp.float32
    nodes = displacement.shape[1]
    wide_sum = n_dom * n_sub if n_dom * n_sub <= 64 else n_dom
    made = pl.pallas_call(
        functools.partial(kernel, n_dom, n_sub),
        out_shape=(
            pltpu.VMEM(displacement.shape, f32),
            pltpu.VMEM(energy.shape, f32),
            pltpu.VMEM(displacement.shape, f32),
        ),
        in_specs=[anywhere] * 11,
        out_specs=(vmem, vmem, vmem),
        scratch_shapes=[
            pltpu.VMEM((8, nodes), f32),
            pltpu.VMEM((24, 1024), f32),
            pltpu.VMEM((512, 128), f32),
            pltpu.VMEM((4, 192, 128), f32),
            pltpu.VMEM((192, 128), f32),
            pltpu.VMEM((384, 128), f32),
            pltpu.VMEM((24, 1024), f32),
            pltpu.VMEM((128, 128), f32),
            pltpu.VMEM((32, 128), f32),
            pltpu.VMEM((8, 128), f32),
            pltpu.VMEM((5, 2, 16, 128), f32),
            pltpu.VMEM((6, 16, 128), f32),
            pltpu.VMEM((4, 2, 3, 16, 128), f32),
            pltpu.VMEM((5, 2, 16, 128), f32),
            pltpu.VMEM((5, 4, 8, 128), f32),
            pltpu.VMEM((wide_sum, 1, 128), f32),
            pltpu.VMEM((n_sub, 1, 128), f32),
            pltpu.SemaphoreType.DMA((5, 8)),
            pltpu.SemaphoreType.DMA((5, 8)),
            pltpu.SemaphoreType.DMA((wide_sum,)),
            pltpu.SemaphoreType.DMA((wide_sum,)),
            pltpu.SemaphoreType.DMA((n_sub,)),
            pltpu.SemaphoreType.DMA((n_sub,)),
            pltpu.VMEM(displacement.shape, f32),
            pltpu.VMEM(velocity.shape, f32),
            pltpu.VMEM(energy.shape, f32),
            pltpu.VMEM(mass_density.shape[::-1], f32),
            pltpu.VMEM((1, live_mask.shape[0]), jnp.int32),
            pltpu.SMEM((1, 1), f32),
            pltpu.VMEM(forward.shape, f32),
            pltpu.VMEM(backward.shape, f32),
            pltpu.VMEM(energy_pair.shape, f32),
            pltpu.VMEM(quad_weight.shape, f32),
            pltpu.VMEM(pick.shape, jnp.bfloat16),
            pltpu.SemaphoreType.DMA((11,)),
        ],
        compiler_params=pltpu.CompilerParams(collective_id=0, has_side_effects=True),
    )(
        displacement,
        velocity,
        energy,
        mass_density.T,
        live_mask.reshape(1, -1),
        time_step.reshape(1, 1),
        forward,
        backward,
        energy_pair,
        quad_weight,
        jnp.asarray(pick, jnp.bfloat16),
    )
    return pl.pallas_call(
        hand_on,
        out_shape=[jax.ShapeDtypeStruct(m.shape, f32) for m in made],
        in_specs=[vmem] * 3,
        out_specs=[anywhere] * 3,
        scratch_shapes=[pltpu.SemaphoreType.DMA((3,))],
    )(*[pltpu.with_memory_space_constraint(m, pltpu.VMEM) for m in made])


def solution(mesh):
    split = ("dom", "sub")
    return jax.shard_map(
        functools.partial(body, mesh.shape["dom"], mesh.shape["sub"]),
        mesh=mesh,
        in_specs=(
            P(None, split),
            P(None, split),
            P(None, split),
            P(None, split),
            P(split),
            P(),
        ),
        out_specs=(P(None, split), P(None, split), P(None, split)),
        check_vma=False,
    )
```

```python
import functools
import math

import jax
import jax.numpy as jnp
import numpy as np
from jax import lax
from jax.experimental import pallas as pl
from jax.experimental.pallas import tpu as pltpu
from jax.sharding import PartitionSpec as P

EX = 1
EY = 8
EZ = 6
ELEMS = EX * EY * EZ
HALF = 64
ROW = 8

adiabatic = 5.0 / 3.0
viscosity = 0.3
mesh_step = 0.01
MESH = pl.DeviceIdType.MESH
STEPS = [(dx, dz) for dx in (-1, 0, 1) for dz in (-1, 0, 1) if (dx, dz) != (0, 0)]
WIDE_STEPS = [(dx, dz) for dx in (-2, -1, 0, 1) for dz in (-1, 0, 1) if (dx, dz) != (0, 0)]


def one_dimension():
    root_term = math.sqrt(10.0 / 7.0)
    outer_root = math.sqrt(5.0 + 2.0 * root_term) / 3.0
    inner_root = math.sqrt(5.0 - 2.0 * root_term) / 3.0
    gauss_roots = np.array([-outer_root, -inner_root, 0.0, inner_root, outer_root])
    outer_weight = (322.0 - 13.0 * math.sqrt(70.0)) / 900.0
    middle_weight = (322.0 + 13.0 * math.sqrt(70.0)) / 900.0
    weights = (
        np.array([outer_weight, middle_weight, 128.0 / 225.0, middle_weight, outer_weight]) / 2.0
    )
    points = (1.0 + gauss_roots) / 2.0
    lobatto = [0.0, (1.0 - 1.0 / math.sqrt(5.0)) / 2.0, (1.0 + 1.0 / math.sqrt(5.0)) / 2.0, 1.0]
    values = np.ones((5, 4))
    slopes = np.zeros((5, 4))
    for node in range(4):
        for other in range(4):
            if other != node:
                values[:, node] *= (points - lobatto[other]) / (lobatto[node] - lobatto[other])
                term = np.ones(5) / (lobatto[node] - lobatto[other])
                for third in range(4):
                    if third != node and third != other:
                        term = term * (points - lobatto[third]) / (lobatto[node] - lobatto[third])
                slopes[:, node] += term
    bernstein = np.stack([(1.0 - points) ** 2, 2.0 * points * (1.0 - points), points**2], axis=1)
    return values, slopes, bernstein, weights


def outer_triple(first, second, third):
    product = np.einsum("ia,jb,kc->ijkabc", first, second, third)
    return product.reshape(125, -1)


def halves(table, rows):
    padded = np.concatenate([table, np.repeat(table[-1:], 3, axis=0)], axis=0)
    padded = np.pad(padded, [(0, 0), (0, rows - table.shape[1])])
    return np.concatenate([padded[:64], padded[64:]], axis=1)


def stacked_left(table):
    table = np.asarray(table, np.float32)
    high = table.astype(jnp.bfloat16)
    low = (table - high.astype(np.float32)).astype(jnp.bfloat16)
    return np.concatenate([low, high, high], axis=1)


@functools.lru_cache(None)
def tables():
    values, slopes, bernstein, weights = one_dimension()
    triples = [
        outer_triple(slopes, values, values),
        outer_triple(values, slopes, values),
        outer_triple(values, values, slopes),
    ]
    grad = np.concatenate([halves(t, 64) for t in triples], axis=0)
    whole = [np.concatenate([t, np.repeat(t[-1:], 3, axis=0)], axis=0) for t in triples]
    basis = halves(outer_triple(values, values, values), 64)
    energy = halves(outer_triple(bernstein, bernstein, bernstein), 32)
    weight = np.einsum("i,j,k->ijk", weights, weights, weights).reshape(125)
    weight = np.pad(weight, (0, 3))
    spread_weight = np.zeros((64, 128))
    spread_weight[:, :64] = weight[:64, None]
    spread_weight[:, 64:] = weight[64:, None]
    whole_weight = np.repeat(weight[:, None], 128, axis=1)
    planes_y, planes_z = 3 * EY + 1, 3 * EZ
    pick = np.zeros((planes_y * planes_z, 16 * HALF), np.float32)
    for b in range(4):
        for c in range(4):
            for q in range(EY):
                for r in range(EZ):
                    z = 3 * r + c - 1
                    if z >= 0:
                        lane = (4 * b + c) * HALF + q * ROW + r
                        pick[(3 * q + b) * planes_z + z, lane] = 1.0
    widen = np.zeros((128, 256), np.float32)
    for e in range(ELEMS):
        to = e // EZ * ROW + e % EZ
        widen[e, to] = 1.0
        widen[to, 128 + e] = 1.0
    return [
        pick.astype(jnp.bfloat16),
        stacked_left(grad),
        stacked_left(grad.T),
        stacked_left(basis),
        stacked_left(basis.T),
        stacked_left(energy),
        stacked_left(energy.T),
        stacked_left(np.concatenate(whole, axis=0)),
        stacked_left(np.concatenate(whole, axis=0).T),
        widen.astype(jnp.bfloat16),
        np.asarray(spread_weight, np.float32),
        np.asarray(whole_weight, np.float32),
    ]


def dot(table, right):
    high, low = split_two(right)
    stacked = jnp.concatenate([high, low, high], axis=0)
    return jnp.dot(table[...], stacked, preferred_element_type=jnp.float32)


def split_two(value):
    high = value.astype(jnp.bfloat16)
    return high, (value - high.astype(jnp.float32)).astype(jnp.bfloat16)


def cofactors(m):
    return [
        [
            m[(i + 1) % 3][(j + 1) % 3] * m[(i + 2) % 3][(j + 2) % 3]
            - m[(i + 1) % 3][(j + 2) % 3] * m[(i + 2) % 3][(j + 1) % 3]
            for j in range(3)
        ]
        for i in range(3)
    ]


def turn(value, rows, lanes):
    if rows:
        value = pltpu.roll(value, rows % value.shape[0], 0)
    if lanes % value.shape[1]:
        value = pltpu.roll(value, lanes % value.shape[1], 1)
    return value


def split_three(value):
    high = value.astype(jnp.bfloat16).astype(jnp.float32)
    rest = value - high
    middle = rest.astype(jnp.bfloat16).astype(jnp.float32)
    return jnp.concatenate([high, middle, rest - middle], axis=0).astype(jnp.bfloat16)


def kernel(
    n_dom,
    n_sub,
    disp_in_hbm,
    vel_in_hbm,
    energy_in_hbm,
    density_in_hbm,
    live_in_hbm,
    step_in_hbm,
    pick_hbm,
    grad_forth_hbm,
    grad_back_hbm,
    basis_forth_hbm,
    basis_back_hbm,
    energy_forth_hbm,
    energy_back_hbm,
    whole_forth_hbm,
    whole_back_hbm,
    widen_hbm,
    quad_weight_hbm,
    whole_weight_hbm,
    new_vel_out,
    rate_out,
    mesh_vel_out,
    flat,
    wide,
    first,
    local,
    state,
    out_nodes,
    out_wide,
    density_pad,
    energy_pad,
    live_own,
    live_got,
    packs,
    x_first,
    x_got,
    z_got,
    d_got,
    sum_dom,
    sum_sub,
    send_sems,
    recv_sems,
    dom_send,
    dom_recv,
    sub_send,
    sub_recv,
    disp_in,
    vel_in,
    energy_in,
    density_in,
    live_in,
    step_in,
    pick,
    grad_forth,
    grad_back,
    basis_forth,
    basis_back,
    energy_forth,
    energy_back,
    whole_forth,
    whole_back,
    widen,
    quad_weight,
    whole_weight,
    in_sems,
    ours,
    near,
    z_low,
    z_high,
    slab_got,
    x_face_got,
    layer_got,
    edge_got,
    floor_got,
    wide_nodes,
    wide_send,
    wide_recv,
    live_send,
    live_recv,
):
    dom = lax.axis_index("dom")
    sub = lax.axis_index("sub")
    plane = (3 * EY + 1) * 3 * EZ

    def inside(dx, dz):
        ok = None
        for step, place, size in ((dx, dom, n_dom), (dz, sub, n_sub)):
            if step:
                here = (place + step >= 0) if step < 0 else (place + step < size)
                ok = here if ok is None else jnp.logical_and(ok, here)
        return ok

    held = [
        (disp_in_hbm, disp_in),
        (vel_in_hbm, vel_in),
        (pick_hbm, pick),
        (step_in_hbm, step_in),
        (density_in_hbm, density_in),
        (energy_in_hbm, energy_in),
        (live_in_hbm, live_in),
        (grad_forth_hbm, grad_forth),
        (grad_back_hbm, grad_back),
        (basis_forth_hbm, basis_forth),
        (basis_back_hbm, basis_back),
        (energy_forth_hbm, energy_forth),
        (energy_back_hbm, energy_back),
        (whole_forth_hbm, whole_forth),
        (whole_back_hbm, whole_back),
        (widen_hbm, widen),
        (quad_weight_hbm, quad_weight),
        (whole_weight_hbm, whole_weight),
    ]
    loads = [
        pltpu.make_async_copy(source, target, in_sems.at[number])
        for number, (source, target) in enumerate(held)
    ]
    for load in loads:
        load.start()

    x_first[...] = jnp.zeros_like(x_first)
    x_got[...] = jnp.zeros_like(x_got)
    z_got[...] = jnp.zeros_like(z_got)
    d_got[...] = jnp.zeros_like(d_got)
    for got in (slab_got, x_face_got, layer_got, edge_got, floor_got, live_got):
        got[...] = jnp.zeros_like(got)

    barrier = pltpu.get_barrier_semaphore()
    one_phase = n_dom * n_sub <= 64
    if one_phase:
        devices = n_dom * n_sub
        count = devices - 1

        @pl.loop(1, devices, unroll=True)
        def _(i):
            t = lax.rem(dom * n_sub + sub + i, devices)
            pl.semaphore_signal(
                barrier,
                inc=1,
                device_id=(t // n_sub, lax.rem(t, n_sub)),
                device_id_type=MESH,
            )

    else:
        count = (n_dom - 1) + (n_sub - 1)
        for dx, dz in [(dx, dz) for dx in (-2, -1, 1, 2) for dz in (-1, 1)]:
            if dx and dz:
                ok = inside(dx, dz)
                count = count + ok.astype(jnp.int32)

                @pl.when(ok)
                def _():
                    pl.semaphore_signal(
                        barrier, inc=1, device_id=(dom + dx, sub + dz), device_id_type=MESH
                    )

        @pl.loop(1, n_dom)
        def _(i):
            pl.semaphore_signal(
                barrier, inc=1, device_id=(lax.rem(dom + i, n_dom), sub), device_id_type=MESH
            )

        @pl.loop(1, n_sub)
        def _(i):
            pl.semaphore_signal(
                barrier, inc=1, device_id=(dom, lax.rem(sub + i, n_sub)), device_id_type=MESH
            )

    first[...] = jnp.zeros_like(first)
    density_pad[...] = jnp.zeros_like(density_pad)
    energy_pad[...] = jnp.zeros_like(energy_pad)
    flat[...] = jnp.zeros_like(flat)
    out_wide[...] = jnp.zeros_like(out_wide)

    lane = lax.broadcasted_iota(jnp.int32, (64, 128), 1)
    row = lax.broadcasted_iota(jnp.int32, (64, 128), 0)
    q_of, r_of = (lane % HALF) // ROW, lane % ROW
    a_of, b_of, c_of = row // 16, (row // 4) % 4, row % 4
    low_half = lane < HALF
    valid = low_half & (r_of < EZ)
    triple = lambda x: jnp.concatenate([x, x, x], axis=0)
    y_up = triple((b_of == 3) & (q_of < EY - 1) & valid)
    y_down = triple((b_of == 0) & (q_of > 0) & valid)
    z_up = triple((c_of == 3) & (r_of < EZ - 1) & valid)
    z_down = triple((c_of == 0) & (r_of > 0) & valid)
    off_wall = jnp.where(
        valid
        & jnp.logical_or(a_of > 0, dom > 0)
        & jnp.logical_or(jnp.logical_or(c_of > 0, r_of > 0), sub > 0),
        1.0,
        0.0,
    )
    off_wall = triple(off_wall)
    owned = jnp.where(
        valid & (a_of > 0) & (c_of > 0) & ((b_of < 3) | (q_of == EY - 1)), 1.0, 0.0
    )
    owned = triple(owned)
    lane16, row16 = lane[:16], row[:16]
    r16 = jnp.where(lane16 < HALF, lane16 % ROW, ROW)

    for load in loads[:3]:
        load.wait()
    flat[0:3, :] = disp_in[...]
    flat[3:6, :] = vel_in[...]
    stacked = jnp.concatenate([flat[:, plane * x : plane * (x + 1)] for x in range(3)], axis=0)
    picked = jnp.dot(split_three(stacked), pick[...], preferred_element_type=jnp.float32)
    wide[...] = picked[0:24] + picked[24:48] + picked[48:72]
    for x in range(3):
        for pair in range(8):
            got = wide[8 * x : 8 * x + 8, 128 * pair : 128 * pair + 128]
            other = turn(got, 0, 64)
            at = 16 * (x + 1) + 2 * pair
            keep = lane[:8] < 64
            first[pl.ds(at, 8, stride=64), :] = jnp.where(keep, got, 0.0)
            first[pl.ds(at + 1, 8, stride=64), :] = jnp.where(keep, other, 0.0)

    pl.semaphore_wait(barrier, count)

    def faces(source, fields, place, shifts):
        packed = jnp.zeros((16, 128), jnp.float32)
        for k in range(fields):
            face = source[pl.ds(64 * k + place, 16, stride=4), :]
            if place == 3:
                packed = jnp.where(r16 == EZ - 1 - k, turn(face, 0, -k), packed)
            else:
                packed = jnp.where(r16 == k, turn(face, 0, k), packed)
        return packed

    waits = []

    def exchange_start(rnd, source, fields, x_target, ups, downs):
        if ups:
            packs[rnd, 1] = faces(source, fields, 3, None)
        if downs:
            packs[rnd, 0] = faces(source, fields, 0, None)
        started = []
        for number, (dx, dz) in enumerate(STEPS):
            lead = dz if dz else dx
            going = (dx, dz)
            up = all(s >= 0 for s in going)
            down = all(s <= 0 for s in going)
            if not ((ups and downs) or (ups and up) or (downs and down)):
                continue
            target = (dom + dx, sub + dz)
            jobs = []
            if dz == 0:
                base = 48 if dx > 0 else 0
                slot = 0 if dx > 0 else 1
                jobs.append(
                    (
                        source_blocks(source, fields, base),
                        x_target(slot),
                    )
                )
            elif dx == 0:
                side = 1 if dz > 0 else 0
                jobs.append((packs.at[rnd, side], z_got.at[rnd, 1 - side]))
            else:
                side = 1 if dz > 0 else 0
                half = 8 if dx > 0 else 0
                slot = (0 if dx > 0 else 1) + 2 * (1 - side)
                jobs.append((packs.at[rnd, side, pl.ds(half, 8)], d_got.at[rnd, slot]))
            src, dst = jobs[0]
            copy = pltpu.make_async_remote_copy(
                src_ref=src,
                dst_ref=dst,
                send_sem=send_sems.at[rnd, number],
                recv_sem=recv_sems.at[rnd, number],
                device_id=target,
                device_id_type=MESH,
            )

            @pl.when(inside(dx, dz))
            def _():
                copy.start()

            started.append((copy, (dx, dz)))
        return started

    def source_blocks(source, fields, base):
        blocks = source.reshape(source.shape[0] // 64, 64, 128)
        return blocks.at[pl.ds(0, fields), pl.ds(base, 16)]

    def exchange_wait(started):
        for copy, (dx, dz) in started:

            @pl.when(inside(-dx, -dz))
            def _():
                copy.wait_recv()

        waits.extend(started)

    def exchange_add(rnd, source, target, fields, x_from, ups, downs):
        if target is not source:
            target[...] = source[...]
        top = lax.broadcasted_iota(jnp.int32, (8, 128), 0) < 4
        for came, side, place in ((ups, 0, 0), (downs, 1, 3)):
            if not came:
                continue
            face = z_got[rnd, side]
            low = jnp.where(top, turn(d_got[rnd, 2 * side], 4, 0), 0.0)
            high = jnp.where(top, 0.0, turn(d_got[rnd, 2 * side + 1], 4, 0))
            face = face + jnp.concatenate([low, high], axis=0)
            for k in range(fields):
                if place == 0:
                    part = jnp.where(r16 == 0, turn(face, 0, k - (EZ - 1)), 0.0)
                else:
                    part = jnp.where(r16 == EZ - 1, turn(face, 0, EZ - 1 - k), 0.0)
                at = pl.ds(64 * k + place, 16, stride=4)
                target[at, :] = target[at, :] + part
        for k in range(fields):
            if ups:
                target[64 * k : 64 * k + 16, :] += x_from(0)[k]
            if downs:
                target[64 * k + 48 : 64 * k + 64, :] += x_from(1)[k]

    started = exchange_start(0, first, 6, lambda slot: x_first, True, False)

    for load in loads[3:]:
        load.wait()
    step = step_in[0, 0]
    for q in range(EY):
        density_pad[ROW * q : ROW * q + EZ, 0:125] = density_in[EZ * q : EZ * q + EZ, :]
    energy_pad[0:27, 0:ELEMS] = energy_in[...]
    energy_pad[27:28, 0:ELEMS] = live_in[...].astype(jnp.float32)

    def exact(value, table):
        rows = value.shape[0]
        out = jnp.dot(split_three(value), table, preferred_element_type=jnp.float32)
        return out[0:rows] + out[rows : 2 * rows] + out[2 * rows :]

    by_lane = exact(energy_pad[...], widen[:, 0:128])
    live = by_lane[27:28, :]
    live_own[...] = jnp.broadcast_to(live, (8, 128))
    live_copies = []
    for number, (dx, dz) in enumerate(((-1, 0), (0, -1), (-1, -1))):
        live_copy = pltpu.make_async_remote_copy(
            src_ref=live_own,
            dst_ref=live_got.at[number],
            send_sem=live_send.at[number],
            recv_sem=live_recv.at[number],
            device_id=(dom + dx, sub + dz),
            device_id_type=MESH,
        )
        live_copies.append((live_copy, (dx, dz)))

        @pl.when(inside(dx, dz))
        def _():
            live_copy.start()

    live = live + turn(live, 0, 64)
    by_point = jnp.transpose(density_pad[...])
    mass_density = by_point[0:64] + turn(by_point[64:128], 0, 64)
    weight = quad_weight[...]
    live_weight = weight * live
    mass_weight = live_weight * mass_density
    at_points = dot(energy_forth, jnp.concatenate([by_lane, turn(by_lane, 0, 64)], axis=0))

    def paired(v):
        return jnp.concatenate(
            [
                jnp.concatenate([v[64 * k : 64 * k + 64], turn(v[64 * k : 64 * k + 64], 0, 64)], 0)
                for k in range(v.shape[0] // 64)
            ],
            axis=1,
        )

    def folded(product):
        half = product.shape[0] // 2
        out = []
        for k in range(product.shape[1] // 128):
            part = product[:, 128 * k : 128 * k + 128]
            out.append(part[:half] + turn(part[half:], 0, 64))
        return out

    def gradient(v):
        shaped = dot(grad_forth, paired(v))
        return [
            [shaped[64 * m : 64 * m + 64, 128 * c : 128 * c + 128] for m in range(3)]
            for c in range(3)
        ]

    def jacobian_of(v):
        jacobian = gradient(v)
        for c in range(3):
            jacobian[c][c] = jacobian[c][c] + 1.0
        return jacobian

    def project(fields):
        right = jnp.concatenate(
            [jnp.concatenate([fields[c][m] for c in range(3)], axis=1) for m in range(3)], axis=0
        )
        return share(jnp.concatenate(folded(dot(grad_back, right)), axis=0))

    def share(v):
        v = v * jnp.where(triple(valid), 1.0, 0.0)
        v = v + jnp.where(y_up, turn(v, 12, -ROW), 0.0) + jnp.where(y_down, turn(v, -12, ROW), 0.0)
        v = v + jnp.where(z_up, turn(v, 3, -1), 0.0) + jnp.where(z_down, turn(v, -3, 1), 0.0)
        return v

    def interpolate(v):
        return dot(basis_forth, paired(v))

    def volume_of(jacobian, cofactor):
        return (
            jacobian[0][0] * cofactor[0][0]
            + jacobian[0][1] * cofactor[0][1]
            + jacobian[0][2] * cofactor[0][2]
        )

    def begin(rnd, v, ups=True, downs=True):
        source = local.at[rnd - 1]
        source[...] = v
        return exchange_start(rnd, source, 3, lambda slot: x_got.at[rnd - 1, slot], ups, downs)

    def finish(rnd, started, ups=True, downs=True):
        exchange_wait(started)
        source = local.at[rnd - 1]
        exchange_add(
            rnd, source, state, 3, lambda slot: x_got.at[rnd - 1, slot], ups, downs
        )
        return state[...] * off_wall

    exchange_wait(started)
    out_nodes[...] = first[0:384, :]
    exchange_add(0, out_nodes, out_nodes, 6, lambda slot: x_first, True, False)
    displacement = out_nodes[0:192, :]
    velocity = out_nodes[192:384, :]

    jacobian = jacobian_of(displacement)
    velocity_grad = gradient(velocity)
    cofactor = cofactors(jacobian)
    volume = volume_of(jacobian, cofactor)
    inverse = 1.0 / volume
    density = mass_density * inverse
    pressure = (adiabatic - 1.0) * density * at_points
    spatial = [
        [
            (
                velocity_grad[c][0] * cofactor[m][0]
                + velocity_grad[c][1] * cofactor[m][1]
                + velocity_grad[c][2] * cofactor[m][2]
            )
            * inverse
            for m in range(3)
        ]
        for c in range(3)
    ]
    viscous = viscosity * density
    stress = [[None] * 3 for _ in range(3)]
    for c in range(3):
        for m in range(c, 3):
            value = viscous * (spatial[c][m] + spatial[m][c])
            stress[c][m] = stress[m][c] = value - pressure if c == m else value
    flux = [
        [
            -live_weight
            * (
                stress[c][0] * cofactor[0][m]
                + stress[c][1] * cofactor[1][m]
                + stress[c][2] * cofactor[2][m]
            )
            for m in range(3)
        ]
        for c in range(3)
    ]
    started = begin(1, project(flux))
    power = stress[0][0] * spatial[0][0]
    for c in range(3):
        for m in range(3):
            if c + m > 0:
                power = power + stress[c][m] * spatial[c][m]
    power = live_weight * volume * power
    sums = folded(
        dot(energy_back, jnp.concatenate([power, weight * mass_density], axis=1))
    )
    rates = jnp.where(valid[:32], sums[0] / jnp.where(valid[:32], sums[1], 1.0), 0.0)
    rate_out[...] = exact(rates, widen[:, 128:256])[0:27, 0:ELEMS]
    force = finish(1, started)

    wide_mass = jnp.concatenate([mass_weight] * 3, axis=1)
    values = interpolate(force)
    weighted = wide_mass * values
    image = share(jnp.concatenate(folded(dot(basis_back, weighted)), axis=0))
    started = begin(2, image)

    def total(x):
        return jnp.sum(jnp.sum(x, axis=0, keepdims=True), axis=1, keepdims=True)

    norm_part = total(force * force * owned)
    product_part = total(weighted * values)
    image = finish(2, started)
    image_norm_part = total(image * image * owned)
    values = interpolate(image)
    image_product_part = total(wide_mass * values * values)

    lane1 = lane[0:1]
    packed = jnp.where(
        lane1 == 0,
        norm_part,
        jnp.where(
            lane1 == 1,
            product_part,
            jnp.where(lane1 == 2, image_norm_part, image_product_part),
        ),
    )

    late = []

    def all_sum(value, slots, size, place, target, sends, recvs, cover=None):
        slots[0] = value

        def copy_of(i):
            return pltpu.make_async_remote_copy(
                src_ref=slots.at[0],
                dst_ref=slots.at[i],
                send_sem=sends.at[i],
                recv_sem=recvs.at[i],
                device_id=target(lax.rem(place + i, size)),
                device_id_type=MESH,
            )

        @pl.loop(1, size, unroll=True)
        def _(i):
            copy_of(i).start()

        out = cover() if cover else None

        @pl.loop(1, size, unroll=True)
        def _(i):
            copy_of(i).wait_recv()

        late.append((copy_of, size))
        return jnp.sum(slots[...], axis=0), out

    def ahead():
        return [gradient(v) for v in (displacement + step * velocity, force, image)]

    if one_phase:
        packed, slopes = all_sum(
            packed,
            sum_dom,
            n_dom * n_sub,
            dom * n_sub + sub,
            lambda t: (t // n_sub, lax.rem(t, n_sub)),
            dom_send,
            dom_recv,
            ahead,
        )
    else:
        packed, slopes = all_sum(
            packed, sum_dom, n_dom, dom, lambda t: (t, sub), dom_send, dom_recv, ahead
        )
        packed, _ = all_sum(packed, sum_sub, n_sub, sub, lambda t: (dom, t), sub_send, sub_recv)
    rr, rw, ww, wmw = (
        jnp.sum(jnp.where(lane1 == k, packed, 0.0), axis=1, keepdims=True) for k in range(4)
    )
    first_length = rr / rw
    next_norm = first_length * (first_length * ww) - rr
    conjugacy = next_norm / rr
    residual_image = rw - first_length * ww
    residual_product = rw - 2.0 * first_length * ww + first_length * first_length * wmw
    bend = residual_product + 2.0 * conjugacy * residual_image + conjugacy * conjugacy * rw
    second_length = next_norm / bend
    on_force = first_length + second_length * (1.0 + conjugacy)
    on_image = second_length * first_length
    new_velocity = velocity + step * (on_force * force - on_image * image)
    moved = displacement + step * new_velocity

    def fluxes(jacobian, weights):
        cofactor = cofactors(jacobian)
        volume = volume_of(jacobian, cofactor)
        norm_sq = None
        for c in range(3):
            for m in range(3):
                square = jacobian[c][m] * jacobian[c][m]
                norm_sq = square if norm_sq is None else norm_sq + square
        scale = weights * jnp.exp(jnp.log(volume) * (-2.0 / 3.0))
        along = scale * (2.0 / 3.0)
        across = scale * (2.0 / 9.0) * (norm_sq / volume)
        return [
            [along * jacobian[c][m] - across * cofactor[c][m] for m in range(3)]
            for c in range(3)
        ]

    by_force, by_image = step * step * on_force, step * step * on_image
    jacobian = [
        [
            slopes[0][c][m] + by_force * slopes[1][c][m] - by_image * slopes[2][c][m]
            for m in range(3)
        ]
        for c in range(3)
    ]
    for c in range(3):
        jacobian[c][c] = jacobian[c][c] + 1.0
    shift = -mesh_step * project(fluxes(jacobian, live_weight))

    comps = range(3)
    a_first, c_first = a_of == 0, c_of == 0
    part = [shift[64 * k : 64 * k + 64] for k in comps]
    whole = [moved[64 * k : 64 * k + 64] + part[k] for k in comps]
    ours[...] = shift
    slab = jnp.concatenate([jnp.where(a_first, part[k], whole[k]) for k in comps], axis=0)
    near[...] = slab[0:96] + turn(slab[96:192], 0, 64)
    r64 = jnp.where(low_half, r_of, ROW)

    def lay(fields, place):
        out = None
        for k in comps:
            at = r64[: fields[k].shape[0]]
            piece = jnp.where(at == k, turn(fields[k], 0, k - place), 0.0)
            out = piece if out is None else out + piece
        return out + turn(out, 0, 64)

    layer = lay([jnp.where(c_first, part[k], whole[k]) for k in comps], 0)
    z_low[0:16] = lay([part[k][0:16] for k in comps], 0)
    z_low[16:64] = layer[16:64]
    z_low[64:80] = layer[0:16]
    z_low[80:96] = lay([part[k][48:64] for k in comps], 0)
    z_high[...] = lay([ours[pl.ds(64 * k + 3, 16, stride=4), :] for k in comps], EZ - 1)

    blocks = ours.reshape(3, 64, 128)
    routes = {
        (-1, 0): (near, slab_got),
        (-2, 0): (blocks.at[:, pl.ds(0, 16)], x_face_got.at[0]),
        (1, 0): (blocks.at[:, pl.ds(48, 16)], x_face_got.at[1]),
        (0, -1): (z_low.at[pl.ds(16, 64)], layer_got.at[0]),
        (-1, -1): (z_low.at[pl.ds(0, 64)], layer_got.at[1]),
        (-2, -1): (z_low.at[pl.ds(0, 16)], edge_got.at[0]),
        (1, -1): (z_low.at[pl.ds(80, 16)], edge_got.at[1]),
        (0, 1): (z_high, floor_got.at[0]),
        (-1, 1): (z_high, floor_got.at[1]),
        (-2, 1): (z_high, floor_got.at[2]),
        (1, 1): (z_high, floor_got.at[3]),
    }
    started = []
    for number, (dx, dz) in enumerate(WIDE_STEPS):
        source, target = routes[dx, dz]
        wide_copy = pltpu.make_async_remote_copy(
            src_ref=source,
            dst_ref=target,
            send_sem=wide_send.at[number],
            recv_sem=wide_recv.at[number],
            device_id=(dom + dx, sub + dz),
            device_id_type=MESH,
        )

        @pl.when(inside(dx, dz))
        def _():
            wide_copy.start()

        started.append((wide_copy, (dx, dz)))
    exchange_wait(live_copies)
    high_half = jnp.logical_not(low_half)
    one_low, one_r = low_half[0:1], r_of[0:1]
    live_up = turn(live_got[0, 0:1, :], 0, 64)
    live_layer = live_got[1, 0:1, :] + turn(live_got[2, 0:1, :], 0, 64)
    live_wide = live_own[0:1, :] + live_up + jnp.where(one_r == EZ, turn(live_layer, 0, EZ), 0.0)
    wide_weight = whole_weight[...] * live_wide
    wide_wall = jnp.where(
        jnp.logical_or(high_half, jnp.logical_or(a_of > 0, dom > 0))
        & jnp.logical_or(jnp.logical_or(c_of > 0, r_of > 0), sub > 0),
        1.0,
        0.0,
    )
    low16, row16r = low_half[:16], r_of[:16]

    exchange_wait(started)
    upper = slab_got[...]
    upper = jnp.concatenate([turn(upper, 0, 64), upper], axis=0)
    layers = jnp.where(
        low_half,
        jnp.concatenate([layer_got[0, 48:64], layer_got[0, 0:48]], axis=0),
        layer_got[1],
    )
    layers = layers + jnp.concatenate(
        [
            jnp.where(low16, edge_got[1], 0.0),
            jnp.zeros((32, 128), jnp.float32),
            jnp.where(low16, 0.0, edge_got[0]),
        ],
        axis=0,
    )
    floor = jnp.where(low16, floor_got[0], floor_got[1])
    floor = floor + jnp.where(jnp.logical_not(low16) & (row16 >= 12), turn(floor_got[2], 12, 0), 0.0)
    floor = floor + jnp.where(low16 & (row16 < 4), turn(floor_got[3], 4, 0), 0.0)
    for k in comps:
        at = 64 * k
        u = jnp.where(low_half, whole[k], upper[at : at + 64])
        u = u + jnp.where(r_of == EZ, turn(layers, 0, EZ - k), 0.0)
        wide_nodes[at : at + 64, :] = u
        wide_nodes[at : at + 16, :] += x_face_got[1, k]
        wide_nodes[at + 48 : at + 64, :] += turn(x_face_got[0, k], 0, 64)
        below = pl.ds(at, 16, stride=4)
        above = pl.ds(at + 3, 16, stride=4)
        wide_nodes[below, :] += jnp.where(row16r == 0, turn(floor, 0, -k), 0.0)
        wide_nodes[at + 48 : at + 64, :] += jnp.where(
            low16, turn(wide_nodes[at : at + 16, :], 0, 64), 0.0
        )
        tops = wide_nodes[above, :]
        bottoms = wide_nodes[below, :]
        tops = tops + jnp.where(row16r == EZ - 1, turn(bottoms, 0, -1), 0.0)
        wide_nodes[above, :] = tops
        wide_nodes[below, :] = jnp.where(row16r == EZ, turn(tops, 0, 1), bottoms)
        wide_nodes[at : at + 16, :] = jnp.where(
            low16,
            wide_nodes[at : at + 16, :],
            turn(wide_nodes[at + 48 : at + 64, :], 0, 64),
        )
    relaxed = [wide_nodes[64 * k : 64 * k + 64, :] * wide_wall for k in comps]
    shaped = dot(whole_forth, jnp.concatenate(relaxed, axis=1))
    jacobian = [
        [shaped[128 * m : 128 * m + 128, 128 * c : 128 * c + 128] for m in comps] for c in comps
    ]
    for c in comps:
        jacobian[c][c] = jacobian[c][c] + 1.0
    fields = fluxes(jacobian, wide_weight)
    right = jnp.concatenate(
        [jnp.concatenate([fields[c][m] for c in comps], axis=1) for m in comps], axis=0
    )
    product = dot(whole_back, right)
    last = []
    for k in comps:
        v = product[:, 128 * k : 128 * k + 128]
        v = v + jnp.where((b_of == 0) & (q_of > 0), turn(v, -12, ROW), 0.0)
        v = v + jnp.where((c_of == 3) & (r_of < EZ), turn(v, 3, -1), 0.0)
        v = jnp.concatenate([v[0:48], v[48:64] + turn(v[0:16], 0, 64)], axis=0)
        last.append(moved[64 * k : 64 * k + 64] - relaxed[k] + mesh_step * v)
    last = jnp.concatenate(last, axis=0)
    mesh_velocity = new_velocity - last / step

    out_nodes[0:192, :] = new_velocity * owned
    out_nodes[192:384, :] = mesh_velocity * owned
    for x in range(3):
        for pair in range(8):
            at = 16 * (x + 1) + 2 * pair
            even = out_nodes[pl.ds(at, 6, stride=64), :]
            odd = out_nodes[pl.ds(at + 1, 6, stride=64), :]
            out_wide[8 * x : 8 * x + 6, 128 * pair : 128 * pair + 128] = even + turn(odd, 0, 64)
    back = lax.dot_general(
        split_three(out_wide[...]),
        pick[...],
        (((1,), (1,)), ((), ())),
        preferred_element_type=jnp.float32,
    )
    back = back[0:24] + back[24:48] + back[48:72]
    for x in range(3):
        new_vel_out[:, plane * x : plane * (x + 1)] = back[8 * x : 8 * x + 3]
        mesh_vel_out[:, plane * x : plane * (x + 1)] = back[8 * x + 3 : 8 * x + 6]

    for copy_of, size in late:

        @pl.loop(1, size, unroll=True)
        def _(i, copy_of=copy_of):
            copy_of(i).wait_send()

    for copy, (dx, dz) in waits:

        @pl.when(inside(dx, dz))
        def _():
            copy.wait_send()


def hand_on(*refs):
    copies = [
        pltpu.make_async_copy(refs[k], refs[3 + k], refs[6].at[k]) for k in range(3)
    ]
    for copy in copies:
        copy.start()
    for copy in copies:
        copy.wait()


def body(n_dom, n_sub, displacement, velocity, energy, mass_density, live_mask, time_step):
    made_tables = tables()
    vmem = pl.BlockSpec(memory_space=pltpu.VMEM)
    anywhere = pl.BlockSpec(memory_space=pl.ANY)
    f32 = jnp.float32
    nodes = displacement.shape[1]
    wide_sum = n_dom * n_sub if n_dom * n_sub <= 64 else n_dom
    made = pl.pallas_call(
        functools.partial(kernel, n_dom, n_sub),
        out_shape=(
            pltpu.VMEM(displacement.shape, f32),
            pltpu.VMEM(energy.shape, f32),
            pltpu.VMEM(displacement.shape, f32),
        ),
        in_specs=[anywhere] * (6 + len(made_tables)),
        out_specs=(vmem, vmem, vmem),
        scratch_shapes=[
            pltpu.VMEM((8, nodes), f32),
            pltpu.VMEM((24, 1024), f32),
            pltpu.VMEM((512, 128), f32),
            pltpu.VMEM((2, 192, 128), f32),
            pltpu.VMEM((192, 128), f32),
            pltpu.VMEM((384, 128), f32),
            pltpu.VMEM((24, 1024), f32),
            pltpu.VMEM((128, 128), f32),
            pltpu.VMEM((32, 128), f32),
            pltpu.VMEM((8, 128), f32),
            pltpu.VMEM((3, 8, 128), f32),
            pltpu.VMEM((3, 2, 16, 128), f32),
            pltpu.VMEM((6, 16, 128), f32),
            pltpu.VMEM((2, 2, 3, 16, 128), f32),
            pltpu.VMEM((3, 2, 16, 128), f32),
            pltpu.VMEM((3, 4, 8, 128), f32),
            pltpu.VMEM((wide_sum, 1, 128), f32),
            pltpu.VMEM((n_sub, 1, 128), f32),
            pltpu.SemaphoreType.DMA((3, 8)),
            pltpu.SemaphoreType.DMA((3, 8)),
            pltpu.SemaphoreType.DMA((wide_sum,)),
            pltpu.SemaphoreType.DMA((wide_sum,)),
            pltpu.SemaphoreType.DMA((n_sub,)),
            pltpu.SemaphoreType.DMA((n_sub,)),
            pltpu.VMEM(displacement.shape, f32),
            pltpu.VMEM(velocity.shape, f32),
            pltpu.VMEM(energy.shape, f32),
            pltpu.VMEM(mass_density.shape[::-1], f32),
            pltpu.VMEM((1, live_mask.shape[0]), jnp.int32),
            pltpu.SMEM((1, 1), f32),
            *[pltpu.VMEM(t.shape, t.dtype) for t in made_tables],
            pltpu.SemaphoreType.DMA((6 + len(made_tables),)),
            pltpu.VMEM((192, 128), f32),
            pltpu.VMEM((96, 128), f32),
            pltpu.VMEM((96, 128), f32),
            pltpu.VMEM((16, 128), f32),
            pltpu.VMEM((96, 128), f32),
            pltpu.VMEM((2, 3, 16, 128), f32),
            pltpu.VMEM((2, 64, 128), f32),
            pltpu.VMEM((2, 16, 128), f32),
            pltpu.VMEM((4, 16, 128), f32),
            pltpu.VMEM((192, 128), f32),
            pltpu.SemaphoreType.DMA((len(WIDE_STEPS),)),
            pltpu.SemaphoreType.DMA((len(WIDE_STEPS),)),
            pltpu.SemaphoreType.DMA((3,)),
            pltpu.SemaphoreType.DMA((3,)),
        ],
        compiler_params=pltpu.CompilerParams(collective_id=0, has_side_effects=True),
    )(
        displacement,
        velocity,
        energy,
        mass_density.T,
        live_mask.reshape(1, -1),
        time_step.reshape(1, 1),
        *[jnp.asarray(t) for t in made_tables],
    )
    return pl.pallas_call(
        hand_on,
        out_shape=[jax.ShapeDtypeStruct(m.shape, f32) for m in made],
        in_specs=[vmem] * 3,
        out_specs=[anywhere] * 3,
        scratch_shapes=[pltpu.SemaphoreType.DMA((3,))],
    )(*[pltpu.with_memory_space_constraint(m, pltpu.VMEM) for m in made])


def solution(mesh):
    split = ("dom", "sub")
    return jax.shard_map(
        functools.partial(body, mesh.shape["dom"], mesh.shape["sub"]),
        mesh=mesh,
        in_specs=(
            P(None, split),
            P(None, split),
            P(None, split),
            P(None, split),
            P(split),
            P(),
        ),
        out_specs=(P(None, split), P(None, split), P(None, split)),
        check_vma=False,
    )
```

```python
import functools
import math

import jax
import jax.numpy as jnp
import numpy as np
from jax import lax
from jax.experimental import pallas as pl
from jax.experimental.pallas import tpu as pltpu
from jax.sharding import PartitionSpec as P

EX = 1
EY = 8
EZ = 6
ELEMS = EX * EY * EZ
HALF = 64
ROW = 8

adiabatic = 5.0 / 3.0
viscosity = 0.3
mesh_step = 0.01
MESH = pl.DeviceIdType.MESH
STEPS = [(dx, dz) for dx in (-1, 0, 1) for dz in (-1, 0, 1) if (dx, dz) != (0, 0)]
WIDE_STEPS = [(-2, -1), (-2, 1), (1, -1), (1, 1), (-1, 1), (-1, -1)]
WIDE_STEPS += [(0, -1), (0, 1), (-2, 0), (1, 0), (-1, 0)]


def one_dimension():
    root_term = math.sqrt(10.0 / 7.0)
    outer_root = math.sqrt(5.0 + 2.0 * root_term) / 3.0
    inner_root = math.sqrt(5.0 - 2.0 * root_term) / 3.0
    gauss_roots = np.array([-outer_root, -inner_root, 0.0, inner_root, outer_root])
    outer_weight = (322.0 - 13.0 * math.sqrt(70.0)) / 900.0
    middle_weight = (322.0 + 13.0 * math.sqrt(70.0)) / 900.0
    weights = (
        np.array([outer_weight, middle_weight, 128.0 / 225.0, middle_weight, outer_weight]) / 2.0
    )
    points = (1.0 + gauss_roots) / 2.0
    lobatto = [0.0, (1.0 - 1.0 / math.sqrt(5.0)) / 2.0, (1.0 + 1.0 / math.sqrt(5.0)) / 2.0, 1.0]
    values = np.ones((5, 4))
    slopes = np.zeros((5, 4))
    for node in range(4):
        for other in range(4):
            if other != node:
                values[:, node] *= (points - lobatto[other]) / (lobatto[node] - lobatto[other])
                term = np.ones(5) / (lobatto[node] - lobatto[other])
                for third in range(4):
                    if third != node and third != other:
                        term = term * (points - lobatto[third]) / (lobatto[node] - lobatto[third])
                slopes[:, node] += term
    bernstein = np.stack([(1.0 - points) ** 2, 2.0 * points * (1.0 - points), points**2], axis=1)
    return values, slopes, bernstein, weights


def outer_triple(first, second, third):
    product = np.einsum("ia,jb,kc->ijkabc", first, second, third)
    return product.reshape(125, -1)


def halves(table, rows):
    padded = np.concatenate([table, np.repeat(table[-1:], 3, axis=0)], axis=0)
    padded = np.pad(padded, [(0, 0), (0, rows - table.shape[1])])
    return np.concatenate([padded[:64], padded[64:]], axis=1)


def stacked_left(table):
    table = np.asarray(table, np.float32)
    high = table.astype(jnp.bfloat16)
    low = (table - high.astype(np.float32)).astype(jnp.bfloat16)
    return np.concatenate([low, high, high], axis=1)


@functools.lru_cache(None)
def tables():
    values, slopes, bernstein, weights = one_dimension()
    triples = [
        outer_triple(slopes, values, values),
        outer_triple(values, slopes, values),
        outer_triple(values, values, slopes),
    ]
    grad = np.concatenate([halves(t, 64) for t in triples], axis=0)
    whole = [np.concatenate([t, np.repeat(t[-1:], 3, axis=0)], axis=0) for t in triples]
    basis = halves(outer_triple(values, values, values), 64)
    energy = halves(outer_triple(bernstein, bernstein, bernstein), 32)
    weight = np.einsum("i,j,k->ijk", weights, weights, weights).reshape(125)
    weight = np.pad(weight, (0, 3))
    spread_weight = np.zeros((64, 128))
    spread_weight[:, :64] = weight[:64, None]
    spread_weight[:, 64:] = weight[64:, None]
    whole_weight = np.repeat(weight[:, None], 128, axis=1)
    planes_y, planes_z = 3 * EY + 1, 3 * EZ
    pick = np.zeros((planes_y * planes_z, 16 * HALF), np.float32)
    for b in range(4):
        for c in range(4):
            for q in range(EY):
                for r in range(EZ):
                    z = 3 * r + c - 1
                    if z >= 0:
                        lane = (4 * b + c) * HALF + q * ROW + r
                        pick[(3 * q + b) * planes_z + z, lane] = 1.0
    widen = np.zeros((128, 256), np.float32)
    for e in range(ELEMS):
        to = e // EZ * ROW + e % EZ
        widen[e, to] = 1.0
        widen[to, 128 + e] = 1.0
    return [
        pick.astype(jnp.bfloat16),
        stacked_left(grad),
        stacked_left(grad.T),
        stacked_left(basis),
        stacked_left(basis.T),
        stacked_left(energy),
        stacked_left(energy.T),
        stacked_left(np.concatenate(whole, axis=0)),
        stacked_left(np.concatenate(whole, axis=0).T),
        widen.astype(jnp.bfloat16),
        np.asarray(spread_weight, np.float32),
        np.asarray(whole_weight, np.float32),
    ]


def dot(table, right):
    high, low = split_two(right)
    stacked = jnp.concatenate([high, low, high], axis=0)
    return jnp.dot(table[...], stacked, preferred_element_type=jnp.float32)


def split_two(value):
    high = value.astype(jnp.bfloat16)
    return high, (value - high.astype(jnp.float32)).astype(jnp.bfloat16)


def cofactors(m):
    return [
        [
            m[(i + 1) % 3][(j + 1) % 3] * m[(i + 2) % 3][(j + 2) % 3]
            - m[(i + 1) % 3][(j + 2) % 3] * m[(i + 2) % 3][(j + 1) % 3]
            for j in range(3)
        ]
        for i in range(3)
    ]


def turn(value, rows, lanes):
    if rows:
        value = pltpu.roll(value, rows % value.shape[0], 0)
    if lanes % value.shape[1]:
        value = pltpu.roll(value, lanes % value.shape[1], 1)
    return value


def split_three(value):
    high = value.astype(jnp.bfloat16).astype(jnp.float32)
    rest = value - high
    middle = rest.astype(jnp.bfloat16).astype(jnp.float32)
    return jnp.concatenate([high, middle, rest - middle], axis=0).astype(jnp.bfloat16)


def kernel(
    n_dom,
    n_sub,
    disp_in_hbm,
    vel_in_hbm,
    energy_in_hbm,
    density_in_hbm,
    live_in_hbm,
    step_in_hbm,
    pick_hbm,
    grad_forth_hbm,
    grad_back_hbm,
    basis_forth_hbm,
    basis_back_hbm,
    energy_forth_hbm,
    energy_back_hbm,
    whole_forth_hbm,
    whole_back_hbm,
    widen_hbm,
    quad_weight_hbm,
    whole_weight_hbm,
    new_vel_out,
    rate_out,
    mesh_vel_out,
    flat,
    wide,
    first,
    local,
    state,
    out_nodes,
    out_wide,
    density_pad,
    energy_pad,
    live_own,
    live_got,
    packs,
    x_first,
    x_got,
    z_got,
    d_got,
    sum_dom,
    sum_sub,
    send_sems,
    recv_sems,
    dom_send,
    dom_recv,
    sub_send,
    sub_recv,
    disp_in,
    vel_in,
    energy_in,
    density_in,
    live_in,
    step_in,
    pick,
    grad_forth,
    grad_back,
    basis_forth,
    basis_back,
    energy_forth,
    energy_back,
    whole_forth,
    whole_back,
    widen,
    quad_weight,
    whole_weight,
    in_sems,
    ours,
    near,
    z_low,
    z_high,
    x_face,
    slab_got,
    x_face_got,
    layer_got,
    edge_got,
    floor_got,
    wide_nodes,
    wide_send,
    wide_recv,
    live_send,
    live_recv,
):
    dom = lax.axis_index("dom")
    sub = lax.axis_index("sub")
    plane = (3 * EY + 1) * 3 * EZ

    def inside(dx, dz):
        ok = None
        for step, place, size in ((dx, dom, n_dom), (dz, sub, n_sub)):
            if step:
                here = (place + step >= 0) if step < 0 else (place + step < size)
                ok = here if ok is None else jnp.logical_and(ok, here)
        return ok

    held = [
        (disp_in_hbm, disp_in),
        (vel_in_hbm, vel_in),
        (pick_hbm, pick),
        (step_in_hbm, step_in),
        (density_in_hbm, density_in),
        (energy_in_hbm, energy_in),
        (live_in_hbm, live_in),
        (grad_forth_hbm, grad_forth),
        (grad_back_hbm, grad_back),
        (basis_forth_hbm, basis_forth),
        (basis_back_hbm, basis_back),
        (energy_forth_hbm, energy_forth),
        (energy_back_hbm, energy_back),
        (whole_forth_hbm, whole_forth),
        (widen_hbm, widen),
        (quad_weight_hbm, quad_weight),
        (whole_weight_hbm, whole_weight),
        (whole_back_hbm, whole_back),
    ]
    loads = [
        pltpu.make_async_copy(source, target, in_sems.at[number])
        for number, (source, target) in enumerate(held)
    ]
    for load in loads:
        load.start()

    x_first[...] = jnp.zeros_like(x_first)
    x_got[...] = jnp.zeros_like(x_got)
    z_got[...] = jnp.zeros_like(z_got)
    d_got[...] = jnp.zeros_like(d_got)
    for got in (slab_got, x_face_got, layer_got, edge_got, floor_got, live_got):
        got[...] = jnp.zeros_like(got)

    barrier = pltpu.get_barrier_semaphore()
    one_phase = n_dom * n_sub <= 64
    if one_phase and n_sub <= 4:
        count = n_dom - 1
        for dz in (-1, 1):
            count = count + n_dom * inside(0, dz).astype(jnp.int32)
        for dz in (0, -1, 1):

            def greet(dz=dz):
                @pl.loop(0 if dz else 1, n_dom, unroll=True)
                def _(i):
                    pl.semaphore_signal(
                        barrier,
                        inc=1,
                        device_id=(lax.rem(dom + i, n_dom), sub + dz),
                        device_id_type=MESH,
                    )

            if dz:
                pl.when(inside(0, dz))(greet)
            else:
                greet()

    elif one_phase:
        devices = n_dom * n_sub
        count = devices - 1

        @pl.loop(1, devices, unroll=True)
        def _(i):
            t = lax.rem(dom * n_sub + sub + i, devices)
            pl.semaphore_signal(
                barrier,
                inc=1,
                device_id=(t // n_sub, lax.rem(t, n_sub)),
                device_id_type=MESH,
            )

    else:
        count = (n_dom - 1) + (n_sub - 1)
        for dx, dz in [(dx, dz) for dx in (-2, -1, 1, 2) for dz in (-1, 1)]:
            if dx and dz:
                ok = inside(dx, dz)
                count = count + ok.astype(jnp.int32)

                @pl.when(ok)
                def _():
                    pl.semaphore_signal(
                        barrier, inc=1, device_id=(dom + dx, sub + dz), device_id_type=MESH
                    )

        @pl.loop(1, n_dom)
        def _(i):
            pl.semaphore_signal(
                barrier, inc=1, device_id=(lax.rem(dom + i, n_dom), sub), device_id_type=MESH
            )

        @pl.loop(1, n_sub)
        def _(i):
            pl.semaphore_signal(
                barrier, inc=1, device_id=(dom, lax.rem(sub + i, n_sub)), device_id_type=MESH
            )

    first[...] = jnp.zeros_like(first)
    density_pad[...] = jnp.zeros_like(density_pad)
    energy_pad[...] = jnp.zeros_like(energy_pad)
    flat[...] = jnp.zeros_like(flat)
    out_wide[...] = jnp.zeros_like(out_wide)

    lane = lax.broadcasted_iota(jnp.int32, (64, 128), 1)
    row = lax.broadcasted_iota(jnp.int32, (64, 128), 0)
    q_of, r_of = (lane % HALF) // ROW, lane % ROW
    a_of, b_of, c_of = row // 16, (row // 4) % 4, row % 4
    low_half = lane < HALF
    valid = low_half & (r_of < EZ)
    triple = lambda x: jnp.concatenate([x, x, x], axis=0)
    y_up = triple((b_of == 3) & (q_of < EY - 1) & valid)
    y_down = triple((b_of == 0) & (q_of > 0) & valid)
    z_up = triple((c_of == 3) & (r_of < EZ - 1) & valid)
    z_down = triple((c_of == 0) & (r_of > 0) & valid)
    off_wall = jnp.where(
        valid
        & jnp.logical_or(a_of > 0, dom > 0)
        & jnp.logical_or(jnp.logical_or(c_of > 0, r_of > 0), sub > 0),
        1.0,
        0.0,
    )
    off_wall = triple(off_wall)
    owned = jnp.where(
        valid & (a_of > 0) & (c_of > 0) & ((b_of < 3) | (q_of == EY - 1)), 1.0, 0.0
    )
    owned = triple(owned)
    lane16, row16 = lane[:16], row[:16]
    r16 = jnp.where(lane16 < HALF, lane16 % ROW, ROW)

    for load in loads[:3]:
        load.wait()
    flat[0:3, :] = disp_in[...]
    flat[3:6, :] = vel_in[...]
    stacked = jnp.concatenate([flat[:, plane * x : plane * (x + 1)] for x in range(3)], axis=0)
    picked = jnp.dot(split_three(stacked), pick[...], preferred_element_type=jnp.float32)
    wide[...] = picked[0:24] + picked[24:48] + picked[48:72]
    for x in range(3):
        for pair in range(8):
            got = wide[8 * x : 8 * x + 8, 128 * pair : 128 * pair + 128]
            other = turn(got, 0, 64)
            at = 16 * (x + 1) + 2 * pair
            keep = lane[:8] < 64
            first[pl.ds(at, 8, stride=64), :] = jnp.where(keep, got, 0.0)
            first[pl.ds(at + 1, 8, stride=64), :] = jnp.where(keep, other, 0.0)

    pl.semaphore_wait(barrier, count)

    def faces(source, fields, place, shifts):
        packed = jnp.zeros((16, 128), jnp.float32)
        for k in range(fields):
            face = source[pl.ds(64 * k + place, 16, stride=4), :]
            if place == 3:
                packed = jnp.where(r16 == EZ - 1 - k, turn(face, 0, -k), packed)
            else:
                packed = jnp.where(r16 == k, turn(face, 0, k), packed)
        return packed

    waits = []

    def exchange_start(rnd, source, fields, x_target, ups, downs):
        if ups:
            packs[rnd, 1] = faces(source, fields, 3, None)
        if downs:
            packs[rnd, 0] = faces(source, fields, 0, None)
        started = []
        for number, (dx, dz) in enumerate(STEPS):
            lead = dz if dz else dx
            going = (dx, dz)
            up = all(s >= 0 for s in going)
            down = all(s <= 0 for s in going)
            if not ((ups and downs) or (ups and up) or (downs and down)):
                continue
            target = (dom + dx, sub + dz)
            jobs = []
            if dz == 0:
                base = 48 if dx > 0 else 0
                slot = 0 if dx > 0 else 1
                jobs.append(
                    (
                        source_blocks(source, fields, base),
                        x_target(slot),
                    )
                )
            elif dx == 0:
                side = 1 if dz > 0 else 0
                jobs.append((packs.at[rnd, side], z_got.at[rnd, 1 - side]))
            else:
                side = 1 if dz > 0 else 0
                half = 8 if dx > 0 else 0
                slot = (0 if dx > 0 else 1) + 2 * (1 - side)
                jobs.append((packs.at[rnd, side, pl.ds(half, 8)], d_got.at[rnd, slot]))
            src, dst = jobs[0]
            copy = pltpu.make_async_remote_copy(
                src_ref=src,
                dst_ref=dst,
                send_sem=send_sems.at[rnd, number],
                recv_sem=recv_sems.at[rnd, number],
                device_id=target,
                device_id_type=MESH,
            )

            @pl.when(inside(dx, dz))
            def _():
                copy.start()

            started.append((copy, (dx, dz)))
        return started

    def source_blocks(source, fields, base):
        blocks = source.reshape(source.shape[0] // 64, 64, 128)
        return blocks.at[pl.ds(0, fields), pl.ds(base, 16)]

    def exchange_wait(started):
        for copy, (dx, dz) in started:

            @pl.when(inside(-dx, -dz))
            def _():
                copy.wait_recv()

        waits.extend(started)

    def exchange_add(rnd, source, target, fields, x_from, ups, downs):
        if target is not source:
            target[...] = source[...]
        top = lax.broadcasted_iota(jnp.int32, (8, 128), 0) < 4
        for came, side, place in ((ups, 0, 0), (downs, 1, 3)):
            if not came:
                continue
            face = z_got[rnd, side]
            low = jnp.where(top, turn(d_got[rnd, 2 * side], 4, 0), 0.0)
            high = jnp.where(top, 0.0, turn(d_got[rnd, 2 * side + 1], 4, 0))
            face = face + jnp.concatenate([low, high], axis=0)
            for k in range(fields):
                if place == 0:
                    part = jnp.where(r16 == 0, turn(face, 0, k - (EZ - 1)), 0.0)
                else:
                    part = jnp.where(r16 == EZ - 1, turn(face, 0, EZ - 1 - k), 0.0)
                at = pl.ds(64 * k + place, 16, stride=4)
                target[at, :] = target[at, :] + part
        for k in range(fields):
            if ups:
                target[64 * k : 64 * k + 16, :] += x_from(0)[k]
            if downs:
                target[64 * k + 48 : 64 * k + 64, :] += x_from(1)[k]

    started = exchange_start(0, first, 6, lambda slot: x_first, True, False)

    for load in loads[3:]:
        load.wait()
    step = step_in[0, 0]
    for q in range(EY):
        density_pad[ROW * q : ROW * q + EZ, 0:125] = density_in[EZ * q : EZ * q + EZ, :]
    energy_pad[0:27, 0:ELEMS] = energy_in[...]
    energy_pad[27:28, 0:ELEMS] = live_in[...].astype(jnp.float32)

    def exact(value, table):
        rows = value.shape[0]
        out = jnp.dot(split_three(value), table, preferred_element_type=jnp.float32)
        return out[0:rows] + out[rows : 2 * rows] + out[2 * rows :]

    by_lane = exact(energy_pad[...], widen[:, 0:128])
    live = by_lane[27:28, :]
    live_own[...] = jnp.broadcast_to(live, (8, 128))
    live_copies = []
    for number, (dx, dz) in enumerate(((-1, 0), (0, -1), (-1, -1))):
        live_copy = pltpu.make_async_remote_copy(
            src_ref=live_own,
            dst_ref=live_got.at[number],
            send_sem=live_send.at[number],
            recv_sem=live_recv.at[number],
            device_id=(dom + dx, sub + dz),
            device_id_type=MESH,
        )
        live_copies.append((live_copy, (dx, dz)))

        @pl.when(inside(dx, dz))
        def _():
            live_copy.start()

    live = live + turn(live, 0, 64)
    by_point = jnp.transpose(density_pad[...])
    mass_density = by_point[0:64] + turn(by_point[64:128], 0, 64)
    weight = quad_weight[...]
    live_weight = weight * live
    mass_weight = live_weight * mass_density
    at_points = dot(energy_forth, jnp.concatenate([by_lane, turn(by_lane, 0, 64)], axis=0))

    def paired(v):
        return jnp.concatenate(
            [
                jnp.concatenate([v[64 * k : 64 * k + 64], turn(v[64 * k : 64 * k + 64], 0, 64)], 0)
                for k in range(v.shape[0] // 64)
            ],
            axis=1,
        )

    def folded(product):
        half = product.shape[0] // 2
        out = []
        for k in range(product.shape[1] // 128):
            part = product[:, 128 * k : 128 * k + 128]
            out.append(part[:half] + turn(part[half:], 0, 64))
        return out

    def gradient(v):
        shaped = dot(grad_forth, paired(v))
        return [
            [shaped[64 * m : 64 * m + 64, 128 * c : 128 * c + 128] for m in range(3)]
            for c in range(3)
        ]

    def jacobian_of(v):
        jacobian = gradient(v)
        for c in range(3):
            jacobian[c][c] = jacobian[c][c] + 1.0
        return jacobian

    def project(fields):
        right = jnp.concatenate(
            [jnp.concatenate([fields[c][m] for c in range(3)], axis=1) for m in range(3)], axis=0
        )
        return share(jnp.concatenate(folded(dot(grad_back, right)), axis=0))

    def share(v):
        v = v * jnp.where(triple(valid), 1.0, 0.0)
        v = v + jnp.where(y_up, turn(v, 12, -ROW), 0.0) + jnp.where(y_down, turn(v, -12, ROW), 0.0)
        v = v + jnp.where(z_up, turn(v, 3, -1), 0.0) + jnp.where(z_down, turn(v, -3, 1), 0.0)
        return v

    def interpolate(v):
        return dot(basis_forth, paired(v))

    def volume_of(jacobian, cofactor):
        return (
            jacobian[0][0] * cofactor[0][0]
            + jacobian[0][1] * cofactor[0][1]
            + jacobian[0][2] * cofactor[0][2]
        )

    def begin(rnd, v, ups=True, downs=True):
        source = local.at[rnd - 1]
        source[...] = v
        return exchange_start(rnd, source, 3, lambda slot: x_got.at[rnd - 1, slot], ups, downs)

    def finish(rnd, started, ups=True, downs=True):
        exchange_wait(started)
        source = local.at[rnd - 1]
        exchange_add(
            rnd, source, state, 3, lambda slot: x_got.at[rnd - 1, slot], ups, downs
        )
        return state[...] * off_wall

    exchange_wait(started)
    out_nodes[...] = first[0:384, :]
    exchange_add(0, out_nodes, out_nodes, 6, lambda slot: x_first, True, False)
    displacement = out_nodes[0:192, :]
    velocity = out_nodes[192:384, :]

    jacobian = jacobian_of(displacement)
    velocity_grad = gradient(velocity)
    cofactor = cofactors(jacobian)
    volume = volume_of(jacobian, cofactor)
    inverse = 1.0 / volume
    density = mass_density * inverse
    pressure = (adiabatic - 1.0) * density * at_points
    spatial = [
        [
            (
                velocity_grad[c][0] * cofactor[m][0]
                + velocity_grad[c][1] * cofactor[m][1]
                + velocity_grad[c][2] * cofactor[m][2]
            )
            * inverse
            for m in range(3)
        ]
        for c in range(3)
    ]
    viscous = viscosity * density
    stress = [[None] * 3 for _ in range(3)]
    for c in range(3):
        for m in range(c, 3):
            value = viscous * (spatial[c][m] + spatial[m][c])
            stress[c][m] = stress[m][c] = value - pressure if c == m else value
    flux = [
        [
            -live_weight
            * (
                stress[c][0] * cofactor[0][m]
                + stress[c][1] * cofactor[1][m]
                + stress[c][2] * cofactor[2][m]
            )
            for m in range(3)
        ]
        for c in range(3)
    ]
    started = begin(1, project(flux))
    power = stress[0][0] * spatial[0][0]
    for c in range(3):
        for m in range(3):
            if c + m > 0:
                power = power + stress[c][m] * spatial[c][m]
    power = live_weight * volume * power
    sums = folded(
        dot(energy_back, jnp.concatenate([power, weight * mass_density], axis=1))
    )
    rates = jnp.where(valid[:32], sums[0] / jnp.where(valid[:32], sums[1], 1.0), 0.0)
    rate_out[...] = exact(rates, widen[:, 128:256])[0:27, 0:ELEMS]
    force = finish(1, started)

    wide_mass = jnp.concatenate([mass_weight] * 3, axis=1)
    values = interpolate(force)
    weighted = wide_mass * values
    image = share(jnp.concatenate(folded(dot(basis_back, weighted)), axis=0))
    started = begin(2, image)

    def total(x):
        return jnp.sum(jnp.sum(x, axis=0, keepdims=True), axis=1, keepdims=True)

    norm_part = total(force * force * owned)
    product_part = total(weighted * values)
    image = finish(2, started)
    image_norm_part = total(image * image * owned)
    values = interpolate(image)
    image_product_part = total(wide_mass * values * values)

    lane1 = lane[0:1]
    packed = jnp.where(
        lane1 == 0,
        norm_part,
        jnp.where(
            lane1 == 1,
            product_part,
            jnp.where(lane1 == 2, image_norm_part, image_product_part),
        ),
    )

    late = []

    def all_sum(value, slots, size, place, target, sends, recvs, cover=None):
        slots[0] = value

        def copy_of(i):
            return pltpu.make_async_remote_copy(
                src_ref=slots.at[0],
                dst_ref=slots.at[i],
                send_sem=sends.at[i],
                recv_sem=recvs.at[i],
                device_id=target(lax.rem(place + i, size)),
                device_id_type=MESH,
            )

        @pl.loop(1, size, unroll=True)
        def _(i):
            copy_of(i).start()

        out = cover() if cover else None

        @pl.loop(1, size, unroll=True)
        def _(i):
            copy_of(i).wait_recv()

        late.append((copy_of, size))
        return jnp.sum(slots[...], axis=0), out

    def ahead():
        return [gradient(v) for v in (displacement + step * velocity, force, image)]

    if one_phase:
        packed, slopes = all_sum(
            packed,
            sum_dom,
            n_dom * n_sub,
            dom * n_sub + sub,
            lambda t: (t // n_sub, lax.rem(t, n_sub)),
            dom_send,
            dom_recv,
            ahead,
        )
    else:
        packed, slopes = all_sum(
            packed, sum_dom, n_dom, dom, lambda t: (t, sub), dom_send, dom_recv, ahead
        )
        packed, _ = all_sum(packed, sum_sub, n_sub, sub, lambda t: (dom, t), sub_send, sub_recv)
    rr, rw, ww, wmw = (
        jnp.sum(jnp.where(lane1 == k, packed, 0.0), axis=1, keepdims=True) for k in range(4)
    )
    first_length = rr / rw
    next_norm = first_length * (first_length * ww) - rr
    conjugacy = next_norm / rr
    residual_image = rw - first_length * ww
    residual_product = rw - 2.0 * first_length * ww + first_length * first_length * wmw
    bend = residual_product + 2.0 * conjugacy * residual_image + conjugacy * conjugacy * rw
    second_length = next_norm / bend
    on_force = first_length + second_length * (1.0 + conjugacy)
    on_image = second_length * first_length
    new_velocity = velocity + step * (on_force * force - on_image * image)
    moved = displacement + step * new_velocity

    def fluxes(jacobian, weights):
        cofactor = cofactors(jacobian)
        volume = volume_of(jacobian, cofactor)
        norm_sq = None
        for c in range(3):
            for m in range(3):
                square = jacobian[c][m] * jacobian[c][m]
                norm_sq = square if norm_sq is None else norm_sq + square
        scale = weights * jnp.exp(jnp.log(volume) * (-2.0 / 3.0))
        along = scale * (2.0 / 3.0)
        across = scale * (2.0 / 9.0) * (norm_sq / volume)
        return [
            [along * jacobian[c][m] - across * cofactor[c][m] for m in range(3)]
            for c in range(3)
        ]

    def back_to_lattice(nodes):
        for x in range(3):
            for pair in range(8):
                at = 16 * (x + 1) + 2 * pair
                even = nodes[pl.ds(at, 3, stride=64), :]
                odd = nodes[pl.ds(at + 1, 3, stride=64), :]
                out_wide[8 * x : 8 * x + 3, 128 * pair : 128 * pair + 128] = even + turn(odd, 0, 64)
        back = lax.dot_general(
            split_three(out_wide[...]), pick[...], (((1,), (1,)), ((), ())), preferred_element_type=jnp.float32
        )
        return back[0:24] + back[24:48] + back[48:72]

    by_force, by_image = step * step * on_force, step * step * on_image
    jacobian = [
        [
            slopes[0][c][m] + by_force * slopes[1][c][m] - by_image * slopes[2][c][m]
            for m in range(3)
        ]
        for c in range(3)
    ]
    for c in range(3):
        jacobian[c][c] = jacobian[c][c] + 1.0
    shift = -mesh_step * project(fluxes(jacobian, live_weight))

    comps = range(3)
    a_first, c_first = a_of == 0, c_of == 0
    part = [shift[64 * k : 64 * k + 64] for k in comps]
    whole = [moved[64 * k : 64 * k + 64] + part[k] for k in comps]
    ours[...] = shift
    slab = jnp.concatenate([jnp.where(a_first, part[k], whole[k]) for k in comps], axis=0)
    near[...] = slab[0:96] + turn(slab[96:192], 0, 64)
    r64 = jnp.where(low_half, r_of, ROW)

    def lay(fields, place):
        out = None
        for k in comps:
            at = r64[: fields[k].shape[0]]
            piece = jnp.where(at == k, turn(fields[k], 0, k - place), 0.0)
            out = piece if out is None else out + piece
        return out + turn(out, 0, 64)

    layer = [jnp.where(c_first, part[k], whole[k]) for k in comps]
    right_half = jnp.logical_not(low_half)
    r_here = r_of[:16]

    def lay_group(fields, a):
        out = None
        half = low_half[:16] if a < 2 else right_half[:16]
        for k in comps:
            spot = 3 * (a % 2) + k
            piece = jnp.where(
                half & (r_here == spot), turn(fields[k], 0, 64 * (a // 2) + spot), 0.0
            )
            out = piece if out is None else out + piece
        return out

    groups = [lay_group([f[16 * a : 16 * a + 16] for f in layer], a) for a in range(4)]
    upper_groups = groups[1] + groups[2] + groups[3]
    face_part = lay_group([part[k][0:16] for k in comps], 0)
    z_low[0] = turn(face_part + upper_groups, 0, 64)
    z_low[1] = groups[0] + upper_groups
    z_low[2] = lay([part[k][48:64] for k in comps], 0)
    z_high[...] = lay([ours[pl.ds(64 * k + 3, 16, stride=4), :] for k in comps], EZ - 1)
    x_face[0, 0:16] = part[1][0:16] + turn(part[0][0:16], 0, 64)
    x_face[0, 16:24] = part[2][8:16] + turn(part[2][0:8], 0, 64)
    x_face[1, 0:16] = part[0][48:64] + turn(part[1][48:64], 0, 64)
    x_face[1, 16:24] = part[2][48:56] + turn(part[2][56:64], 0, 64)

    routes = {
        (-1, 0): (near, slab_got),
        (-2, 0): (x_face.at[0], x_face_got.at[0]),
        (1, 0): (x_face.at[1], x_face_got.at[1]),
        (0, -1): (z_low.at[1], layer_got.at[0]),
        (-1, -1): (z_low.at[0], layer_got.at[1]),
        (-2, -1): (z_low.at[0], edge_got.at[0]),
        (1, -1): (z_low.at[2], edge_got.at[1]),
        (0, 1): (z_high, floor_got.at[0]),
        (-1, 1): (z_high, floor_got.at[1]),
        (-2, 1): (z_high.at[pl.ds(0, 8)], floor_got.at[2, pl.ds(0, 8)]),
        (1, 1): (z_high.at[pl.ds(8, 8)], floor_got.at[3, pl.ds(8, 8)]),
    }
    started = []
    for number, (dx, dz) in enumerate(WIDE_STEPS):
        source, target = routes[dx, dz]
        wide_copy = pltpu.make_async_remote_copy(
            src_ref=source,
            dst_ref=target,
            send_sem=wide_send.at[number],
            recv_sem=wide_recv.at[number],
            device_id=(dom + dx, sub + dz),
            device_id_type=MESH,
        )

        @pl.when(inside(dx, dz))
        def _():
            wide_copy.start()

        started.append((wide_copy, (dx, dz)))
    exchange_wait(live_copies)
    out_nodes[0:192, :] = new_velocity * owned
    new_back = back_to_lattice(out_nodes)
    one_low, one_r = low_half[0:1], r_of[0:1]
    live_up = turn(live_got[0, 0:1, :], 0, 64)
    live_layer = live_got[1, 0:1, :] + turn(live_got[2, 0:1, :], 0, 64)
    live_wide = live_own[0:1, :] + live_up + jnp.where(one_r == EZ, turn(live_layer, 0, EZ), 0.0)
    wide_weight = whole_weight[...] * live_wide
    wide_wall = jnp.where(
        jnp.logical_or(right_half, jnp.logical_or(a_of > 0, dom > 0))
        & jnp.logical_or(jnp.logical_or(c_of > 0, r_of > 0), sub > 0),
        1.0,
        0.0,
    )
    low16, row16r = low_half[:16], r_of[:16]

    exchange_wait(started)
    upper = slab_got[...]
    upper = jnp.concatenate([turn(upper, 0, 64), upper], axis=0)
    first_got, second_got = layer_got[0], layer_got[1]
    mixed = (
        jnp.where(low16, first_got, second_got),
        jnp.where(low16, second_got, first_got),
    )
    right16 = right_half[:16]
    edge_up = jnp.where(right16, edge_got[0], 0.0)
    edge_down = jnp.where(low16, edge_got[1], 0.0)
    floor = jnp.where(low16, floor_got[0], floor_got[1])
    floor = floor + jnp.where(right16 & (row16 >= 12), turn(floor_got[2], 12, 0), 0.0)
    floor = floor + jnp.where(low16 & (row16 < 4), turn(floor_got[3], 4, 0), 0.0)
    face_low = [
        x_face_got[1, 0:16],
        turn(x_face_got[1, 0:16], 0, 64),
        jnp.concatenate([x_face_got[1, 16:24], turn(x_face_got[1, 16:24], 0, 64)], axis=0),
    ]
    face_high = [
        x_face_got[0, 0:16],
        turn(x_face_got[0, 0:16], 0, 64),
        jnp.concatenate([x_face_got[0, 16:24], turn(x_face_got[0, 16:24], 0, 64)], axis=0),
    ]
    for k in comps:
        at = 64 * k
        rows = []
        for a in range(4):
            u = jnp.where(low16, whole[k][16 * a : 16 * a + 16], upper[at + 16 * a : at + 16 * a + 16])
            spot = 3 * (a % 2) + k
            piece = turn(mixed[a // 2], 0, EZ - spot - 64 * (a // 2))
            if a == 0:
                piece = piece + jnp.where(low16, turn(edge_down, 0, EZ - k), 0.0)
                u = u + jnp.where(low16, face_low[k], 0.0)
            if a == 3:
                piece = piece + jnp.where(low16, 0.0, turn(edge_up, 0, EZ - k))
                u = u + jnp.where(low16, 0.0, face_high[k])
            rows.append(u + jnp.where(row16r == EZ, piece, 0.0))
        wide_nodes[at : at + 64, :] = jnp.concatenate(rows, axis=0)
        below = pl.ds(at, 16, stride=4)
        above = pl.ds(at + 3, 16, stride=4)
        wide_nodes[below, :] += jnp.where(row16r == 0, turn(floor, 0, -k), 0.0)
        near_face = wide_nodes[at : at + 16, :]
        far_face = wide_nodes[at + 48 : at + 64, :]
        wide_nodes[at : at + 16, :] = near_face + jnp.where(low16, 0.0, turn(far_face, 0, 64))
        wide_nodes[at + 48 : at + 64, :] = far_face + jnp.where(low16, turn(near_face, 0, 64), 0.0)
        tops = wide_nodes[above, :]
        bottoms = wide_nodes[below, :]
        wide_nodes[above, :] = tops + jnp.where(row16r == EZ - 1, turn(bottoms, 0, -1), 0.0)
        wide_nodes[below, :] = bottoms + jnp.where(row16r == EZ, turn(tops, 0, 1), 0.0)
    relaxed = [wide_nodes[64 * k : 64 * k + 64, :] * wide_wall for k in comps]
    shaped = dot(whole_forth, jnp.concatenate(relaxed, axis=1))
    jacobian = [
        [shaped[128 * m : 128 * m + 128, 128 * c : 128 * c + 128] for m in comps] for c in comps
    ]
    for c in comps:
        jacobian[c][c] = jacobian[c][c] + 1.0
    fields = fluxes(jacobian, wide_weight)
    right = jnp.concatenate(
        [jnp.concatenate([fields[c][m] for c in comps], axis=1) for m in comps], axis=0
    )
    product = dot(whole_back, right)
    last = []
    for k in comps:
        v = product[:, 128 * k : 128 * k + 128]
        v = v + jnp.where((b_of == 0) & (q_of > 0), turn(v, -12, ROW), 0.0)
        v = v + jnp.where((c_of == 3) & (r_of < EZ), turn(v, 3, -1), 0.0)
        v = jnp.concatenate([v[0:48], v[48:64] + turn(v[0:16], 0, 64)], axis=0)
        last.append(moved[64 * k : 64 * k + 64] - relaxed[k] + mesh_step * v)
    last = jnp.concatenate(last, axis=0)
    mesh_velocity = new_velocity - last / step

    out_nodes[192:384, :] = mesh_velocity * owned
    mesh_back = back_to_lattice(out_nodes.at[pl.ds(192, 192)])
    for x in range(3):
        new_vel_out[:, plane * x : plane * (x + 1)] = new_back[8 * x : 8 * x + 3]
        mesh_vel_out[:, plane * x : plane * (x + 1)] = mesh_back[8 * x : 8 * x + 3]

    for copy_of, size in late:

        @pl.loop(1, size, unroll=True)
        def _(i, copy_of=copy_of):
            copy_of(i).wait_send()

    for copy, (dx, dz) in waits:

        @pl.when(inside(dx, dz))
        def _():
            copy.wait_send()


def hand_on(*refs):
    copies = [
        pltpu.make_async_copy(refs[k], refs[3 + k], refs[6].at[k]) for k in range(3)
    ]
    for copy in copies:
        copy.start()
    for copy in copies:
        copy.wait()


def body(n_dom, n_sub, displacement, velocity, energy, mass_density, live_mask, time_step):
    made_tables = tables()
    vmem = pl.BlockSpec(memory_space=pltpu.VMEM)
    anywhere = pl.BlockSpec(memory_space=pl.ANY)
    f32 = jnp.float32
    nodes = displacement.shape[1]
    wide_sum = n_dom * n_sub if n_dom * n_sub <= 64 else n_dom
    made = pl.pallas_call(
        functools.partial(kernel, n_dom, n_sub),
        out_shape=(
            pltpu.VMEM(displacement.shape, f32),
            pltpu.VMEM(energy.shape, f32),
            pltpu.VMEM(displacement.shape, f32),
        ),
        in_specs=[anywhere] * (6 + len(made_tables)),
        out_specs=(vmem, vmem, vmem),
        scratch_shapes=[
            pltpu.VMEM((8, nodes), f32),
            pltpu.VMEM((24, 1024), f32),
            pltpu.VMEM((512, 128), f32),
            pltpu.VMEM((2, 192, 128), f32),
            pltpu.VMEM((192, 128), f32),
            pltpu.VMEM((384, 128), f32),
            pltpu.VMEM((24, 1024), f32),
            pltpu.VMEM((128, 128), f32),
            pltpu.VMEM((32, 128), f32),
            pltpu.VMEM((8, 128), f32),
            pltpu.VMEM((3, 8, 128), f32),
            pltpu.VMEM((3, 2, 16, 128), f32),
            pltpu.VMEM((6, 16, 128), f32),
            pltpu.VMEM((2, 2, 3, 16, 128), f32),
            pltpu.VMEM((3, 2, 16, 128), f32),
            pltpu.VMEM((3, 4, 8, 128), f32),
            pltpu.VMEM((wide_sum, 1, 128), f32),
            pltpu.VMEM((n_sub, 1, 128), f32),
            pltpu.SemaphoreType.DMA((3, 8)),
            pltpu.SemaphoreType.DMA((3, 8)),
            pltpu.SemaphoreType.DMA((wide_sum,)),
            pltpu.SemaphoreType.DMA((wide_sum,)),
            pltpu.SemaphoreType.DMA((n_sub,)),
            pltpu.SemaphoreType.DMA((n_sub,)),
            pltpu.VMEM(displacement.shape, f32),
            pltpu.VMEM(velocity.shape, f32),
            pltpu.VMEM(energy.shape, f32),
            pltpu.VMEM(mass_density.shape[::-1], f32),
            pltpu.VMEM((1, live_mask.shape[0]), jnp.int32),
            pltpu.SMEM((1, 1), f32),
            *[pltpu.VMEM(t.shape, t.dtype) for t in made_tables],
            pltpu.SemaphoreType.DMA((6 + len(made_tables),)),
            pltpu.VMEM((192, 128), f32),
            pltpu.VMEM((96, 128), f32),
            pltpu.VMEM((3, 16, 128), f32),
            pltpu.VMEM((16, 128), f32),
            pltpu.VMEM((2, 24, 128), f32),
            pltpu.VMEM((96, 128), f32),
            pltpu.VMEM((2, 24, 128), f32),
            pltpu.VMEM((2, 16, 128), f32),
            pltpu.VMEM((2, 16, 128), f32),
            pltpu.VMEM((4, 16, 128), f32),
            pltpu.VMEM((192, 128), f32),
            pltpu.SemaphoreType.DMA((len(WIDE_STEPS),)),
            pltpu.SemaphoreType.DMA((len(WIDE_STEPS),)),
            pltpu.SemaphoreType.DMA((3,)),
            pltpu.SemaphoreType.DMA((3,)),
        ],
        compiler_params=pltpu.CompilerParams(collective_id=0, has_side_effects=True),
    )(
        displacement,
        velocity,
        energy,
        mass_density.T,
        live_mask.reshape(1, -1),
        time_step.reshape(1, 1),
        *[jnp.asarray(t) for t in made_tables],
    )
    return pl.pallas_call(
        hand_on,
        out_shape=[jax.ShapeDtypeStruct(m.shape, f32) for m in made],
        in_specs=[vmem] * 3,
        out_specs=[anywhere] * 3,
        scratch_shapes=[pltpu.SemaphoreType.DMA((3,))],
    )(*[pltpu.with_memory_space_constraint(m, pltpu.VMEM) for m in made])


def solution(mesh):
    split = ("dom", "sub")
    return jax.shard_map(
        functools.partial(body, mesh.shape["dom"], mesh.shape["sub"]),
        mesh=mesh,
        in_specs=(
            P(None, split),
            P(None, split),
            P(None, split),
            P(None, split),
            P(split),
            P(),
        ),
        out_specs=(P(None, split), P(None, split), P(None, split)),
        check_vma=False,
    )
```

```python
import functools
import math

import jax
import jax.numpy as jnp
import numpy as np
from jax import lax
from jax.experimental import pallas as pl
from jax.experimental.pallas import tpu as pltpu
from jax.sharding import PartitionSpec as P

EX = 1
EY = 8
EZ = 6
ELEMS = EX * EY * EZ
HALF = 64
ROW = 8

adiabatic = 5.0 / 3.0
viscosity = 0.3
mesh_step = 0.01
MESH = pl.DeviceIdType.MESH
STEPS = [(-1, -1), (-1, 1), (1, -1), (1, 1), (0, -1), (0, 1), (-1, 0), (1, 0)]
WIDE_STEPS = [(-2, -1), (-2, 1), (1, -1), (1, 1), (-1, 1), (-1, -1)]
WIDE_STEPS += [(0, -1), (0, 1), (-2, 0), (1, 0), (-1, 0)]


def one_dimension():
    root_term = math.sqrt(10.0 / 7.0)
    outer_root = math.sqrt(5.0 + 2.0 * root_term) / 3.0
    inner_root = math.sqrt(5.0 - 2.0 * root_term) / 3.0
    gauss_roots = np.array([-outer_root, -inner_root, 0.0, inner_root, outer_root])
    outer_weight = (322.0 - 13.0 * math.sqrt(70.0)) / 900.0
    middle_weight = (322.0 + 13.0 * math.sqrt(70.0)) / 900.0
    weights = (
        np.array([outer_weight, middle_weight, 128.0 / 225.0, middle_weight, outer_weight]) / 2.0
    )
    points = (1.0 + gauss_roots) / 2.0
    lobatto = [0.0, (1.0 - 1.0 / math.sqrt(5.0)) / 2.0, (1.0 + 1.0 / math.sqrt(5.0)) / 2.0, 1.0]
    values = np.ones((5, 4))
    slopes = np.zeros((5, 4))
    for node in range(4):
        for other in range(4):
            if other != node:
                values[:, node] *= (points - lobatto[other]) / (lobatto[node] - lobatto[other])
                term = np.ones(5) / (lobatto[node] - lobatto[other])
                for third in range(4):
                    if third != node and third != other:
                        term = term * (points - lobatto[third]) / (lobatto[node] - lobatto[third])
                slopes[:, node] += term
    bernstein = np.stack([(1.0 - points) ** 2, 2.0 * points * (1.0 - points), points**2], axis=1)
    return values, slopes, bernstein, weights


def outer_triple(first, second, third):
    product = np.einsum("ia,jb,kc->ijkabc", first, second, third)
    return product.reshape(125, -1)


def halves(table, rows):
    padded = np.concatenate([table, np.repeat(table[-1:], 3, axis=0)], axis=0)
    padded = np.pad(padded, [(0, 0), (0, rows - table.shape[1])])
    return np.concatenate([padded[:64], padded[64:]], axis=1)


def stacked_left(table):
    table = np.asarray(table, np.float32)
    high = table.astype(jnp.bfloat16)
    low = (table - high.astype(np.float32)).astype(jnp.bfloat16)
    return np.concatenate([low, high, high], axis=1)


@functools.lru_cache(None)
def tables():
    values, slopes, bernstein, weights = one_dimension()
    triples = [
        outer_triple(slopes, values, values),
        outer_triple(values, slopes, values),
        outer_triple(values, values, slopes),
    ]
    grad = np.concatenate([halves(t, 64) for t in triples], axis=0)
    whole = [np.concatenate([t, np.repeat(t[-1:], 3, axis=0)], axis=0) for t in triples]
    basis = halves(outer_triple(values, values, values), 64)
    energy = halves(outer_triple(bernstein, bernstein, bernstein), 32)
    weight = np.einsum("i,j,k->ijk", weights, weights, weights).reshape(125)
    weight = np.pad(weight, (0, 3))
    spread_weight = np.zeros((64, 128))
    spread_weight[:, :64] = weight[:64, None]
    spread_weight[:, 64:] = weight[64:, None]
    whole_weight = np.repeat(weight[:, None], 128, axis=1)
    planes_y, planes_z = 3 * EY + 1, 3 * EZ
    pick = np.zeros((planes_y * planes_z, 16 * HALF), np.float32)
    for b in range(4):
        for c in range(4):
            for q in range(EY):
                for r in range(EZ):
                    z = 3 * r + c - 1
                    if z >= 0:
                        lane = (4 * b + c) * HALF + q * ROW + r
                        pick[(3 * q + b) * planes_z + z, lane] = 1.0
    widen = np.zeros((128, 256), np.float32)
    for e in range(ELEMS):
        to = e // EZ * ROW + e % EZ
        widen[e, to] = 1.0
        widen[to, 128 + e] = 1.0
    return [
        pick.astype(jnp.bfloat16),
        stacked_left(grad),
        stacked_left(grad.T),
        stacked_left(basis),
        stacked_left(basis.T),
        stacked_left(energy),
        stacked_left(energy.T),
        stacked_left(np.concatenate(whole, axis=0)),
        stacked_left(np.concatenate(whole, axis=0).T),
        widen.astype(jnp.bfloat16),
        np.asarray(spread_weight, np.float32),
        np.asarray(whole_weight, np.float32),
    ]


def dot(table, right):
    high, low = split_two(right)
    stacked = jnp.concatenate([high, low, high], axis=0)
    return jnp.dot(table[...], stacked, preferred_element_type=jnp.float32)


def split_two(value):
    high = value.astype(jnp.bfloat16)
    return high, (value - high.astype(jnp.float32)).astype(jnp.bfloat16)


def cofactors(m):
    return [
        [
            m[(i + 1) % 3][(j + 1) % 3] * m[(i + 2) % 3][(j + 2) % 3]
            - m[(i + 1) % 3][(j + 2) % 3] * m[(i + 2) % 3][(j + 1) % 3]
            for j in range(3)
        ]
        for i in range(3)
    ]


def turn(value, rows, lanes):
    if rows:
        value = pltpu.roll(value, rows % value.shape[0], 0)
    if lanes % value.shape[1]:
        value = pltpu.roll(value, lanes % value.shape[1], 1)
    return value


def split_three(value):
    high = value.astype(jnp.bfloat16).astype(jnp.float32)
    rest = value - high
    middle = rest.astype(jnp.bfloat16).astype(jnp.float32)
    return jnp.concatenate([high, middle, rest - middle], axis=0).astype(jnp.bfloat16)


def kernel(
    n_dom,
    n_sub,
    disp_in_hbm,
    vel_in_hbm,
    energy_in_hbm,
    density_in_hbm,
    live_in_hbm,
    step_in_hbm,
    pick_hbm,
    grad_forth_hbm,
    grad_back_hbm,
    basis_forth_hbm,
    basis_back_hbm,
    energy_forth_hbm,
    energy_back_hbm,
    whole_forth_hbm,
    whole_back_hbm,
    widen_hbm,
    quad_weight_hbm,
    whole_weight_hbm,
    new_vel_out,
    rate_out,
    mesh_vel_out,
    flat,
    wide,
    first,
    local,
    state,
    out_nodes,
    out_wide,
    density_pad,
    energy_pad,
    live_own,
    live_got,
    packs,
    x_first,
    x_got,
    z_got,
    d_got,
    sum_dom,
    sum_sub,
    send_sems,
    recv_sems,
    dom_send,
    dom_recv,
    sub_send,
    sub_recv,
    disp_in,
    vel_in,
    energy_in,
    density_in,
    live_in,
    step_in,
    pick,
    grad_forth,
    grad_back,
    basis_forth,
    basis_back,
    energy_forth,
    energy_back,
    whole_forth,
    whole_back,
    widen,
    quad_weight,
    whole_weight,
    in_sems,
    ours,
    near,
    z_low,
    z_high,
    x_face,
    slab_got,
    x_face_got,
    layer_got,
    edge_got,
    floor_got,
    wide_nodes,
    wide_send,
    wide_recv,
    live_send,
    live_recv,
):
    dom = lax.axis_index("dom")
    sub = lax.axis_index("sub")
    plane = (3 * EY + 1) * 3 * EZ

    def inside(dx, dz):
        ok = None
        for step, place, size in ((dx, dom, n_dom), (dz, sub, n_sub)):
            if step:
                here = (place + step >= 0) if step < 0 else (place + step < size)
                ok = here if ok is None else jnp.logical_and(ok, here)
        return ok

    held = [
        (disp_in_hbm, disp_in),
        (vel_in_hbm, vel_in),
        (pick_hbm, pick),
        (step_in_hbm, step_in),
        (density_in_hbm, density_in),
        (energy_in_hbm, energy_in),
        (live_in_hbm, live_in),
        (grad_forth_hbm, grad_forth),
        (grad_back_hbm, grad_back),
        (basis_forth_hbm, basis_forth),
        (basis_back_hbm, basis_back),
        (energy_forth_hbm, energy_forth),
        (energy_back_hbm, energy_back),
        (whole_forth_hbm, whole_forth),
        (widen_hbm, widen),
        (quad_weight_hbm, quad_weight),
        (whole_weight_hbm, whole_weight),
        (whole_back_hbm, whole_back),
    ]
    loads = [
        pltpu.make_async_copy(source, target, in_sems.at[number])
        for number, (source, target) in enumerate(held)
    ]
    x_first[...] = jnp.zeros_like(x_first)
    x_got[...] = jnp.zeros_like(x_got)
    z_got[...] = jnp.zeros_like(z_got)
    d_got[...] = jnp.zeros_like(d_got)
    for got in (slab_got, x_face_got, layer_got, edge_got, floor_got, live_got):
        got[...] = jnp.zeros_like(got)

    barrier = pltpu.get_barrier_semaphore()
    one_phase = n_dom * n_sub <= 64
    if one_phase and n_sub <= 4:
        count = n_dom - 1
        for dz in (-1, 1):
            count = count + n_dom * inside(0, dz).astype(jnp.int32)
        for dz in (0, -1, 1):

            def greet(dz=dz):
                @pl.loop(0 if dz else 1, n_dom, unroll=True)
                def _(i):
                    pl.semaphore_signal(
                        barrier,
                        inc=1,
                        device_id=(lax.rem(dom + i, n_dom), sub + dz),
                        device_id_type=MESH,
                    )

            if dz:
                pl.when(inside(0, dz))(greet)
            else:
                greet()

    elif one_phase:
        devices = n_dom * n_sub
        count = devices - 1

        @pl.loop(1, devices, unroll=True)
        def _(i):
            t = lax.rem(dom * n_sub + sub + i, devices)
            pl.semaphore_signal(
                barrier,
                inc=1,
                device_id=(t // n_sub, lax.rem(t, n_sub)),
                device_id_type=MESH,
            )

    else:
        count = (n_dom - 1) + (n_sub - 1)
        for dx, dz in [(dx, dz) for dx in (-2, -1, 1, 2) for dz in (-1, 1)]:
            if dx and dz:
                ok = inside(dx, dz)
                count = count + ok.astype(jnp.int32)

                @pl.when(ok)
                def _():
                    pl.semaphore_signal(
                        barrier, inc=1, device_id=(dom + dx, sub + dz), device_id_type=MESH
                    )

        @pl.loop(1, n_dom)
        def _(i):
            pl.semaphore_signal(
                barrier, inc=1, device_id=(lax.rem(dom + i, n_dom), sub), device_id_type=MESH
            )

        @pl.loop(1, n_sub)
        def _(i):
            pl.semaphore_signal(
                barrier, inc=1, device_id=(dom, lax.rem(sub + i, n_sub)), device_id_type=MESH
            )

    for load in loads:
        load.start()

    first[...] = jnp.zeros_like(first)
    density_pad[...] = jnp.zeros_like(density_pad)
    energy_pad[...] = jnp.zeros_like(energy_pad)
    flat[...] = jnp.zeros_like(flat)
    out_wide[...] = jnp.zeros_like(out_wide)

    lane = lax.broadcasted_iota(jnp.int32, (64, 128), 1)
    row = lax.broadcasted_iota(jnp.int32, (64, 128), 0)
    q_of, r_of = (lane % HALF) // ROW, lane % ROW
    a_of, b_of, c_of = row // 16, (row // 4) % 4, row % 4
    low_half = lane < HALF
    valid = low_half & (r_of < EZ)
    triple = lambda x: jnp.concatenate([x, x, x], axis=0)
    y_up = triple((b_of == 3) & (q_of < EY - 1) & valid)
    y_down = triple((b_of == 0) & (q_of > 0) & valid)
    z_up = triple((c_of == 3) & (r_of < EZ - 1) & valid)
    z_down = triple((c_of == 0) & (r_of > 0) & valid)
    off_wall = jnp.where(
        valid
        & jnp.logical_or(a_of > 0, dom > 0)
        & jnp.logical_or(jnp.logical_or(c_of > 0, r_of > 0), sub > 0),
        1.0,
        0.0,
    )
    off_wall = triple(off_wall)
    owned = jnp.where(
        valid & (a_of > 0) & (c_of > 0) & ((b_of < 3) | (q_of == EY - 1)), 1.0, 0.0
    )
    owned = triple(owned)
    lane16, row16 = lane[:16], row[:16]
    r16 = jnp.where(lane16 < HALF, lane16 % ROW, ROW)

    for load in loads[:3]:
        load.wait()
    flat[0:3, :] = disp_in[...]
    flat[3:6, :] = vel_in[...]
    stacked = jnp.concatenate([flat[:, plane * x : plane * (x + 1)] for x in range(3)], axis=0)
    picked = jnp.dot(split_three(stacked), pick[...], preferred_element_type=jnp.float32)
    wide[...] = picked[0:24] + picked[24:48] + picked[48:72]
    for x in range(3):
        for pair in range(8):
            got = wide[8 * x : 8 * x + 8, 128 * pair : 128 * pair + 128]
            other = turn(got, 0, 64)
            at = 16 * (x + 1) + 2 * pair
            keep = lane[:8] < 64
            first[pl.ds(at, 8, stride=64), :] = jnp.where(keep, got, 0.0)
            first[pl.ds(at + 1, 8, stride=64), :] = jnp.where(keep, other, 0.0)

    pl.semaphore_wait(barrier, count)

    def faces(source, fields, place, shifts):
        packed = jnp.zeros((16, 128), jnp.float32)
        for k in range(fields):
            face = source[pl.ds(64 * k + place, 16, stride=4), :]
            if place == 3:
                packed = jnp.where(r16 == EZ - 1 - k, turn(face, 0, -k), packed)
            else:
                packed = jnp.where(r16 == k, turn(face, 0, k), packed)
        return packed

    waits = []

    def exchange_start(rnd, source, fields, x_target, ups, downs):
        if ups:
            packs[rnd, 1] = faces(source, fields, 3, None)
        if downs:
            packs[rnd, 0] = faces(source, fields, 0, None)
        started = []
        for number, (dx, dz) in enumerate(STEPS):
            lead = dz if dz else dx
            going = (dx, dz)
            up = all(s >= 0 for s in going)
            down = all(s <= 0 for s in going)
            if not ((ups and downs) or (ups and up) or (downs and down)):
                continue
            target = (dom + dx, sub + dz)
            jobs = []
            if dz == 0:
                base = 48 if dx > 0 else 0
                slot = 0 if dx > 0 else 1
                jobs.append(
                    (
                        source_blocks(source, fields, base),
                        x_target(slot),
                    )
                )
            elif dx == 0:
                side = 1 if dz > 0 else 0
                jobs.append((packs.at[rnd, side], z_got.at[rnd, 1 - side]))
            else:
                side = 1 if dz > 0 else 0
                half = 8 if dx > 0 else 0
                slot = (0 if dx > 0 else 1) + 2 * (1 - side)
                jobs.append((packs.at[rnd, side, pl.ds(half, 8)], d_got.at[rnd, slot]))
            src, dst = jobs[0]
            copy = pltpu.make_async_remote_copy(
                src_ref=src,
                dst_ref=dst,
                send_sem=send_sems.at[rnd, number],
                recv_sem=recv_sems.at[rnd, number],
                device_id=target,
                device_id_type=MESH,
            )

            @pl.when(inside(dx, dz))
            def _():
                copy.start()

            started.append((copy, (dx, dz)))
        return started

    def source_blocks(source, fields, base):
        blocks = source.reshape(source.shape[0] // 64, 64, 128)
        return blocks.at[pl.ds(0, fields), pl.ds(base, 16)]

    def exchange_wait(started):
        for copy, (dx, dz) in started:

            @pl.when(inside(-dx, -dz))
            def _():
                copy.wait_recv()

        waits.extend(started)

    def exchange_add(rnd, source, target, fields, x_from, ups, downs):
        if target is not source:
            target[...] = source[...]
        top = lax.broadcasted_iota(jnp.int32, (8, 128), 0) < 4
        for came, side, place in ((ups, 0, 0), (downs, 1, 3)):
            if not came:
                continue
            face = z_got[rnd, side]
            low = jnp.where(top, turn(d_got[rnd, 2 * side], 4, 0), 0.0)
            high = jnp.where(top, 0.0, turn(d_got[rnd, 2 * side + 1], 4, 0))
            face = face + jnp.concatenate([low, high], axis=0)
            for k in range(fields):
                if place == 0:
                    part = jnp.where(r16 == 0, turn(face, 0, k - (EZ - 1)), 0.0)
                else:
                    part = jnp.where(r16 == EZ - 1, turn(face, 0, EZ - 1 - k), 0.0)
                at = pl.ds(64 * k + place, 16, stride=4)
                target[at, :] = target[at, :] + part
        for k in range(fields):
            if ups:
                target[64 * k : 64 * k + 16, :] += x_from(0)[k]
            if downs:
                target[64 * k + 48 : 64 * k + 64, :] += x_from(1)[k]

    started = exchange_start(0, first, 6, lambda slot: x_first, True, False)

    for load in loads[3:]:
        load.wait()
    step = step_in[0, 0]
    for q in range(EY):
        density_pad[ROW * q : ROW * q + EZ, 0:125] = density_in[EZ * q : EZ * q + EZ, :]
    energy_pad[0:27, 0:ELEMS] = energy_in[...]
    energy_pad[27:28, 0:ELEMS] = live_in[...].astype(jnp.float32)

    def exact(value, table):
        rows = value.shape[0]
        out = jnp.dot(split_three(value), table, preferred_element_type=jnp.float32)
        return out[0:rows] + out[rows : 2 * rows] + out[2 * rows :]

    by_lane = exact(energy_pad[...], widen[:, 0:128])
    live = by_lane[27:28, :]
    live_own[...] = jnp.broadcast_to(live, (8, 128))
    live_copies = []
    for number, (dx, dz) in enumerate(((-1, 0), (0, -1), (-1, -1))):
        live_copy = pltpu.make_async_remote_copy(
            src_ref=live_own,
            dst_ref=live_got.at[number],
            send_sem=live_send.at[number],
            recv_sem=live_recv.at[number],
            device_id=(dom + dx, sub + dz),
            device_id_type=MESH,
        )
        live_copies.append((live_copy, (dx, dz)))

        @pl.when(inside(dx, dz))
        def _():
            live_copy.start()

    live = live + turn(live, 0, 64)
    by_point = jnp.transpose(density_pad[...])
    mass_density = by_point[0:64] + turn(by_point[64:128], 0, 64)
    weight = quad_weight[...]
    live_weight = weight * live
    mass_weight = live_weight * mass_density
    at_points = dot(energy_forth, jnp.concatenate([by_lane, turn(by_lane, 0, 64)], axis=0))

    def paired(v):
        return jnp.concatenate(
            [
                jnp.concatenate([v[64 * k : 64 * k + 64], turn(v[64 * k : 64 * k + 64], 0, 64)], 0)
                for k in range(v.shape[0] // 64)
            ],
            axis=1,
        )

    def folded(product):
        half = product.shape[0] // 2
        out = []
        for k in range(product.shape[1] // 128):
            part = product[:, 128 * k : 128 * k + 128]
            out.append(part[:half] + turn(part[half:], 0, 64))
        return out

    def gradient(v):
        shaped = dot(grad_forth, paired(v))
        return [
            [shaped[64 * m : 64 * m + 64, 128 * c : 128 * c + 128] for m in range(3)]
            for c in range(3)
        ]

    def jacobian_of(v):
        jacobian = gradient(v)
        for c in range(3):
            jacobian[c][c] = jacobian[c][c] + 1.0
        return jacobian

    def project(fields):
        right = jnp.concatenate(
            [jnp.concatenate([fields[c][m] for c in range(3)], axis=1) for m in range(3)], axis=0
        )
        return share(jnp.concatenate(folded(dot(grad_back, right)), axis=0))

    def share(v):
        v = v * jnp.where(triple(valid), 1.0, 0.0)
        v = v + jnp.where(y_up, turn(v, 12, -ROW), 0.0) + jnp.where(y_down, turn(v, -12, ROW), 0.0)
        v = v + jnp.where(z_up, turn(v, 3, -1), 0.0) + jnp.where(z_down, turn(v, -3, 1), 0.0)
        return v

    def interpolate(v):
        return dot(basis_forth, paired(v))

    def volume_of(jacobian, cofactor):
        return (
            jacobian[0][0] * cofactor[0][0]
            + jacobian[0][1] * cofactor[0][1]
            + jacobian[0][2] * cofactor[0][2]
        )

    def begin(rnd, v, ups=True, downs=True):
        source = local.at[rnd - 1]
        source[...] = v
        return exchange_start(rnd, source, 3, lambda slot: x_got.at[rnd - 1, slot], ups, downs)

    def finish(rnd, started, ups=True, downs=True):
        exchange_wait(started)
        source = local.at[rnd - 1]
        exchange_add(
            rnd, source, state, 3, lambda slot: x_got.at[rnd - 1, slot], ups, downs
        )
        return state[...] * off_wall

    exchange_wait(started)
    out_nodes[...] = first[0:384, :]
    exchange_add(0, out_nodes, out_nodes, 6, lambda slot: x_first, True, False)
    displacement = out_nodes[0:192, :]
    velocity = out_nodes[192:384, :]

    jacobian = jacobian_of(displacement)
    velocity_grad = gradient(velocity)
    cofactor = cofactors(jacobian)
    volume = volume_of(jacobian, cofactor)
    inverse = 1.0 / volume
    density = mass_density * inverse
    pressure = (adiabatic - 1.0) * density * at_points
    spatial = [
        [
            (
                velocity_grad[c][0] * cofactor[m][0]
                + velocity_grad[c][1] * cofactor[m][1]
                + velocity_grad[c][2] * cofactor[m][2]
            )
            * inverse
            for m in range(3)
        ]
        for c in range(3)
    ]
    viscous = viscosity * density
    stress = [[None] * 3 for _ in range(3)]
    for c in range(3):
        for m in range(c, 3):
            value = viscous * (spatial[c][m] + spatial[m][c])
            stress[c][m] = stress[m][c] = value - pressure if c == m else value
    flux = [
        [
            -live_weight
            * (
                stress[c][0] * cofactor[0][m]
                + stress[c][1] * cofactor[1][m]
                + stress[c][2] * cofactor[2][m]
            )
            for m in range(3)
        ]
        for c in range(3)
    ]
    started = begin(1, project(flux))
    power = stress[0][0] * spatial[0][0]
    for c in range(3):
        for m in range(3):
            if c + m > 0:
                power = power + stress[c][m] * spatial[c][m]
    power = live_weight * volume * power
    sums = folded(
        dot(energy_back, jnp.concatenate([power, weight * mass_density], axis=1))
    )
    rates = jnp.where(valid[:32], sums[0] / jnp.where(valid[:32], sums[1], 1.0), 0.0)
    rate_out[...] = exact(rates, widen[:, 128:256])[0:27, 0:ELEMS]
    force = finish(1, started)

    wide_mass = jnp.concatenate([mass_weight] * 3, axis=1)
    values = interpolate(force)
    weighted = wide_mass * values
    image = share(jnp.concatenate(folded(dot(basis_back, weighted)), axis=0))
    started = begin(2, image)

    def total(x):
        return jnp.sum(jnp.sum(x, axis=0, keepdims=True), axis=1, keepdims=True)

    norm_part = total(force * force * owned)
    product_part = total(weighted * values)
    image = finish(2, started)
    image_norm_part = total(image * image * owned)
    values = interpolate(image)
    image_product_part = total(wide_mass * values * values)

    lane1 = lane[0:1]
    packed = jnp.where(
        lane1 == 0,
        norm_part,
        jnp.where(
            lane1 == 1,
            product_part,
            jnp.where(lane1 == 2, image_norm_part, image_product_part),
        ),
    )

    late = []

    def all_sum(value, slots, targets, sends, recvs, cover=None):
        slots[0] = value

        def copy_of(source, target, device):
            return pltpu.make_async_remote_copy(
                src_ref=source,
                dst_ref=target,
                send_sem=sends.at[0],
                recv_sem=recvs.at[0],
                device_id=device,
                device_id_type=MESH,
            )

        for number, device in targets:
            copy_of(slots.at[0], slots.at[number], device).start()

        out = cover() if cover else None

        others = slots.at[pl.ds(1, len(targets))]
        whole_sum = copy_of(others, others, targets[0][1])
        whole_sum.wait_recv()
        late.append(whole_sum)
        return jnp.sum(slots[...], axis=0), out

    doms = [lax.rem(dom + i, n_dom) for i in range(n_dom)]
    subs = [lax.rem(sub + i, n_sub) for i in range(n_sub)]

    def ahead():
        return [gradient(v) for v in (displacement + step * velocity, force, image)]

    if one_phase:
        targets = [
            (j * n_dom + i, (doms[i], subs[j]))
            for j in [*range(1, n_sub), 0]
            for i in range(n_dom)
            if i + j > 0
        ]
        packed, slopes = all_sum(packed, sum_dom, targets, dom_send, dom_recv, ahead)
    else:
        targets = [(i, (doms[i], sub)) for i in range(1, n_dom)]
        packed, slopes = all_sum(packed, sum_dom, targets, dom_send, dom_recv, ahead)
        targets = [(j, (dom, subs[j])) for j in range(1, n_sub)]
        packed, _ = all_sum(packed, sum_sub, targets, sub_send, sub_recv)
    rr, rw, ww, wmw = (
        jnp.sum(jnp.where(lane1 == k, packed, 0.0), axis=1, keepdims=True) for k in range(4)
    )
    first_length = rr / rw
    next_norm = first_length * (first_length * ww) - rr
    conjugacy = next_norm / rr
    residual_image = rw - first_length * ww
    residual_product = rw - 2.0 * first_length * ww + first_length * first_length * wmw
    bend = residual_product + 2.0 * conjugacy * residual_image + conjugacy * conjugacy * rw
    second_length = next_norm / bend
    on_force = first_length + second_length * (1.0 + conjugacy)
    on_image = second_length * first_length
    new_velocity = velocity + step * (on_force * force - on_image * image)
    moved = displacement + step * new_velocity

    def fluxes(jacobian, weights):
        cofactor = cofactors(jacobian)
        volume = volume_of(jacobian, cofactor)
        norm_sq = None
        for c in range(3):
            for m in range(3):
                square = jacobian[c][m] * jacobian[c][m]
                norm_sq = square if norm_sq is None else norm_sq + square
        scale = weights * jnp.exp(jnp.log(volume) * (-2.0 / 3.0))
        along = scale * (2.0 / 3.0)
        across = scale * (2.0 / 9.0) * (norm_sq / volume)
        return [
            [along * jacobian[c][m] - across * cofactor[c][m] for m in range(3)]
            for c in range(3)
        ]

    def back_to_lattice(nodes):
        for x in range(3):
            for pair in range(8):
                at = 16 * (x + 1) + 2 * pair
                even = nodes[pl.ds(at, 3, stride=64), :]
                odd = nodes[pl.ds(at + 1, 3, stride=64), :]
                out_wide[8 * x : 8 * x + 3, 128 * pair : 128 * pair + 128] = even + turn(odd, 0, 64)
        back = lax.dot_general(
            split_three(out_wide[...]), pick[...], (((1,), (1,)), ((), ())), preferred_element_type=jnp.float32
        )
        return back[0:24] + back[24:48] + back[48:72]

    by_force, by_image = step * step * on_force, step * step * on_image
    jacobian = [
        [
            slopes[0][c][m] + by_force * slopes[1][c][m] - by_image * slopes[2][c][m]
            for m in range(3)
        ]
        for c in range(3)
    ]
    for c in range(3):
        jacobian[c][c] = jacobian[c][c] + 1.0
    shift = -mesh_step * project(fluxes(jacobian, live_weight))

    comps = range(3)
    a_first, c_first = a_of == 0, c_of == 0
    part = [shift[64 * k : 64 * k + 64] for k in comps]
    whole = [moved[64 * k : 64 * k + 64] + part[k] for k in comps]
    ours[...] = shift
    slab = jnp.concatenate([jnp.where(a_first, part[k], whole[k]) for k in comps], axis=0)
    near[...] = slab[0:96] + turn(slab[96:192], 0, 64)
    r64 = jnp.where(low_half, r_of, ROW)

    def lay(fields, place):
        out = None
        for k in comps:
            at = r64[: fields[k].shape[0]]
            piece = jnp.where(at == k, turn(fields[k], 0, k - place), 0.0)
            out = piece if out is None else out + piece
        return out + turn(out, 0, 64)

    layer = [jnp.where(c_first, part[k], whole[k]) for k in comps]
    right_half = jnp.logical_not(low_half)
    r_here = r_of[:16]

    def lay_group(fields, a):
        out = None
        half = low_half[:16] if a < 2 else right_half[:16]
        for k in comps:
            spot = 3 * (a % 2) + k
            piece = jnp.where(
                half & (r_here == spot), turn(fields[k], 0, 64 * (a // 2) + spot), 0.0
            )
            out = piece if out is None else out + piece
        return out

    groups = [lay_group([f[16 * a : 16 * a + 16] for f in layer], a) for a in range(4)]
    upper_groups = groups[1] + groups[2] + groups[3]
    face_part = lay_group([part[k][0:16] for k in comps], 0)
    z_low[0] = turn(face_part + upper_groups, 0, 64)
    z_low[1] = groups[0] + upper_groups
    z_low[2] = lay([part[k][48:64] for k in comps], 0)
    z_high[...] = lay([ours[pl.ds(64 * k + 3, 16, stride=4), :] for k in comps], EZ - 1)
    x_face[0, 0:16] = part[1][0:16] + turn(part[0][0:16], 0, 64)
    x_face[0, 16:24] = part[2][8:16] + turn(part[2][0:8], 0, 64)
    x_face[1, 0:16] = part[0][48:64] + turn(part[1][48:64], 0, 64)
    x_face[1, 16:24] = part[2][48:56] + turn(part[2][56:64], 0, 64)

    routes = {
        (-1, 0): (near, slab_got),
        (-2, 0): (x_face.at[0], x_face_got.at[0]),
        (1, 0): (x_face.at[1], x_face_got.at[1]),
        (0, -1): (z_low.at[1], layer_got.at[0]),
        (-1, -1): (z_low.at[0], layer_got.at[1]),
        (-2, -1): (z_low.at[0], edge_got.at[0]),
        (1, -1): (z_low.at[2], edge_got.at[1]),
        (0, 1): (z_high, floor_got.at[0]),
        (-1, 1): (z_high, floor_got.at[1]),
        (-2, 1): (z_high.at[pl.ds(0, 8)], floor_got.at[2, pl.ds(0, 8)]),
        (1, 1): (z_high.at[pl.ds(8, 8)], floor_got.at[3, pl.ds(8, 8)]),
    }
    started = []
    for number, (dx, dz) in enumerate(WIDE_STEPS):
        source, target = routes[dx, dz]
        wide_copy = pltpu.make_async_remote_copy(
            src_ref=source,
            dst_ref=target,
            send_sem=wide_send.at[number],
            recv_sem=wide_recv.at[number],
            device_id=(dom + dx, sub + dz),
            device_id_type=MESH,
        )

        @pl.when(inside(dx, dz))
        def _():
            wide_copy.start()

        started.append((wide_copy, (dx, dz)))
    exchange_wait(live_copies)
    out_nodes[0:192, :] = new_velocity * owned
    new_back = back_to_lattice(out_nodes)
    one_low, one_r = low_half[0:1], r_of[0:1]
    live_up = turn(live_got[0, 0:1, :], 0, 64)
    live_layer = live_got[1, 0:1, :] + turn(live_got[2, 0:1, :], 0, 64)
    live_wide = live_own[0:1, :] + live_up + jnp.where(one_r == EZ, turn(live_layer, 0, EZ), 0.0)
    wide_weight = whole_weight[...] * live_wide
    wide_wall = jnp.where(
        jnp.logical_or(right_half, jnp.logical_or(a_of > 0, dom > 0))
        & jnp.logical_or(jnp.logical_or(c_of > 0, r_of > 0), sub > 0),
        1.0,
        0.0,
    )
    low16, row16r = low_half[:16], r_of[:16]

    for whole_sum in late:
        whole_sum.wait_send()
    for copy, (dx, dz) in waits + started:

        @pl.when(inside(dx, dz))
        def _():
            copy.wait_send()

    exchange_wait(started)
    upper = slab_got[...]
    upper = jnp.concatenate([turn(upper, 0, 64), upper], axis=0)
    first_got, second_got = layer_got[0], layer_got[1]
    mixed = (
        jnp.where(low16, first_got, second_got),
        jnp.where(low16, second_got, first_got),
    )
    right16 = right_half[:16]
    edge_up = jnp.where(right16, edge_got[0], 0.0)
    edge_down = jnp.where(low16, edge_got[1], 0.0)
    floor = jnp.where(low16, floor_got[0], floor_got[1])
    floor = floor + jnp.where(right16 & (row16 >= 12), turn(floor_got[2], 12, 0), 0.0)
    floor = floor + jnp.where(low16 & (row16 < 4), turn(floor_got[3], 4, 0), 0.0)
    face_low = [
        x_face_got[1, 0:16],
        turn(x_face_got[1, 0:16], 0, 64),
        jnp.concatenate([x_face_got[1, 16:24], turn(x_face_got[1, 16:24], 0, 64)], axis=0),
    ]
    face_high = [
        x_face_got[0, 0:16],
        turn(x_face_got[0, 0:16], 0, 64),
        jnp.concatenate([x_face_got[0, 16:24], turn(x_face_got[0, 16:24], 0, 64)], axis=0),
    ]
    for k in comps:
        at = 64 * k
        rows = []
        for a in range(4):
            u = jnp.where(low16, whole[k][16 * a : 16 * a + 16], upper[at + 16 * a : at + 16 * a + 16])
            spot = 3 * (a % 2) + k
            piece = turn(mixed[a // 2], 0, EZ - spot - 64 * (a // 2))
            if a == 0:
                piece = piece + jnp.where(low16, turn(edge_down, 0, EZ - k), 0.0)
                u = u + jnp.where(low16, face_low[k], 0.0)
            if a == 3:
                piece = piece + jnp.where(low16, 0.0, turn(edge_up, 0, EZ - k))
                u = u + jnp.where(low16, 0.0, face_high[k])
            rows.append(u + jnp.where(row16r == EZ, piece, 0.0))
        wide_nodes[at : at + 64, :] = jnp.concatenate(rows, axis=0)
        below = pl.ds(at, 16, stride=4)
        above = pl.ds(at + 3, 16, stride=4)
        wide_nodes[below, :] += jnp.where(row16r == 0, turn(floor, 0, -k), 0.0)
        near_face = wide_nodes[at : at + 16, :]
        far_face = wide_nodes[at + 48 : at + 64, :]
        wide_nodes[at : at + 16, :] = near_face + jnp.where(low16, 0.0, turn(far_face, 0, 64))
        wide_nodes[at + 48 : at + 64, :] = far_face + jnp.where(low16, turn(near_face, 0, 64), 0.0)
        tops = wide_nodes[above, :]
        bottoms = wide_nodes[below, :]
        wide_nodes[above, :] = tops + jnp.where(row16r == EZ - 1, turn(bottoms, 0, -1), 0.0)
        wide_nodes[below, :] = bottoms + jnp.where(row16r == EZ, turn(tops, 0, 1), 0.0)
    relaxed = [wide_nodes[64 * k : 64 * k + 64, :] * wide_wall for k in comps]
    shaped = dot(whole_forth, jnp.concatenate(relaxed, axis=1))
    jacobian = [
        [shaped[128 * m : 128 * m + 128, 128 * c : 128 * c + 128] for m in comps] for c in comps
    ]
    for c in comps:
        jacobian[c][c] = jacobian[c][c] + 1.0
    fields = fluxes(jacobian, wide_weight)
    right = jnp.concatenate(
        [jnp.concatenate([fields[c][m] for c in comps], axis=1) for m in comps], axis=0
    )
    product = dot(whole_back, right)
    last = []
    for k in comps:
        v = product[:, 128 * k : 128 * k + 128]
        v = v + jnp.where((b_of == 0) & (q_of > 0), turn(v, -12, ROW), 0.0)
        v = v + jnp.where((c_of == 3) & (r_of < EZ), turn(v, 3, -1), 0.0)
        v = jnp.concatenate([v[0:48], v[48:64] + turn(v[0:16], 0, 64)], axis=0)
        last.append(moved[64 * k : 64 * k + 64] - relaxed[k] + mesh_step * v)
    last = jnp.concatenate(last, axis=0)
    mesh_velocity = new_velocity - last / step

    out_nodes[192:384, :] = mesh_velocity * owned
    mesh_back = back_to_lattice(out_nodes.at[pl.ds(192, 192)])
    for x in range(3):
        new_vel_out[:, plane * x : plane * (x + 1)] = new_back[8 * x : 8 * x + 3]
        mesh_vel_out[:, plane * x : plane * (x + 1)] = mesh_back[8 * x : 8 * x + 3]


def hand_on(*refs):
    copies = [
        pltpu.make_async_copy(refs[k], refs[3 + k], refs[6].at[k]) for k in range(3)
    ]
    for copy in copies:
        copy.start()
    for copy in copies:
        copy.wait()


def body(n_dom, n_sub, displacement, velocity, energy, mass_density, live_mask, time_step):
    made_tables = tables()
    vmem = pl.BlockSpec(memory_space=pltpu.VMEM)
    anywhere = pl.BlockSpec(memory_space=pl.ANY)
    f32 = jnp.float32
    nodes = displacement.shape[1]
    wide_sum = n_dom * n_sub if n_dom * n_sub <= 64 else n_dom
    made = pl.pallas_call(
        functools.partial(kernel, n_dom, n_sub),
        out_shape=(
            pltpu.VMEM(displacement.shape, f32),
            pltpu.VMEM(energy.shape, f32),
            pltpu.VMEM(displacement.shape, f32),
        ),
        in_specs=[anywhere] * (6 + len(made_tables)),
        out_specs=(vmem, vmem, vmem),
        scratch_shapes=[
            pltpu.VMEM((8, nodes), f32),
            pltpu.VMEM((24, 1024), f32),
            pltpu.VMEM((512, 128), f32),
            pltpu.VMEM((2, 192, 128), f32),
            pltpu.VMEM((192, 128), f32),
            pltpu.VMEM((384, 128), f32),
            pltpu.VMEM((24, 1024), f32),
            pltpu.VMEM((128, 128), f32),
            pltpu.VMEM((32, 128), f32),
            pltpu.VMEM((8, 128), f32),
            pltpu.VMEM((3, 8, 128), f32),
            pltpu.VMEM((3, 2, 16, 128), f32),
            pltpu.VMEM((6, 16, 128), f32),
            pltpu.VMEM((2, 2, 3, 16, 128), f32),
            pltpu.VMEM((3, 2, 16, 128), f32),
            pltpu.VMEM((3, 4, 8, 128), f32),
            pltpu.VMEM((wide_sum, 1, 128), f32),
            pltpu.VMEM((n_sub, 1, 128), f32),
            pltpu.SemaphoreType.DMA((3, 8)),
            pltpu.SemaphoreType.DMA((3, 8)),
            pltpu.SemaphoreType.DMA((wide_sum,)),
            pltpu.SemaphoreType.DMA((wide_sum,)),
            pltpu.SemaphoreType.DMA((n_sub,)),
            pltpu.SemaphoreType.DMA((n_sub,)),
            pltpu.VMEM(displacement.shape, f32),
            pltpu.VMEM(velocity.shape, f32),
            pltpu.VMEM(energy.shape, f32),
            pltpu.VMEM(mass_density.shape[::-1], f32),
            pltpu.VMEM((1, live_mask.shape[0]), jnp.int32),
            pltpu.SMEM((1, 1), f32),
            *[pltpu.VMEM(t.shape, t.dtype) for t in made_tables],
            pltpu.SemaphoreType.DMA((6 + len(made_tables),)),
            pltpu.VMEM((192, 128), f32),
            pltpu.VMEM((96, 128), f32),
            pltpu.VMEM((3, 16, 128), f32),
            pltpu.VMEM((16, 128), f32),
            pltpu.VMEM((2, 24, 128), f32),
            pltpu.VMEM((96, 128), f32),
            pltpu.VMEM((2, 24, 128), f32),
            pltpu.VMEM((2, 16, 128), f32),
            pltpu.VMEM((2, 16, 128), f32),
            pltpu.VMEM((4, 16, 128), f32),
            pltpu.VMEM((192, 128), f32),
            pltpu.SemaphoreType.DMA((len(WIDE_STEPS),)),
            pltpu.SemaphoreType.DMA((len(WIDE_STEPS),)),
            pltpu.SemaphoreType.DMA((3,)),
            pltpu.SemaphoreType.DMA((3,)),
        ],
        compiler_params=pltpu.CompilerParams(collective_id=0, has_side_effects=True),
    )(
        displacement,
        velocity,
        energy,
        mass_density.T,
        live_mask.reshape(1, -1),
        time_step.reshape(1, 1),
        *[jnp.asarray(t) for t in made_tables],
    )
    return pl.pallas_call(
        hand_on,
        out_shape=[jax.ShapeDtypeStruct(m.shape, f32) for m in made],
        in_specs=[vmem] * 3,
        out_specs=[anywhere] * 3,
        scratch_shapes=[pltpu.SemaphoreType.DMA((3,))],
    )(*[pltpu.with_memory_space_constraint(m, pltpu.VMEM) for m in made])


def solution(mesh):
    split = ("dom", "sub")
    return jax.shard_map(
        functools.partial(body, mesh.shape["dom"], mesh.shape["sub"]),
        mesh=mesh,
        in_specs=(
            P(None, split),
            P(None, split),
            P(None, split),
            P(None, split),
            P(split),
            P(),
        ),
        out_specs=(P(None, split), P(None, split), P(None, split)),
        check_vma=False,
    )
```

```python
import functools
import math

import jax
import jax.numpy as jnp
import numpy as np
from jax import lax
from jax.experimental import pallas as pl
from jax.experimental.pallas import tpu as pltpu
from jax.sharding import PartitionSpec as P

EX = 1
EY = 8
EZ = 6
ELEMS = EX * EY * EZ
HALF = 64
ROW = 8

adiabatic = 5.0 / 3.0
viscosity = 0.3
mesh_step = 0.01
MESH = pl.DeviceIdType.MESH
STEPS = [(-1, -1), (-1, 1), (1, -1), (1, 1), (0, -1), (0, 1), (-1, 0), (1, 0)]
WIDE_STEPS = [(-2, -1), (-2, 1), (1, -1), (1, 1), (-1, 1), (-1, -1)]
WIDE_STEPS += [(0, -1), (0, 1), (-2, 0), (1, 0), (-1, 0)]


def one_dimension():
    root_term = math.sqrt(10.0 / 7.0)
    outer_root = math.sqrt(5.0 + 2.0 * root_term) / 3.0
    inner_root = math.sqrt(5.0 - 2.0 * root_term) / 3.0
    gauss_roots = np.array([-outer_root, -inner_root, 0.0, inner_root, outer_root])
    outer_weight = (322.0 - 13.0 * math.sqrt(70.0)) / 900.0
    middle_weight = (322.0 + 13.0 * math.sqrt(70.0)) / 900.0
    weights = (
        np.array([outer_weight, middle_weight, 128.0 / 225.0, middle_weight, outer_weight]) / 2.0
    )
    points = (1.0 + gauss_roots) / 2.0
    lobatto = [0.0, (1.0 - 1.0 / math.sqrt(5.0)) / 2.0, (1.0 + 1.0 / math.sqrt(5.0)) / 2.0, 1.0]
    values = np.ones((5, 4))
    slopes = np.zeros((5, 4))
    for node in range(4):
        for other in range(4):
            if other != node:
                values[:, node] *= (points - lobatto[other]) / (lobatto[node] - lobatto[other])
                term = np.ones(5) / (lobatto[node] - lobatto[other])
                for third in range(4):
                    if third != node and third != other:
                        term = term * (points - lobatto[third]) / (lobatto[node] - lobatto[third])
                slopes[:, node] += term
    bernstein = np.stack([(1.0 - points) ** 2, 2.0 * points * (1.0 - points), points**2], axis=1)
    return values, slopes, bernstein, weights


def outer_triple(first, second, third):
    product = np.einsum("ia,jb,kc->ijkabc", first, second, third)
    return product.reshape(125, -1)


def halves(table, rows):
    padded = np.concatenate([table, np.repeat(table[-1:], 3, axis=0)], axis=0)
    padded = np.pad(padded, [(0, 0), (0, rows - table.shape[1])])
    return np.concatenate([padded[:64], padded[64:]], axis=1)


def stacked_left(table):
    table = np.asarray(table, np.float32)
    high = table.astype(jnp.bfloat16)
    low = (table - high.astype(np.float32)).astype(jnp.bfloat16)
    return np.concatenate([low, high, high], axis=1)


@functools.lru_cache(None)
def tables():
    values, slopes, bernstein, weights = one_dimension()
    triples = [
        outer_triple(slopes, values, values),
        outer_triple(values, slopes, values),
        outer_triple(values, values, slopes),
    ]
    grad = np.concatenate([halves(t, 64) for t in triples], axis=0)
    whole = [np.concatenate([t, np.repeat(t[-1:], 3, axis=0)], axis=0) for t in triples]
    basis = outer_triple(values, values, values)
    basis = np.concatenate([basis, np.repeat(basis[-1:], 3, axis=0)], axis=0)
    energy = halves(outer_triple(bernstein, bernstein, bernstein), 32)
    weight = np.einsum("i,j,k->ijk", weights, weights, weights).reshape(125)
    weight = np.pad(weight, (0, 3))
    spread_weight = np.zeros((64, 128))
    spread_weight[:, :64] = weight[:64, None]
    spread_weight[:, 64:] = weight[64:, None]
    whole_weight = np.repeat(weight[:, None], 128, axis=1)
    planes_y, planes_z = 3 * EY + 1, 3 * EZ
    pick = np.zeros((planes_y * planes_z, 16 * HALF), np.float32)
    for b in range(4):
        for c in range(4):
            for q in range(EY):
                for r in range(EZ):
                    z = 3 * r + c - 1
                    if z >= 0:
                        lane = (4 * b + c) * HALF + q * ROW + r
                        pick[(3 * q + b) * planes_z + z, lane] = 1.0
    widen = np.zeros((128, 256), np.float32)
    for e in range(ELEMS):
        to = e // EZ * ROW + e % EZ
        widen[e, to] = 1.0
        widen[to, 128 + e] = 1.0
    return [
        pick.astype(jnp.bfloat16),
        stacked_left(grad),
        stacked_left(grad.T),
        stacked_left(basis),
        stacked_left(basis.T),
        stacked_left(energy),
        stacked_left(energy.T),
        stacked_left(np.concatenate(whole, axis=0)),
        stacked_left(np.concatenate(whole, axis=0).T),
        widen.astype(jnp.bfloat16),
        np.asarray(spread_weight, np.float32),
        np.asarray(whole_weight, np.float32),
    ]


def dot(table, right):
    high, low = split_two(right)
    stacked = jnp.concatenate([high, low, high], axis=0)
    return jnp.dot(table[...], stacked, preferred_element_type=jnp.float32)


def split_two(value):
    high = value.astype(jnp.bfloat16)
    return high, (value - high.astype(jnp.float32)).astype(jnp.bfloat16)


def cofactors(m):
    return [
        [
            m[(i + 1) % 3][(j + 1) % 3] * m[(i + 2) % 3][(j + 2) % 3]
            - m[(i + 1) % 3][(j + 2) % 3] * m[(i + 2) % 3][(j + 1) % 3]
            for j in range(3)
        ]
        for i in range(3)
    ]


def turn(value, rows, lanes):
    if rows:
        value = pltpu.roll(value, rows % value.shape[0], 0)
    if lanes % value.shape[1]:
        value = pltpu.roll(value, lanes % value.shape[1], 1)
    return value


def split_three(value):
    high = value.astype(jnp.bfloat16).astype(jnp.float32)
    rest = value - high
    middle = rest.astype(jnp.bfloat16).astype(jnp.float32)
    return jnp.concatenate([high, middle, rest - middle], axis=0).astype(jnp.bfloat16)


def kernel(
    n_dom,
    n_sub,
    disp_in_hbm,
    vel_in_hbm,
    energy_in_hbm,
    density_in_hbm,
    live_in_hbm,
    step_in_hbm,
    pick_hbm,
    grad_forth_hbm,
    grad_back_hbm,
    basis_forth_hbm,
    basis_back_hbm,
    energy_forth_hbm,
    energy_back_hbm,
    whole_forth_hbm,
    whole_back_hbm,
    widen_hbm,
    quad_weight_hbm,
    whole_weight_hbm,
    new_vel_out,
    rate_out,
    mesh_vel_out,
    flat,
    wide,
    first,
    local,
    state,
    out_nodes,
    out_wide,
    density_pad,
    energy_pad,
    live_own,
    live_got,
    packs,
    x_first,
    x_got,
    z_got,
    d_got,
    sum_dom,
    sum_sub,
    send_sems,
    recv_sems,
    dom_send,
    dom_recv,
    sub_send,
    sub_recv,
    disp_in,
    vel_in,
    energy_in,
    density_in,
    live_in,
    step_in,
    pick,
    grad_forth,
    grad_back,
    basis_forth,
    basis_back,
    energy_forth,
    energy_back,
    whole_forth,
    whole_back,
    widen,
    quad_weight,
    whole_weight,
    in_sems,
    ours,
    near,
    z_low,
    z_high,
    x_face,
    slab_got,
    x_face_got,
    layer_got,
    edge_got,
    floor_got,
    wide_nodes,
    wide_send,
    wide_recv,
    live_send,
    live_recv,
):
    dom = lax.axis_index("dom")
    sub = lax.axis_index("sub")
    plane = (3 * EY + 1) * 3 * EZ

    def inside(dx, dz):
        ok = None
        for step, place, size in ((dx, dom, n_dom), (dz, sub, n_sub)):
            if step:
                here = (place + step >= 0) if step < 0 else (place + step < size)
                ok = here if ok is None else jnp.logical_and(ok, here)
        return ok

    held = [
        (disp_in_hbm, disp_in),
        (vel_in_hbm, vel_in),
        (pick_hbm, pick),
        (step_in_hbm, step_in),
        (density_in_hbm, density_in),
        (energy_in_hbm, energy_in),
        (live_in_hbm, live_in),
        (grad_forth_hbm, grad_forth),
        (grad_back_hbm, grad_back),
        (basis_forth_hbm, basis_forth),
        (basis_back_hbm, basis_back),
        (energy_forth_hbm, energy_forth),
        (energy_back_hbm, energy_back),
        (whole_forth_hbm, whole_forth),
        (widen_hbm, widen),
        (quad_weight_hbm, quad_weight),
        (whole_weight_hbm, whole_weight),
        (whole_back_hbm, whole_back),
    ]
    loads = [
        pltpu.make_async_copy(source, target, in_sems.at[number])
        for number, (source, target) in enumerate(held)
    ]
    x_first[...] = jnp.zeros_like(x_first)
    x_got[...] = jnp.zeros_like(x_got)
    z_got[...] = jnp.zeros_like(z_got)
    d_got[...] = jnp.zeros_like(d_got)
    for got in (slab_got, x_face_got, layer_got, edge_got, floor_got, live_got):
        got[...] = jnp.zeros_like(got)

    barrier = pltpu.get_barrier_semaphore()
    one_phase = n_dom * n_sub <= 64
    if one_phase and n_sub <= 4:
        count = n_dom - 1
        for dz in (-1, 1):
            count = count + n_dom * inside(0, dz).astype(jnp.int32)
        for dz in (0, -1, 1):

            def greet(dz=dz):
                @pl.loop(0 if dz else 1, n_dom, unroll=True)
                def _(i):
                    pl.semaphore_signal(
                        barrier,
                        inc=1,
                        device_id=(lax.rem(dom + i, n_dom), sub + dz),
                        device_id_type=MESH,
                    )

            if dz:
                pl.when(inside(0, dz))(greet)
            else:
                greet()

    elif one_phase:
        devices = n_dom * n_sub
        count = devices - 1

        @pl.loop(1, devices, unroll=True)
        def _(i):
            t = lax.rem(dom * n_sub + sub + i, devices)
            pl.semaphore_signal(
                barrier,
                inc=1,
                device_id=(t // n_sub, lax.rem(t, n_sub)),
                device_id_type=MESH,
            )

    else:
        count = (n_dom - 1) + (n_sub - 1)
        for dx, dz in [(dx, dz) for dx in (-2, -1, 1, 2) for dz in (-1, 1)]:
            if dx and dz:
                ok = inside(dx, dz)
                count = count + ok.astype(jnp.int32)

                @pl.when(ok)
                def _():
                    pl.semaphore_signal(
                        barrier, inc=1, device_id=(dom + dx, sub + dz), device_id_type=MESH
                    )

        @pl.loop(1, n_dom)
        def _(i):
            pl.semaphore_signal(
                barrier, inc=1, device_id=(lax.rem(dom + i, n_dom), sub), device_id_type=MESH
            )

        @pl.loop(1, n_sub)
        def _(i):
            pl.semaphore_signal(
                barrier, inc=1, device_id=(dom, lax.rem(sub + i, n_sub)), device_id_type=MESH
            )

    for load in loads:
        load.start()

    first[...] = jnp.zeros_like(first)
    density_pad[...] = jnp.zeros_like(density_pad)
    energy_pad[...] = jnp.zeros_like(energy_pad)
    flat[...] = jnp.zeros_like(flat)
    out_wide[...] = jnp.zeros_like(out_wide)

    lane = lax.broadcasted_iota(jnp.int32, (64, 128), 1)
    row = lax.broadcasted_iota(jnp.int32, (64, 128), 0)
    q_of, r_of = (lane % HALF) // ROW, lane % ROW
    a_of, b_of, c_of = row // 16, (row // 4) % 4, row % 4
    low_half = lane < HALF
    valid = low_half & (r_of < EZ)
    triple = lambda x: jnp.concatenate([x, x, x], axis=0)
    y_up = triple((b_of == 3) & (q_of < EY - 1) & valid)
    y_down = triple((b_of == 0) & (q_of > 0) & valid)
    z_up = triple((c_of == 3) & (r_of < EZ - 1) & valid)
    z_down = triple((c_of == 0) & (r_of > 0) & valid)
    off_wall = jnp.where(
        valid
        & jnp.logical_or(a_of > 0, dom > 0)
        & jnp.logical_or(jnp.logical_or(c_of > 0, r_of > 0), sub > 0),
        1.0,
        0.0,
    )
    off_wall = triple(off_wall)
    owned = jnp.where(
        valid & (a_of > 0) & (c_of > 0) & ((b_of < 3) | (q_of == EY - 1)), 1.0, 0.0
    )
    owned = triple(owned)
    lane16, row16 = lane[:16], row[:16]
    r16 = jnp.where(lane16 < HALF, lane16 % ROW, ROW)

    for load in loads[:3]:
        load.wait()
    flat[0:3, :] = disp_in[...]
    flat[3:6, :] = vel_in[...]
    stacked = jnp.concatenate([flat[:, plane * x : plane * (x + 1)] for x in range(3)], axis=0)
    picked = jnp.dot(split_three(stacked), pick[...], preferred_element_type=jnp.float32)
    wide[...] = picked[0:24] + picked[24:48] + picked[48:72]
    for x in range(3):
        for pair in range(8):
            got = wide[8 * x : 8 * x + 8, 128 * pair : 128 * pair + 128]
            other = turn(got, 0, 64)
            at = 16 * (x + 1) + 2 * pair
            keep = lane[:8] < 64
            first[pl.ds(at, 8, stride=64), :] = jnp.where(keep, got, 0.0)
            first[pl.ds(at + 1, 8, stride=64), :] = jnp.where(keep, other, 0.0)

    pl.semaphore_wait(barrier, count)

    def faces(source, fields, place, shifts):
        packed = jnp.zeros((16, 128), jnp.float32)
        for k in range(fields):
            face = source[pl.ds(64 * k + place, 16, stride=4), :]
            if place == 3:
                packed = jnp.where(r16 == EZ - 1 - k, turn(face, 0, -k), packed)
            else:
                packed = jnp.where(r16 == k, turn(face, 0, k), packed)
        return packed

    waits = []

    def exchange_start(rnd, source, fields, x_target, ups, downs):
        if ups:
            packs[rnd, 1] = faces(source, fields, 3, None)
        if downs:
            packs[rnd, 0] = faces(source, fields, 0, None)
        started = []
        for number, (dx, dz) in enumerate(STEPS):
            lead = dz if dz else dx
            going = (dx, dz)
            up = all(s >= 0 for s in going)
            down = all(s <= 0 for s in going)
            if not ((ups and downs) or (ups and up) or (downs and down)):
                continue
            target = (dom + dx, sub + dz)
            jobs = []
            if dz == 0:
                base = 48 if dx > 0 else 0
                slot = 0 if dx > 0 else 1
                jobs.append(
                    (
                        source_blocks(source, fields, base),
                        x_target(slot),
                    )
                )
            elif dx == 0:
                side = 1 if dz > 0 else 0
                jobs.append((packs.at[rnd, side], z_got.at[rnd, 1 - side]))
            else:
                side = 1 if dz > 0 else 0
                half = 8 if dx > 0 else 0
                slot = (0 if dx > 0 else 1) + 2 * (1 - side)
                jobs.append((packs.at[rnd, side, pl.ds(half, 8)], d_got.at[rnd, slot]))
            src, dst = jobs[0]
            copy = pltpu.make_async_remote_copy(
                src_ref=src,
                dst_ref=dst,
                send_sem=send_sems.at[rnd, number],
                recv_sem=recv_sems.at[rnd, number],
                device_id=target,
                device_id_type=MESH,
            )

            @pl.when(inside(dx, dz))
            def _():
                copy.start()

            started.append((copy, (dx, dz)))
        return started

    def source_blocks(source, fields, base):
        blocks = source.reshape(source.shape[0] // 64, 64, 128)
        return blocks.at[pl.ds(0, fields), pl.ds(base, 16)]

    def exchange_wait(started):
        for copy, (dx, dz) in started:

            @pl.when(inside(-dx, -dz))
            def _():
                copy.wait_recv()

        waits.extend(started)

    def exchange_add(rnd, source, target, fields, x_from, ups, downs):
        top = lax.broadcasted_iota(jnp.int32, (8, 128), 0) < 4
        for came, side, place in ((ups, 0, 0), (downs, 1, 3)):
            if not came:
                continue
            face = z_got[rnd, side]
            low = jnp.where(top, turn(d_got[rnd, 2 * side], 4, 0), 0.0)
            high = jnp.where(top, 0.0, turn(d_got[rnd, 2 * side + 1], 4, 0))
            face = face + jnp.concatenate([low, high], axis=0)
            for k in range(fields):
                if place == 0:
                    part = jnp.where(r16 == 0, turn(face, 0, k - (EZ - 1)), 0.0)
                else:
                    part = jnp.where(r16 == EZ - 1, turn(face, 0, EZ - 1 - k), 0.0)
                at = pl.ds(64 * k + place, 16, stride=4)
                target[at, :] = target[at, :] + part
        for k in range(fields):
            if ups:
                target[64 * k : 64 * k + 16, :] += x_from(0)[k]
            if downs:
                target[64 * k + 48 : 64 * k + 64, :] += x_from(1)[k]

    started = exchange_start(0, first, 6, lambda slot: x_first, True, False)

    for load in loads[3:]:
        load.wait()
    step = step_in[0, 0]
    for q in range(EY):
        density_pad[ROW * q : ROW * q + EZ, 0:125] = density_in[EZ * q : EZ * q + EZ, :]
    energy_pad[0:27, 0:ELEMS] = energy_in[...]
    energy_pad[27:28, 0:ELEMS] = live_in[...].astype(jnp.float32)

    def exact(value, table):
        rows = value.shape[0]
        out = jnp.dot(split_three(value), table, preferred_element_type=jnp.float32)
        return out[0:rows] + out[rows : 2 * rows] + out[2 * rows :]

    by_lane = exact(energy_pad[...], widen[:, 0:128])
    live = by_lane[27:28, :]
    live_own[...] = jnp.broadcast_to(live, (8, 128))
    live_copies = []
    for number, (dx, dz) in enumerate(((-1, 0), (0, -1), (-1, -1))):
        live_copy = pltpu.make_async_remote_copy(
            src_ref=live_own,
            dst_ref=live_got.at[number],
            send_sem=live_send.at[number],
            recv_sem=live_recv.at[number],
            device_id=(dom + dx, sub + dz),
            device_id_type=MESH,
        )
        live_copies.append((live_copy, (dx, dz)))

        @pl.when(inside(dx, dz))
        def _():
            live_copy.start()

    live = live + turn(live, 0, 64)
    by_point = jnp.transpose(density_pad[...])
    mass_density = by_point[0:64] + turn(by_point[64:128], 0, 64)
    weight = quad_weight[...]
    live_weight = weight * live
    mass_weight = whole_weight[...] * (live_own[0:1, :] * by_point)
    at_points = dot(energy_forth, jnp.concatenate([by_lane, turn(by_lane, 0, 64)], axis=0))

    def paired(v):
        return jnp.concatenate(
            [
                jnp.concatenate([v[64 * k : 64 * k + 64], turn(v[64 * k : 64 * k + 64], 0, 64)], 0)
                for k in range(v.shape[0] // 64)
            ],
            axis=1,
        )

    def folded(product):
        half = product.shape[0] // 2
        out = []
        for k in range(product.shape[1] // 128):
            part = product[:, 128 * k : 128 * k + 128]
            out.append(part[:half] + turn(part[half:], 0, 64))
        return out

    def gradient(v):
        shaped = dot(grad_forth, paired(v))
        return [
            [shaped[64 * m : 64 * m + 64, 128 * c : 128 * c + 128] for m in range(3)]
            for c in range(3)
        ]

    def jacobian_of(v):
        jacobian = gradient(v)
        for c in range(3):
            jacobian[c][c] = jacobian[c][c] + 1.0
        return jacobian

    def project(fields):
        right = jnp.concatenate(
            [jnp.concatenate([fields[c][m] for c in range(3)], axis=1) for m in range(3)], axis=0
        )
        return share(jnp.concatenate(folded(dot(grad_back, right)), axis=0))

    def share(v):
        v = v * jnp.where(triple(valid), 1.0, 0.0)
        v = v + jnp.where(y_up, turn(v, 12, -ROW), 0.0) + jnp.where(y_down, turn(v, -12, ROW), 0.0)
        v = v + jnp.where(z_up, turn(v, 3, -1), 0.0) + jnp.where(z_down, turn(v, -3, 1), 0.0)
        return v

    def interpolate(v):
        return dot(basis_forth, jnp.concatenate([v[0:64], v[64:128], v[128:192]], axis=1))

    def volume_of(jacobian, cofactor):
        return (
            jacobian[0][0] * cofactor[0][0]
            + jacobian[0][1] * cofactor[0][1]
            + jacobian[0][2] * cofactor[0][2]
        )

    def begin(rnd, v, ups=True, downs=True):
        source = local.at[rnd - 1]
        source[...] = v
        state[...] = v
        return exchange_start(rnd, source, 3, lambda slot: x_got.at[rnd - 1, slot], ups, downs)

    def finish(rnd, started, ups=True, downs=True):
        exchange_wait(started)
        source = local.at[rnd - 1]
        exchange_add(
            rnd, source, state, 3, lambda slot: x_got.at[rnd - 1, slot], ups, downs
        )
        return state[...] * off_wall

    out_nodes[...] = first[0:384, :]
    exchange_wait(started)
    exchange_add(0, out_nodes, out_nodes, 6, lambda slot: x_first, True, False)
    displacement = out_nodes[0:192, :]
    velocity = out_nodes[192:384, :]

    jacobian = jacobian_of(displacement)
    velocity_grad = gradient(velocity)
    cofactor = cofactors(jacobian)
    volume = volume_of(jacobian, cofactor)
    inverse = 1.0 / volume
    density = mass_density * inverse
    pressure = (adiabatic - 1.0) * density * at_points
    spatial = [
        [
            (
                velocity_grad[c][0] * cofactor[m][0]
                + velocity_grad[c][1] * cofactor[m][1]
                + velocity_grad[c][2] * cofactor[m][2]
            )
            * inverse
            for m in range(3)
        ]
        for c in range(3)
    ]
    viscous = viscosity * density
    stress = [[None] * 3 for _ in range(3)]
    for c in range(3):
        for m in range(c, 3):
            value = viscous * (spatial[c][m] + spatial[m][c])
            stress[c][m] = stress[m][c] = value - pressure if c == m else value
    flux = [
        [
            -live_weight
            * (
                stress[c][0] * cofactor[0][m]
                + stress[c][1] * cofactor[1][m]
                + stress[c][2] * cofactor[2][m]
            )
            for m in range(3)
        ]
        for c in range(3)
    ]
    started = begin(1, project(flux))
    power = stress[0][0] * spatial[0][0]
    for c in range(3):
        for m in range(3):
            if c + m > 0:
                power = power + stress[c][m] * spatial[c][m]
    power = live_weight * volume * power
    sums = folded(
        dot(energy_back, jnp.concatenate([power, weight * mass_density], axis=1))
    )
    rates = jnp.where(valid[:32], sums[0] / jnp.where(valid[:32], sums[1], 1.0), 0.0)
    rate_out[...] = exact(rates, widen[:, 128:256])[0:27, 0:ELEMS]
    force = finish(1, started)

    wide_mass = jnp.concatenate([mass_weight] * 3, axis=1)
    values = interpolate(force)
    weighted = wide_mass * values
    product = dot(basis_back, weighted)
    image = share(
        jnp.concatenate([product[:, 128 * k : 128 * k + 128] for k in range(3)], axis=0)
    )
    started = begin(2, image)

    def total(x):
        return jnp.sum(jnp.sum(x, axis=0, keepdims=True), axis=1, keepdims=True)

    norm_part = total(force * force * owned)
    product_part = total(weighted * values)
    image = finish(2, started)
    image_norm_part = total(image * image * owned)
    values = interpolate(image)
    image_product_part = total(wide_mass * values * values)

    lane1 = lane[0:1]
    packed = jnp.where(
        lane1 == 0,
        norm_part,
        jnp.where(
            lane1 == 1,
            product_part,
            jnp.where(lane1 == 2, image_norm_part, image_product_part),
        ),
    )

    late = []

    def all_sum(value, slots, targets, sends, recvs, cover=None):
        slots[0] = value

        def copy_of(source, target, device):
            return pltpu.make_async_remote_copy(
                src_ref=source,
                dst_ref=target,
                send_sem=sends.at[0],
                recv_sem=recvs.at[0],
                device_id=device,
                device_id_type=MESH,
            )

        for number, device in targets:
            copy_of(slots.at[0], slots.at[number], device).start()

        out = cover() if cover else None

        others = slots.at[pl.ds(1, len(targets))]
        whole_sum = copy_of(others, others, targets[0][1])
        whole_sum.wait_recv()
        late.append(whole_sum)
        return jnp.sum(slots[...], axis=0), out

    doms = [lax.rem(dom + i, n_dom) for i in range(n_dom)]
    subs = [lax.rem(sub + i, n_sub) for i in range(n_sub)]

    def ahead():
        return [gradient(v) for v in (displacement + step * velocity, force, image)]

    if one_phase:
        targets = [
            (j * n_dom + i, (doms[i], subs[j]))
            for j in [*range(1, n_sub), 0]
            for i in range(n_dom)
            if i + j > 0
        ]
        packed, slopes = all_sum(packed, sum_dom, targets, dom_send, dom_recv, ahead)
    else:
        targets = [(i, (doms[i], sub)) for i in range(1, n_dom)]
        packed, slopes = all_sum(packed, sum_dom, targets, dom_send, dom_recv, ahead)
        targets = [(j, (dom, subs[j])) for j in range(1, n_sub)]
        packed, _ = all_sum(packed, sum_sub, targets, sub_send, sub_recv)
    rr, rw, ww, wmw = (
        jnp.sum(jnp.where(lane1 == k, packed, 0.0), axis=1, keepdims=True) for k in range(4)
    )
    first_length = rr / rw
    next_norm = first_length * (first_length * ww) - rr
    conjugacy = next_norm / rr
    residual_image = rw - first_length * ww
    residual_product = rw - 2.0 * first_length * ww + first_length * first_length * wmw
    bend = residual_product + 2.0 * conjugacy * residual_image + conjugacy * conjugacy * rw
    second_length = next_norm / bend
    on_force = first_length + second_length * (1.0 + conjugacy)
    on_image = second_length * first_length
    new_velocity = velocity + step * (on_force * force - on_image * image)
    moved = displacement + step * new_velocity

    def fluxes(jacobian, weights):
        cofactor = cofactors(jacobian)
        volume = volume_of(jacobian, cofactor)
        norm_sq = None
        for c in range(3):
            for m in range(3):
                square = jacobian[c][m] * jacobian[c][m]
                norm_sq = square if norm_sq is None else norm_sq + square
        scale = weights * jnp.exp(jnp.log(volume) * (-2.0 / 3.0))
        along = scale * (2.0 / 3.0)
        across = scale * (2.0 / 9.0) * (norm_sq / volume)
        return [
            [along * jacobian[c][m] - across * cofactor[c][m] for m in range(3)]
            for c in range(3)
        ]

    def back_to_lattice(nodes):
        for x in range(3):
            for pair in range(8):
                at = 16 * (x + 1) + 2 * pair
                even = nodes[pl.ds(at, 3, stride=64), :]
                odd = nodes[pl.ds(at + 1, 3, stride=64), :]
                out_wide[8 * x : 8 * x + 3, 128 * pair : 128 * pair + 128] = even + turn(odd, 0, 64)
        back = lax.dot_general(
            split_three(out_wide[...]), pick[...], (((1,), (1,)), ((), ())), preferred_element_type=jnp.float32
        )
        return back[0:24] + back[24:48] + back[48:72]

    by_force, by_image = step * step * on_force, step * step * on_image
    jacobian = [
        [
            slopes[0][c][m] + by_force * slopes[1][c][m] - by_image * slopes[2][c][m]
            for m in range(3)
        ]
        for c in range(3)
    ]
    for c in range(3):
        jacobian[c][c] = jacobian[c][c] + 1.0
    shift = -mesh_step * project(fluxes(jacobian, live_weight))

    comps = range(3)
    a_first, c_first = a_of == 0, c_of == 0
    part = [shift[64 * k : 64 * k + 64] for k in comps]
    whole = [moved[64 * k : 64 * k + 64] + part[k] for k in comps]
    ours[...] = shift
    slab = jnp.concatenate([jnp.where(a_first, part[k], whole[k]) for k in comps], axis=0)
    near[...] = slab[0:96] + turn(slab[96:192], 0, 64)
    r64 = jnp.where(low_half, r_of, ROW)

    def lay(fields, place):
        out = None
        for k in comps:
            at = r64[: fields[k].shape[0]]
            piece = jnp.where(at == k, turn(fields[k], 0, k - place), 0.0)
            out = piece if out is None else out + piece
        return out + turn(out, 0, 64)

    layer = [jnp.where(c_first, part[k], whole[k]) for k in comps]
    right_half = jnp.logical_not(low_half)
    r_here = r_of[:16]

    def lay_group(fields, a):
        out = None
        half = low_half[:16] if a < 2 else right_half[:16]
        for k in comps:
            spot = 3 * (a % 2) + k
            piece = jnp.where(
                half & (r_here == spot), turn(fields[k], 0, 64 * (a // 2) + spot), 0.0
            )
            out = piece if out is None else out + piece
        return out

    groups = [lay_group([f[16 * a : 16 * a + 16] for f in layer], a) for a in range(4)]
    upper_groups = groups[1] + groups[2] + groups[3]
    face_part = lay_group([part[k][0:16] for k in comps], 0)
    z_low[0] = turn(face_part + upper_groups, 0, 64)
    z_low[1] = groups[0] + upper_groups
    z_low[2] = lay([part[k][48:64] for k in comps], 0)
    z_high[...] = lay([ours[pl.ds(64 * k + 3, 16, stride=4), :] for k in comps], EZ - 1)
    x_face[0, 0:16] = part[1][0:16] + turn(part[0][0:16], 0, 64)
    x_face[0, 16:24] = part[2][8:16] + turn(part[2][0:8], 0, 64)
    x_face[1, 0:16] = part[0][48:64] + turn(part[1][48:64], 0, 64)
    x_face[1, 16:24] = part[2][48:56] + turn(part[2][56:64], 0, 64)

    routes = {
        (-1, 0): (near, slab_got),
        (-2, 0): (x_face.at[0], x_face_got.at[0]),
        (1, 0): (x_face.at[1], x_face_got.at[1]),
        (0, -1): (z_low.at[1], layer_got.at[0]),
        (-1, -1): (z_low.at[0], layer_got.at[1]),
        (-2, -1): (z_low.at[0], edge_got.at[0]),
        (1, -1): (z_low.at[2], edge_got.at[1]),
        (0, 1): (z_high, floor_got.at[0]),
        (-1, 1): (z_high, floor_got.at[1]),
        (-2, 1): (z_high.at[pl.ds(0, 8)], floor_got.at[2, pl.ds(0, 8)]),
        (1, 1): (z_high.at[pl.ds(8, 8)], floor_got.at[3, pl.ds(8, 8)]),
    }
    started = []
    for number, (dx, dz) in enumerate(WIDE_STEPS):
        source, target = routes[dx, dz]
        wide_copy = pltpu.make_async_remote_copy(
            src_ref=source,
            dst_ref=target,
            send_sem=wide_send.at[number],
            recv_sem=wide_recv.at[number],
            device_id=(dom + dx, sub + dz),
            device_id_type=MESH,
        )

        @pl.when(inside(dx, dz))
        def _():
            wide_copy.start()

        started.append((wide_copy, (dx, dz)))
    exchange_wait(live_copies)
    out_nodes[0:192, :] = new_velocity * owned
    new_back = back_to_lattice(out_nodes)
    one_low, one_r = low_half[0:1], r_of[0:1]
    live_up = turn(live_got[0, 0:1, :], 0, 64)
    live_layer = live_got[1, 0:1, :] + turn(live_got[2, 0:1, :], 0, 64)
    live_wide = live_own[0:1, :] + live_up + jnp.where(one_r == EZ, turn(live_layer, 0, EZ), 0.0)
    wide_weight = whole_weight[...] * live_wide
    wide_wall = jnp.where(
        jnp.logical_or(right_half, jnp.logical_or(a_of > 0, dom > 0))
        & jnp.logical_or(jnp.logical_or(c_of > 0, r_of > 0), sub > 0),
        1.0,
        0.0,
    )
    low16, row16r = low_half[:16], r_of[:16]

    for whole_sum in late:
        whole_sum.wait_send()
    for copy, (dx, dz) in waits + started:

        @pl.when(inside(dx, dz))
        def _():
            copy.wait_send()

    exchange_wait(started)
    upper = slab_got[...]
    upper = jnp.concatenate([turn(upper, 0, 64), upper], axis=0)
    first_got, second_got = layer_got[0], layer_got[1]
    mixed = (
        jnp.where(low16, first_got, second_got),
        jnp.where(low16, second_got, first_got),
    )
    right16 = right_half[:16]
    edge_up = jnp.where(right16, edge_got[0], 0.0)
    edge_down = jnp.where(low16, edge_got[1], 0.0)
    floor = jnp.where(low16, floor_got[0], floor_got[1])
    floor = floor + jnp.where(right16 & (row16 >= 12), turn(floor_got[2], 12, 0), 0.0)
    floor = floor + jnp.where(low16 & (row16 < 4), turn(floor_got[3], 4, 0), 0.0)
    face_low = [
        x_face_got[1, 0:16],
        turn(x_face_got[1, 0:16], 0, 64),
        jnp.concatenate([x_face_got[1, 16:24], turn(x_face_got[1, 16:24], 0, 64)], axis=0),
    ]
    face_high = [
        x_face_got[0, 0:16],
        turn(x_face_got[0, 0:16], 0, 64),
        jnp.concatenate([x_face_got[0, 16:24], turn(x_face_got[0, 16:24], 0, 64)], axis=0),
    ]
    for k in comps:
        at = 64 * k
        rows = []
        for a in range(4):
            u = jnp.where(low16, whole[k][16 * a : 16 * a + 16], upper[at + 16 * a : at + 16 * a + 16])
            spot = 3 * (a % 2) + k
            piece = turn(mixed[a // 2], 0, EZ - spot - 64 * (a // 2))
            if a == 0:
                piece = piece + jnp.where(low16, turn(edge_down, 0, EZ - k), 0.0)
                u = u + jnp.where(low16, face_low[k], 0.0)
            if a == 3:
                piece = piece + jnp.where(low16, 0.0, turn(edge_up, 0, EZ - k))
                u = u + jnp.where(low16, 0.0, face_high[k])
            rows.append(u + jnp.where(row16r == EZ, piece, 0.0))
        wide_nodes[at : at + 64, :] = jnp.concatenate(rows, axis=0)
        below = pl.ds(at, 16, stride=4)
        above = pl.ds(at + 3, 16, stride=4)
        wide_nodes[below, :] += jnp.where(row16r == 0, turn(floor, 0, -k), 0.0)
        near_face = wide_nodes[at : at + 16, :]
        far_face = wide_nodes[at + 48 : at + 64, :]
        wide_nodes[at : at + 16, :] = near_face + jnp.where(low16, 0.0, turn(far_face, 0, 64))
        wide_nodes[at + 48 : at + 64, :] = far_face + jnp.where(low16, turn(near_face, 0, 64), 0.0)
        tops = wide_nodes[above, :]
        bottoms = wide_nodes[below, :]
        wide_nodes[above, :] = tops + jnp.where(row16r == EZ - 1, turn(bottoms, 0, -1), 0.0)
        wide_nodes[below, :] = bottoms + jnp.where(row16r == EZ, turn(tops, 0, 1), 0.0)
    relaxed = [wide_nodes[64 * k : 64 * k + 64, :] * wide_wall for k in comps]
    shaped = dot(whole_forth, jnp.concatenate(relaxed, axis=1))
    jacobian = [
        [shaped[128 * m : 128 * m + 128, 128 * c : 128 * c + 128] for m in comps] for c in comps
    ]
    for c in comps:
        jacobian[c][c] = jacobian[c][c] + 1.0
    fields = fluxes(jacobian, wide_weight)
    right = jnp.concatenate(
        [jnp.concatenate([fields[c][m] for c in comps], axis=1) for m in comps], axis=0
    )
    product = dot(whole_back, right)
    last = []
    for k in comps:
        v = product[:, 128 * k : 128 * k + 128]
        v = v + jnp.where((b_of == 0) & (q_of > 0), turn(v, -12, ROW), 0.0)
        v = v + jnp.where((c_of == 3) & (r_of < EZ), turn(v, 3, -1), 0.0)
        v = jnp.concatenate([v[0:48], v[48:64] + turn(v[0:16], 0, 64)], axis=0)
        last.append(moved[64 * k : 64 * k + 64] - relaxed[k] + mesh_step * v)
    last = jnp.concatenate(last, axis=0)
    mesh_velocity = new_velocity - last / step

    out_nodes[192:384, :] = mesh_velocity * owned
    mesh_back = back_to_lattice(out_nodes.at[pl.ds(192, 192)])
    for x in range(3):
        new_vel_out[:, plane * x : plane * (x + 1)] = new_back[8 * x : 8 * x + 3]
        mesh_vel_out[:, plane * x : plane * (x + 1)] = mesh_back[8 * x : 8 * x + 3]


def hand_on(*refs):
    copies = [
        pltpu.make_async_copy(refs[k], refs[3 + k], refs[6].at[k]) for k in range(3)
    ]
    for copy in copies:
        copy.start()
    for copy in copies:
        copy.wait()


def body(n_dom, n_sub, displacement, velocity, energy, mass_density, live_mask, time_step):
    made_tables = tables()
    vmem = pl.BlockSpec(memory_space=pltpu.VMEM)
    anywhere = pl.BlockSpec(memory_space=pl.ANY)
    f32 = jnp.float32
    nodes = displacement.shape[1]
    wide_sum = n_dom * n_sub if n_dom * n_sub <= 64 else n_dom
    made = pl.pallas_call(
        functools.partial(kernel, n_dom, n_sub),
        out_shape=(
            pltpu.VMEM(displacement.shape, f32),
            pltpu.VMEM(energy.shape, f32),
            pltpu.VMEM(displacement.shape, f32),
        ),
        in_specs=[anywhere] * (6 + len(made_tables)),
        out_specs=(vmem, vmem, vmem),
        scratch_shapes=[
            pltpu.VMEM((8, nodes), f32),
            pltpu.VMEM((24, 1024), f32),
            pltpu.VMEM((512, 128), f32),
            pltpu.VMEM((2, 192, 128), f32),
            pltpu.VMEM((192, 128), f32),
            pltpu.VMEM((384, 128), f32),
            pltpu.VMEM((24, 1024), f32),
            pltpu.VMEM((128, 128), f32),
            pltpu.VMEM((32, 128), f32),
            pltpu.VMEM((8, 128), f32),
            pltpu.VMEM((3, 8, 128), f32),
            pltpu.VMEM((3, 2, 16, 128), f32),
            pltpu.VMEM((6, 16, 128), f32),
            pltpu.VMEM((2, 2, 3, 16, 128), f32),
            pltpu.VMEM((3, 2, 16, 128), f32),
            pltpu.VMEM((3, 4, 8, 128), f32),
            pltpu.VMEM((wide_sum, 1, 128), f32),
            pltpu.VMEM((n_sub, 1, 128), f32),
            pltpu.SemaphoreType.DMA((3, 8)),
            pltpu.SemaphoreType.DMA((3, 8)),
            pltpu.SemaphoreType.DMA((wide_sum,)),
            pltpu.SemaphoreType.DMA((wide_sum,)),
            pltpu.SemaphoreType.DMA((n_sub,)),
            pltpu.SemaphoreType.DMA((n_sub,)),
            pltpu.VMEM(displacement.shape, f32),
            pltpu.VMEM(velocity.shape, f32),
            pltpu.VMEM(energy.shape, f32),
            pltpu.VMEM(mass_density.shape[::-1], f32),
            pltpu.VMEM((1, live_mask.shape[0]), jnp.int32),
            pltpu.SMEM((1, 1), f32),
            *[pltpu.VMEM(t.shape, t.dtype) for t in made_tables],
            pltpu.SemaphoreType.DMA((6 + len(made_tables),)),
            pltpu.VMEM((192, 128), f32),
            pltpu.VMEM((96, 128), f32),
            pltpu.VMEM((3, 16, 128), f32),
            pltpu.VMEM((16, 128), f32),
            pltpu.VMEM((2, 24, 128), f32),
            pltpu.VMEM((96, 128), f32),
            pltpu.VMEM((2, 24, 128), f32),
            pltpu.VMEM((2, 16, 128), f32),
            pltpu.VMEM((2, 16, 128), f32),
            pltpu.VMEM((4, 16, 128), f32),
            pltpu.VMEM((192, 128), f32),
            pltpu.SemaphoreType.DMA((len(WIDE_STEPS),)),
            pltpu.SemaphoreType.DMA((len(WIDE_STEPS),)),
            pltpu.SemaphoreType.DMA((3,)),
            pltpu.SemaphoreType.DMA((3,)),
        ],
        compiler_params=pltpu.CompilerParams(collective_id=0, has_side_effects=True),
    )(
        displacement,
        velocity,
        energy,
        mass_density.T,
        live_mask.reshape(1, -1),
        time_step.reshape(1, 1),
        *[jnp.asarray(t) for t in made_tables],
    )
    return pl.pallas_call(
        hand_on,
        out_shape=[jax.ShapeDtypeStruct(m.shape, f32) for m in made],
        in_specs=[vmem] * 3,
        out_specs=[anywhere] * 3,
        scratch_shapes=[pltpu.SemaphoreType.DMA((3,))],
    )(*[pltpu.with_memory_space_constraint(m, pltpu.VMEM) for m in made])


def solution(mesh):
    split = ("dom", "sub")
    return jax.shard_map(
        functools.partial(body, mesh.shape["dom"], mesh.shape["sub"]),
        mesh=mesh,
        in_specs=(
            P(None, split),
            P(None, split),
            P(None, split),
            P(None, split),
            P(split),
            P(),
        ),
        out_specs=(P(None, split), P(None, split), P(None, split)),
        check_vma=False,
    )
```

```python
import functools
import math

import jax
import jax.numpy as jnp
import numpy as np
from jax import lax
from jax.experimental import pallas as pl
from jax.experimental.pallas import tpu as pltpu
from jax.sharding import PartitionSpec as P

EX = 1
EY = 8
EZ = 6
ELEMS = EX * EY * EZ
HALF = 64
ROW = 8

adiabatic = 5.0 / 3.0
viscosity = 0.3
mesh_step = 0.01
MESH = pl.DeviceIdType.MESH
STEPS = [(-1, -1), (-1, 1), (1, -1), (1, 1), (0, -1), (0, 1), (-1, 0), (1, 0)]
WIDE_STEPS = [(-2, -1), (-2, 1), (1, -1), (1, 1), (-1, 1), (-1, -1)]
WIDE_STEPS += [(0, -1), (0, 1), (-2, 0), (1, 0), (-1, 0)]


def one_dimension():
    root_term = math.sqrt(10.0 / 7.0)
    outer_root = math.sqrt(5.0 + 2.0 * root_term) / 3.0
    inner_root = math.sqrt(5.0 - 2.0 * root_term) / 3.0
    gauss_roots = np.array([-outer_root, -inner_root, 0.0, inner_root, outer_root])
    outer_weight = (322.0 - 13.0 * math.sqrt(70.0)) / 900.0
    middle_weight = (322.0 + 13.0 * math.sqrt(70.0)) / 900.0
    weights = (
        np.array([outer_weight, middle_weight, 128.0 / 225.0, middle_weight, outer_weight]) / 2.0
    )
    points = (1.0 + gauss_roots) / 2.0
    lobatto = [0.0, (1.0 - 1.0 / math.sqrt(5.0)) / 2.0, (1.0 + 1.0 / math.sqrt(5.0)) / 2.0, 1.0]
    values = np.ones((5, 4))
    slopes = np.zeros((5, 4))
    for node in range(4):
        for other in range(4):
            if other != node:
                values[:, node] *= (points - lobatto[other]) / (lobatto[node] - lobatto[other])
                term = np.ones(5) / (lobatto[node] - lobatto[other])
                for third in range(4):
                    if third != node and third != other:
                        term = term * (points - lobatto[third]) / (lobatto[node] - lobatto[third])
                slopes[:, node] += term
    bernstein = np.stack([(1.0 - points) ** 2, 2.0 * points * (1.0 - points), points**2], axis=1)
    return values, slopes, bernstein, weights


def outer_triple(first, second, third):
    product = np.einsum("ia,jb,kc->ijkabc", first, second, third)
    return product.reshape(125, -1)


def halves(table, rows):
    padded = np.concatenate([table, np.repeat(table[-1:], 3, axis=0)], axis=0)
    padded = np.pad(padded, [(0, 0), (0, rows - table.shape[1])])
    return np.concatenate([padded[:64], padded[64:]], axis=1)


def stacked_left(table):
    table = np.asarray(table, np.float32)
    high = table.astype(jnp.bfloat16)
    low = (table - high.astype(np.float32)).astype(jnp.bfloat16)
    return np.concatenate([low, high, high], axis=1)


@functools.lru_cache(None)
def tables():
    values, slopes, bernstein, weights = one_dimension()
    triples = [
        outer_triple(slopes, values, values),
        outer_triple(values, slopes, values),
        outer_triple(values, values, slopes),
    ]
    grad = np.concatenate([halves(t, 64) for t in triples], axis=0)
    whole = [np.concatenate([t, np.repeat(t[-1:], 3, axis=0)], axis=0) for t in triples]
    basis = outer_triple(values, values, values)
    basis = np.concatenate([basis, np.repeat(basis[-1:], 3, axis=0)], axis=0)
    energy = halves(outer_triple(bernstein, bernstein, bernstein), 32)
    weight = np.einsum("i,j,k->ijk", weights, weights, weights).reshape(125)
    weight = np.pad(weight, (0, 3))
    spread_weight = np.zeros((64, 128))
    spread_weight[:, :64] = weight[:64, None]
    spread_weight[:, 64:] = weight[64:, None]
    whole_weight = np.repeat(weight[:, None], 128, axis=1)
    planes_y, planes_z = 3 * EY + 1, 3 * EZ
    pick = np.zeros((planes_y * planes_z, 16 * HALF), np.float32)
    for b in range(4):
        for c in range(4):
            for q in range(EY):
                for r in range(EZ):
                    z = 3 * r + c - 1
                    if z >= 0:
                        lane = (4 * b + c) * HALF + q * ROW + r
                        pick[(3 * q + b) * planes_z + z, lane] = 1.0
    widen = np.zeros((128, 256), np.float32)
    for e in range(ELEMS):
        to = e // EZ * ROW + e % EZ
        widen[e, to] = 1.0
        widen[to, 128 + e] = 1.0
    return [
        pick.astype(jnp.bfloat16),
        stacked_left(grad),
        stacked_left(grad.T),
        stacked_left(basis),
        stacked_left(basis.T),
        stacked_left(energy),
        stacked_left(energy.T),
        stacked_left(np.concatenate(whole, axis=0)),
        stacked_left(np.concatenate(whole, axis=0).T),
        widen.astype(jnp.bfloat16),
        np.asarray(spread_weight, np.float32),
        np.asarray(whole_weight, np.float32),
    ]


def dot(table, right):
    high, low = split_two(right)
    stacked = jnp.concatenate([high, low, high], axis=0)
    return jnp.dot(table[...], stacked, preferred_element_type=jnp.float32)


def split_two(value):
    high = value.astype(jnp.bfloat16)
    return high, (value - high.astype(jnp.float32)).astype(jnp.bfloat16)


def cofactors(m):
    return [
        [
            m[(i + 1) % 3][(j + 1) % 3] * m[(i + 2) % 3][(j + 2) % 3]
            - m[(i + 1) % 3][(j + 2) % 3] * m[(i + 2) % 3][(j + 1) % 3]
            for j in range(3)
        ]
        for i in range(3)
    ]


def turn(value, rows, lanes):
    if rows:
        value = pltpu.roll(value, rows % value.shape[0], 0)
    if lanes % value.shape[1]:
        value = pltpu.roll(value, lanes % value.shape[1], 1)
    return value


def split_three(value):
    high = value.astype(jnp.bfloat16).astype(jnp.float32)
    rest = value - high
    middle = rest.astype(jnp.bfloat16).astype(jnp.float32)
    return jnp.concatenate([high, middle, rest - middle], axis=0).astype(jnp.bfloat16)


def kernel(
    n_dom,
    n_sub,
    disp_in_hbm,
    vel_in_hbm,
    energy_in_hbm,
    density_in_hbm,
    live_in_hbm,
    step_in_hbm,
    pick_hbm,
    grad_forth_hbm,
    grad_back_hbm,
    basis_forth_hbm,
    basis_back_hbm,
    energy_forth_hbm,
    energy_back_hbm,
    whole_forth_hbm,
    whole_back_hbm,
    widen_hbm,
    quad_weight_hbm,
    whole_weight_hbm,
    new_vel_out,
    rate_out,
    mesh_vel_out,
    flat,
    wide,
    first,
    local,
    state,
    out_nodes,
    out_wide,
    density_pad,
    energy_pad,
    live_own,
    live_got,
    packs,
    x_first,
    x_got,
    z_got,
    d_got,
    sum_dom,
    sum_sub,
    send_sems,
    recv_sems,
    dom_send,
    dom_recv,
    sub_send,
    sub_recv,
    disp_in,
    vel_in,
    energy_in,
    density_in,
    live_in,
    step_in,
    pick,
    grad_forth,
    grad_back,
    basis_forth,
    basis_back,
    energy_forth,
    energy_back,
    whole_forth,
    whole_back,
    widen,
    quad_weight,
    whole_weight,
    in_sems,
    ours,
    near,
    z_low,
    z_high,
    x_face,
    slab_got,
    x_face_got,
    layer_got,
    edge_got,
    floor_got,
    wide_nodes,
    wide_send,
    wide_recv,
    live_send,
    live_recv,
):
    dom = lax.axis_index("dom")
    sub = lax.axis_index("sub")
    plane = (3 * EY + 1) * 3 * EZ

    def inside(dx, dz):
        ok = None
        for step, place, size in ((dx, dom, n_dom), (dz, sub, n_sub)):
            if step:
                here = (place + step >= 0) if step < 0 else (place + step < size)
                ok = here if ok is None else jnp.logical_and(ok, here)
        return ok

    held = [
        (disp_in_hbm, disp_in),
        (vel_in_hbm, vel_in),
        (pick_hbm, pick),
        (step_in_hbm, step_in),
        (density_in_hbm, density_in),
        (energy_in_hbm, energy_in),
        (live_in_hbm, live_in),
        (grad_forth_hbm, grad_forth),
        (grad_back_hbm, grad_back),
        (basis_forth_hbm, basis_forth),
        (basis_back_hbm, basis_back),
        (energy_forth_hbm, energy_forth),
        (energy_back_hbm, energy_back),
        (whole_forth_hbm, whole_forth),
        (widen_hbm, widen),
        (quad_weight_hbm, quad_weight),
        (whole_weight_hbm, whole_weight),
        (whole_back_hbm, whole_back),
    ]
    loads = [
        pltpu.make_async_copy(source, target, in_sems.at[number])
        for number, (source, target) in enumerate(held)
    ]
    x_first[...] = jnp.zeros_like(x_first)
    x_got[...] = jnp.zeros_like(x_got)
    z_got[...] = jnp.zeros_like(z_got)
    d_got[...] = jnp.zeros_like(d_got)
    for got in (slab_got, x_face_got, layer_got, edge_got, floor_got, live_got):
        got[...] = jnp.zeros_like(got)

    barrier = pltpu.get_barrier_semaphore()
    one_phase = n_dom * n_sub <= 64
    if one_phase and n_sub <= 4:
        count = n_dom - 1
        for dz in (-1, 1):
            count = count + n_dom * inside(0, dz).astype(jnp.int32)
        for dz in (0, -1, 1):

            def greet(dz=dz):
                @pl.loop(0 if dz else 1, n_dom, unroll=True)
                def _(i):
                    pl.semaphore_signal(
                        barrier,
                        inc=1,
                        device_id=(lax.rem(dom + i, n_dom), sub + dz),
                        device_id_type=MESH,
                    )

            if dz:
                pl.when(inside(0, dz))(greet)
            else:
                greet()

    elif one_phase:
        devices = n_dom * n_sub
        count = devices - 1

        @pl.loop(1, devices, unroll=True)
        def _(i):
            t = lax.rem(dom * n_sub + sub + i, devices)
            pl.semaphore_signal(
                barrier,
                inc=1,
                device_id=(t // n_sub, lax.rem(t, n_sub)),
                device_id_type=MESH,
            )

    else:
        count = (n_dom - 1) + (n_sub - 1)
        for dx, dz in [(dx, dz) for dx in (-2, -1, 1, 2) for dz in (-1, 1)]:
            if dx and dz:
                ok = inside(dx, dz)
                count = count + ok.astype(jnp.int32)

                @pl.when(ok)
                def _():
                    pl.semaphore_signal(
                        barrier, inc=1, device_id=(dom + dx, sub + dz), device_id_type=MESH
                    )

        @pl.loop(1, n_dom)
        def _(i):
            pl.semaphore_signal(
                barrier, inc=1, device_id=(lax.rem(dom + i, n_dom), sub), device_id_type=MESH
            )

        @pl.loop(1, n_sub)
        def _(i):
            pl.semaphore_signal(
                barrier, inc=1, device_id=(dom, lax.rem(sub + i, n_sub)), device_id_type=MESH
            )

    for load in loads:
        load.start()

    first[...] = jnp.zeros_like(first)
    density_pad[...] = jnp.zeros_like(density_pad)
    energy_pad[...] = jnp.zeros_like(energy_pad)
    flat[...] = jnp.zeros_like(flat)
    out_wide[...] = jnp.zeros_like(out_wide)

    lane = lax.broadcasted_iota(jnp.int32, (64, 128), 1)
    row = lax.broadcasted_iota(jnp.int32, (64, 128), 0)
    q_of, r_of = (lane % HALF) // ROW, lane % ROW
    a_of, b_of, c_of = row // 16, (row // 4) % 4, row % 4
    low_half = lane < HALF
    valid = low_half & (r_of < EZ)
    triple = lambda x: jnp.concatenate([x, x, x], axis=0)
    z_up = triple((c_of == 3) & (r_of < EZ - 1) & valid)
    z_down = triple((c_of == 0) & (r_of > 0) & valid)
    off_wall = jnp.where(
        valid
        & jnp.logical_or(a_of > 0, dom > 0)
        & jnp.logical_or(jnp.logical_or(c_of > 0, r_of > 0), sub > 0),
        1.0,
        0.0,
    )
    off_wall = triple(off_wall)
    owned = jnp.where(
        valid & (a_of > 0) & (c_of > 0) & ((b_of < 3) | (q_of == EY - 1)), 1.0, 0.0
    )
    owned = triple(owned)
    lane16, row16 = lane[:16], row[:16]
    r16 = jnp.where(lane16 < HALF, lane16 % ROW, ROW)

    for load in loads[:3]:
        load.wait()
    flat[0:3, :] = disp_in[...]
    flat[3:6, :] = vel_in[...]
    stacked = jnp.concatenate([flat[:, plane * x : plane * (x + 1)] for x in range(3)], axis=0)
    picked = jnp.dot(split_three(stacked), pick[...], preferred_element_type=jnp.float32)
    wide[...] = picked[0:24] + picked[24:48] + picked[48:72]
    for x in range(3):
        for pair in range(8):
            got = wide[8 * x : 8 * x + 8, 128 * pair : 128 * pair + 128]
            other = turn(got, 0, 64)
            at = 16 * (x + 1) + 2 * pair
            keep = lane[:8] < 64
            first[pl.ds(at, 8, stride=64), :] = jnp.where(keep, got, 0.0)
            first[pl.ds(at + 1, 8, stride=64), :] = jnp.where(keep, other, 0.0)

    pl.semaphore_wait(barrier, count)

    def faces(source, fields, place, shifts):
        packed = jnp.zeros((16, 128), jnp.float32)
        for k in range(fields):
            face = source[pl.ds(64 * k + place, 16, stride=4), :]
            if place == 3:
                packed = jnp.where(r16 == EZ - 1 - k, turn(face, 0, -k), packed)
            else:
                packed = jnp.where(r16 == k, turn(face, 0, k), packed)
        return packed

    waits = []

    def exchange_start(rnd, source, fields, x_target, ups, downs):
        if ups:
            packs[rnd, 1] = faces(source, fields, 3, None)
        if downs:
            packs[rnd, 0] = faces(source, fields, 0, None)
        started = []
        for number, (dx, dz) in enumerate(STEPS):
            lead = dz if dz else dx
            going = (dx, dz)
            up = all(s >= 0 for s in going)
            down = all(s <= 0 for s in going)
            if not ((ups and downs) or (ups and up) or (downs and down)):
                continue
            target = (dom + dx, sub + dz)
            jobs = []
            if dz == 0:
                base = 48 if dx > 0 else 0
                slot = 0 if dx > 0 else 1
                jobs.append(
                    (
                        source_blocks(source, fields, base),
                        x_target(slot),
                    )
                )
            elif dx == 0:
                side = 1 if dz > 0 else 0
                jobs.append((packs.at[rnd, side], z_got.at[rnd, 1 - side]))
            else:
                side = 1 if dz > 0 else 0
                half = 8 if dx > 0 else 0
                slot = (0 if dx > 0 else 1) + 2 * (1 - side)
                jobs.append((packs.at[rnd, side, pl.ds(half, 8)], d_got.at[rnd, slot]))
            src, dst = jobs[0]
            copy = pltpu.make_async_remote_copy(
                src_ref=src,
                dst_ref=dst,
                send_sem=send_sems.at[rnd, number],
                recv_sem=recv_sems.at[rnd, number],
                device_id=target,
                device_id_type=MESH,
            )

            @pl.when(inside(dx, dz))
            def _():
                copy.start()

            started.append((copy, (dx, dz)))
        return started

    def source_blocks(source, fields, base):
        blocks = source.reshape(source.shape[0] // 64, 64, 128)
        return blocks.at[pl.ds(0, fields), pl.ds(base, 16)]

    def exchange_wait(started):
        for copy, (dx, dz) in started:

            @pl.when(inside(-dx, -dz))
            def _():
                copy.wait_recv()

        waits.extend(started)

    def exchange_add(rnd, source, target, fields, x_from, ups, downs):
        top = lax.broadcasted_iota(jnp.int32, (8, 128), 0) < 4
        for came, side, place in ((ups, 0, 0), (downs, 1, 3)):
            if not came:
                continue
            face = z_got[rnd, side]
            low = jnp.where(top, turn(d_got[rnd, 2 * side], 4, 0), 0.0)
            high = jnp.where(top, 0.0, turn(d_got[rnd, 2 * side + 1], 4, 0))
            face = face + jnp.concatenate([low, high], axis=0)
            for k in range(fields):
                if place == 0:
                    part = jnp.where(r16 == 0, turn(face, 0, k - (EZ - 1)), 0.0)
                else:
                    part = jnp.where(r16 == EZ - 1, turn(face, 0, EZ - 1 - k), 0.0)
                at = pl.ds(64 * k + place, 16, stride=4)
                target[at, :] = target[at, :] + part
        for k in range(fields):
            if ups:
                target[64 * k : 64 * k + 16, :] += x_from(0)[k]
            if downs:
                target[64 * k + 48 : 64 * k + 64, :] += x_from(1)[k]

    started = exchange_start(0, first, 6, lambda slot: x_first, True, False)

    for load in loads[3:]:
        load.wait()
    step = step_in[0, 0]
    for q in range(EY):
        density_pad[ROW * q : ROW * q + EZ, 0:125] = density_in[EZ * q : EZ * q + EZ, :]
    energy_pad[0:27, 0:ELEMS] = energy_in[...]
    energy_pad[27:28, 0:ELEMS] = live_in[...].astype(jnp.float32)

    def exact(value, table):
        rows = value.shape[0]
        out = jnp.dot(split_three(value), table, preferred_element_type=jnp.float32)
        return out[0:rows] + out[rows : 2 * rows] + out[2 * rows :]

    by_lane = exact(energy_pad[...], widen[:, 0:128])
    live = by_lane[27:28, :]
    live_own[...] = jnp.broadcast_to(live, (8, 128))
    live_copies = []
    for number, (dx, dz) in enumerate(((-1, 0), (0, -1), (-1, -1))):
        live_copy = pltpu.make_async_remote_copy(
            src_ref=live_own,
            dst_ref=live_got.at[number],
            send_sem=live_send.at[number],
            recv_sem=live_recv.at[number],
            device_id=(dom + dx, sub + dz),
            device_id_type=MESH,
        )
        live_copies.append((live_copy, (dx, dz)))

        @pl.when(inside(dx, dz))
        def _():
            live_copy.start()

    live = live + turn(live, 0, 64)
    by_point = jnp.transpose(density_pad[...])
    mass_density = by_point[0:64] + turn(by_point[64:128], 0, 64)
    weight = quad_weight[...]
    live_weight = weight * live
    mass_weight = whole_weight[...] * (live_own[0:1, :] * by_point)
    at_points = dot(energy_forth, jnp.concatenate([by_lane, turn(by_lane, 0, 64)], axis=0))

    def paired(v):
        return jnp.concatenate(
            [
                jnp.concatenate([v[64 * k : 64 * k + 64], turn(v[64 * k : 64 * k + 64], 0, 64)], 0)
                for k in range(v.shape[0] // 64)
            ],
            axis=1,
        )

    def folded(product):
        half = product.shape[0] // 2
        out = []
        for k in range(product.shape[1] // 128):
            part = product[:, 128 * k : 128 * k + 128]
            out.append(part[:half] + turn(part[half:], 0, 64))
        return out

    def gradient(v):
        shaped = dot(grad_forth, paired(v))
        return [
            [shaped[64 * m : 64 * m + 64, 128 * c : 128 * c + 128] for m in range(3)]
            for c in range(3)
        ]

    def jacobian_of(v):
        jacobian = gradient(v)
        for c in range(3):
            jacobian[c][c] = jacobian[c][c] + 1.0
        return jacobian

    def project(fields):
        right = jnp.concatenate(
            [jnp.concatenate([fields[c][m] for c in range(3)], axis=1) for m in range(3)], axis=0
        )
        return share(jnp.concatenate(folded(dot(grad_back, right)), axis=0))

    def share(v):
        v = v * jnp.where(triple(valid), 1.0, 0.0)
        first_rows = row[:8] < 4
        here = valid[:8]
        up = jnp.logical_not(first_rows) & (q_of[:8] < EY - 1) & here
        down = first_rows & (q_of[:8] > 0) & here
        rows = []
        for at in range(0, 192, 16):
            near_rows, far_rows = v[at : at + 8], v[at + 8 : at + 16]
            swapped = turn(jnp.where(first_rows, near_rows, far_rows), 4, 0)
            rows.append(near_rows + jnp.where(down, turn(swapped, 0, ROW), 0.0))
            rows.append(far_rows + jnp.where(up, turn(swapped, 0, -ROW), 0.0))
        v = jnp.concatenate(rows, axis=0)
        v = v + jnp.where(z_up, turn(v, 3, -1), 0.0) + jnp.where(z_down, turn(v, -3, 1), 0.0)
        return v

    def interpolate(v):
        return dot(basis_forth, jnp.concatenate([v[0:64], v[64:128], v[128:192]], axis=1))

    def volume_of(jacobian, cofactor):
        return (
            jacobian[0][0] * cofactor[0][0]
            + jacobian[0][1] * cofactor[0][1]
            + jacobian[0][2] * cofactor[0][2]
        )

    def begin(rnd, v, ups=True, downs=True):
        source = local.at[rnd - 1]
        source[...] = v
        state[...] = v
        return exchange_start(rnd, source, 3, lambda slot: x_got.at[rnd - 1, slot], ups, downs)

    def finish(rnd, started, ups=True, downs=True):
        exchange_wait(started)
        source = local.at[rnd - 1]
        exchange_add(
            rnd, source, state, 3, lambda slot: x_got.at[rnd - 1, slot], ups, downs
        )
        return state[...] * off_wall

    out_nodes[...] = first[0:384, :]
    exchange_wait(started)
    exchange_add(0, out_nodes, out_nodes, 6, lambda slot: x_first, True, False)
    displacement = out_nodes[0:192, :]
    velocity = out_nodes[192:384, :]

    jacobian = jacobian_of(displacement)
    velocity_grad = gradient(velocity)
    cofactor = cofactors(jacobian)
    volume = volume_of(jacobian, cofactor)
    inverse = 1.0 / volume
    density = mass_density * inverse
    pressure = (adiabatic - 1.0) * density * at_points
    spatial = [
        [
            (
                velocity_grad[c][0] * cofactor[m][0]
                + velocity_grad[c][1] * cofactor[m][1]
                + velocity_grad[c][2] * cofactor[m][2]
            )
            * inverse
            for m in range(3)
        ]
        for c in range(3)
    ]
    viscous = viscosity * density
    stress = [[None] * 3 for _ in range(3)]
    for c in range(3):
        for m in range(c, 3):
            value = viscous * (spatial[c][m] + spatial[m][c])
            stress[c][m] = stress[m][c] = value - pressure if c == m else value
    flux = [
        [
            -live_weight
            * (
                stress[c][0] * cofactor[0][m]
                + stress[c][1] * cofactor[1][m]
                + stress[c][2] * cofactor[2][m]
            )
            for m in range(3)
        ]
        for c in range(3)
    ]
    started = begin(1, project(flux))
    power = stress[0][0] * spatial[0][0]
    for c in range(3):
        for m in range(3):
            if c + m > 0:
                power = power + stress[c][m] * spatial[c][m]
    power = live_weight * volume * power
    sums = folded(
        dot(energy_back, jnp.concatenate([power, weight * mass_density], axis=1))
    )
    rates = jnp.where(valid[:32], sums[0] / jnp.where(valid[:32], sums[1], 1.0), 0.0)
    rate_out[...] = exact(rates, widen[:, 128:256])[0:27, 0:ELEMS]
    force = finish(1, started)

    wide_mass = jnp.concatenate([mass_weight] * 3, axis=1)
    values = interpolate(force)
    weighted = wide_mass * values
    product = dot(basis_back, weighted)
    image = share(
        jnp.concatenate([product[:, 128 * k : 128 * k + 128] for k in range(3)], axis=0)
    )
    started = begin(2, image)

    def total(x):
        return jnp.sum(jnp.sum(x, axis=0, keepdims=True), axis=1, keepdims=True)

    norm_part = total(force * force * owned)
    product_part = total(weighted * values)
    image = finish(2, started)
    image_norm_part = total(image * image * owned)
    values = interpolate(image)
    image_product_part = total(wide_mass * values * values)

    lane1 = lane[0:1]
    packed = jnp.where(
        lane1 == 0,
        norm_part,
        jnp.where(
            lane1 == 1,
            product_part,
            jnp.where(lane1 == 2, image_norm_part, image_product_part),
        ),
    )

    late = []

    def all_sum(value, slots, targets, sends, recvs, cover=None):
        slots[0] = value

        def copy_of(source, target, device):
            return pltpu.make_async_remote_copy(
                src_ref=source,
                dst_ref=target,
                send_sem=sends.at[0],
                recv_sem=recvs.at[0],
                device_id=device,
                device_id_type=MESH,
            )

        for number, device in targets:
            copy_of(slots.at[0], slots.at[number], device).start()

        out = cover() if cover else None

        others = slots.at[pl.ds(1, len(targets))]
        whole_sum = copy_of(others, others, targets[0][1])
        whole_sum.wait_recv()
        late.append(whole_sum)
        return jnp.sum(slots[...], axis=0), out

    doms = [lax.rem(dom + i, n_dom) for i in range(n_dom)]
    subs = [lax.rem(sub + i, n_sub) for i in range(n_sub)]

    def ahead():
        return [gradient(v) for v in (displacement + step * velocity, force, image)]

    if one_phase:
        targets = [
            (j * n_dom + i, (doms[i], subs[j]))
            for j in [*range(1, n_sub), 0]
            for i in range(n_dom)
            if i + j > 0
        ]
        packed, slopes = all_sum(packed, sum_dom, targets, dom_send, dom_recv, ahead)
    else:
        targets = [(i, (doms[i], sub)) for i in range(1, n_dom)]
        packed, slopes = all_sum(packed, sum_dom, targets, dom_send, dom_recv, ahead)
        targets = [(j, (dom, subs[j])) for j in range(1, n_sub)]
        packed, _ = all_sum(packed, sum_sub, targets, sub_send, sub_recv)
    rr, rw, ww, wmw = (
        jnp.sum(jnp.where(lane1 == k, packed, 0.0), axis=1, keepdims=True) for k in range(4)
    )
    first_length = rr / rw
    next_norm = first_length * (first_length * ww) - rr
    conjugacy = next_norm / rr
    residual_image = rw - first_length * ww
    residual_product = rw - 2.0 * first_length * ww + first_length * first_length * wmw
    bend = residual_product + 2.0 * conjugacy * residual_image + conjugacy * conjugacy * rw
    second_length = next_norm / bend
    on_force = first_length + second_length * (1.0 + conjugacy)
    on_image = second_length * first_length
    new_velocity = velocity + step * (on_force * force - on_image * image)
    moved = displacement + step * new_velocity

    def fluxes(jacobian, weights):
        cofactor = cofactors(jacobian)
        volume = volume_of(jacobian, cofactor)
        norm_sq = None
        for c in range(3):
            for m in range(3):
                square = jacobian[c][m] * jacobian[c][m]
                norm_sq = square if norm_sq is None else norm_sq + square
        scale = weights * jnp.exp(jnp.log(volume) * (-2.0 / 3.0))
        along = scale * (2.0 / 3.0)
        across = scale * (2.0 / 9.0) * (norm_sq / volume)
        return [
            [along * jacobian[c][m] - across * cofactor[c][m] for m in range(3)]
            for c in range(3)
        ]

    def back_to_lattice(nodes):
        for x in range(3):
            for pair in range(8):
                at = 16 * (x + 1) + 2 * pair
                even = nodes[pl.ds(at, 3, stride=64), :]
                odd = nodes[pl.ds(at + 1, 3, stride=64), :]
                out_wide[8 * x : 8 * x + 3, 128 * pair : 128 * pair + 128] = even + turn(odd, 0, 64)
        back = lax.dot_general(
            split_three(out_wide[...]), pick[...], (((1,), (1,)), ((), ())), preferred_element_type=jnp.float32
        )
        return back[0:24] + back[24:48] + back[48:72]

    by_force, by_image = step * step * on_force, step * step * on_image
    jacobian = [
        [
            slopes[0][c][m] + by_force * slopes[1][c][m] - by_image * slopes[2][c][m]
            for m in range(3)
        ]
        for c in range(3)
    ]
    for c in range(3):
        jacobian[c][c] = jacobian[c][c] + 1.0
    shift = -mesh_step * project(fluxes(jacobian, live_weight))

    comps = range(3)
    a_first, c_first = a_of == 0, c_of == 0
    part = [shift[64 * k : 64 * k + 64] for k in comps]
    whole = [moved[64 * k : 64 * k + 64] + part[k] for k in comps]
    ours[...] = shift
    slab = jnp.concatenate([jnp.where(a_first, part[k], whole[k]) for k in comps], axis=0)
    near[...] = slab[0:96] + turn(slab[96:192], 0, 64)
    r64 = jnp.where(low_half, r_of, ROW)

    def lay(fields, place):
        out = None
        for k in comps:
            at = r64[: fields[k].shape[0]]
            piece = jnp.where(at == k, turn(fields[k], 0, k - place), 0.0)
            out = piece if out is None else out + piece
        return out + turn(out, 0, 64)

    layer = [jnp.where(c_first, part[k], whole[k]) for k in comps]
    right_half = jnp.logical_not(low_half)
    r_here = r_of[:16]

    def lay_group(fields, a):
        out = None
        half = low_half[:16] if a < 2 else right_half[:16]
        for k in comps:
            spot = 3 * (a % 2) + k
            piece = jnp.where(
                half & (r_here == spot), turn(fields[k], 0, 64 * (a // 2) + spot), 0.0
            )
            out = piece if out is None else out + piece
        return out

    groups = [lay_group([f[16 * a : 16 * a + 16] for f in layer], a) for a in range(4)]
    upper_groups = groups[1] + groups[2] + groups[3]
    face_part = lay_group([part[k][0:16] for k in comps], 0)
    z_low[0] = turn(face_part + upper_groups, 0, 64)
    z_low[1] = groups[0] + upper_groups
    z_low[2] = lay([part[k][48:64] for k in comps], 0)
    z_high[...] = lay([ours[pl.ds(64 * k + 3, 16, stride=4), :] for k in comps], EZ - 1)
    x_face[0, 0:16] = part[1][0:16] + turn(part[0][0:16], 0, 64)
    x_face[0, 16:24] = part[2][8:16] + turn(part[2][0:8], 0, 64)
    x_face[1, 0:16] = part[0][48:64] + turn(part[1][48:64], 0, 64)
    x_face[1, 16:24] = part[2][48:56] + turn(part[2][56:64], 0, 64)

    routes = {
        (-1, 0): (near, slab_got),
        (-2, 0): (x_face.at[0], x_face_got.at[0]),
        (1, 0): (x_face.at[1], x_face_got.at[1]),
        (0, -1): (z_low.at[1], layer_got.at[0]),
        (-1, -1): (z_low.at[0], layer_got.at[1]),
        (-2, -1): (z_low.at[0], edge_got.at[0]),
        (1, -1): (z_low.at[2], edge_got.at[1]),
        (0, 1): (z_high, floor_got.at[0]),
        (-1, 1): (z_high, floor_got.at[1]),
        (-2, 1): (z_high.at[pl.ds(0, 8)], floor_got.at[2, pl.ds(0, 8)]),
        (1, 1): (z_high.at[pl.ds(8, 8)], floor_got.at[3, pl.ds(8, 8)]),
    }
    started = []
    for number, (dx, dz) in enumerate(WIDE_STEPS):
        source, target = routes[dx, dz]
        wide_copy = pltpu.make_async_remote_copy(
            src_ref=source,
            dst_ref=target,
            send_sem=wide_send.at[number],
            recv_sem=wide_recv.at[number],
            device_id=(dom + dx, sub + dz),
            device_id_type=MESH,
        )

        @pl.when(inside(dx, dz))
        def _():
            wide_copy.start()

        started.append((wide_copy, (dx, dz)))
    exchange_wait(live_copies)
    out_nodes[0:192, :] = new_velocity * owned
    new_back = back_to_lattice(out_nodes)
    one_low, one_r = low_half[0:1], r_of[0:1]
    live_up = turn(live_got[0, 0:1, :], 0, 64)
    live_layer = live_got[1, 0:1, :] + turn(live_got[2, 0:1, :], 0, 64)
    live_wide = live_own[0:1, :] + live_up + jnp.where(one_r == EZ, turn(live_layer, 0, EZ), 0.0)
    wide_weight = whole_weight[...] * live_wide
    wide_wall = jnp.where(
        jnp.logical_or(right_half, jnp.logical_or(a_of > 0, dom > 0))
        & jnp.logical_or(jnp.logical_or(c_of > 0, r_of > 0), sub > 0),
        1.0,
        0.0,
    )
    low16, row16r = low_half[:16], r_of[:16]

    for whole_sum in late:
        whole_sum.wait_send()
    for copy, (dx, dz) in waits + started:

        @pl.when(inside(dx, dz))
        def _():
            copy.wait_send()

    exchange_wait(started)
    upper = slab_got[...]
    upper = jnp.concatenate([turn(upper, 0, 64), upper], axis=0)
    first_got, second_got = layer_got[0], layer_got[1]
    mixed = (
        jnp.where(low16, first_got, second_got),
        jnp.where(low16, second_got, first_got),
    )
    right16 = right_half[:16]
    edge_up = jnp.where(right16, edge_got[0], 0.0)
    edge_down = jnp.where(low16, edge_got[1], 0.0)
    floor = jnp.where(low16, floor_got[0], floor_got[1])
    floor = floor + jnp.where(right16 & (row16 >= 12), turn(floor_got[2], 12, 0), 0.0)
    floor = floor + jnp.where(low16 & (row16 < 4), turn(floor_got[3], 4, 0), 0.0)
    face_low = [
        x_face_got[1, 0:16],
        turn(x_face_got[1, 0:16], 0, 64),
        jnp.concatenate([x_face_got[1, 16:24], turn(x_face_got[1, 16:24], 0, 64)], axis=0),
    ]
    face_high = [
        x_face_got[0, 0:16],
        turn(x_face_got[0, 0:16], 0, 64),
        jnp.concatenate([x_face_got[0, 16:24], turn(x_face_got[0, 16:24], 0, 64)], axis=0),
    ]
    for k in comps:
        at = 64 * k
        rows = []
        for a in range(4):
            u = jnp.where(low16, whole[k][16 * a : 16 * a + 16], upper[at + 16 * a : at + 16 * a + 16])
            spot = 3 * (a % 2) + k
            piece = turn(mixed[a // 2], 0, EZ - spot - 64 * (a // 2))
            if a == 0:
                piece = piece + jnp.where(low16, turn(edge_down, 0, EZ - k), 0.0)
                u = u + jnp.where(low16, face_low[k], 0.0)
            if a == 3:
                piece = piece + jnp.where(low16, 0.0, turn(edge_up, 0, EZ - k))
                u = u + jnp.where(low16, 0.0, face_high[k])
            rows.append(u + jnp.where(row16r == EZ, piece, 0.0))
        wide_nodes[at : at + 64, :] = jnp.concatenate(rows, axis=0)
        below = pl.ds(at, 16, stride=4)
        above = pl.ds(at + 3, 16, stride=4)
        wide_nodes[below, :] += jnp.where(row16r == 0, turn(floor, 0, -k), 0.0)
        near_face = wide_nodes[at : at + 16, :]
        far_face = wide_nodes[at + 48 : at + 64, :]
        wide_nodes[at : at + 16, :] = near_face + jnp.where(low16, 0.0, turn(far_face, 0, 64))
        wide_nodes[at + 48 : at + 64, :] = far_face + jnp.where(low16, turn(near_face, 0, 64), 0.0)
        tops = wide_nodes[above, :]
        bottoms = wide_nodes[below, :]
        wide_nodes[above, :] = tops + jnp.where(row16r == EZ - 1, turn(bottoms, 0, -1), 0.0)
        wide_nodes[below, :] = bottoms + jnp.where(row16r == EZ, turn(tops, 0, 1), 0.0)
    relaxed = [wide_nodes[64 * k : 64 * k + 64, :] * wide_wall for k in comps]
    shaped = dot(whole_forth, jnp.concatenate(relaxed, axis=1))
    jacobian = [
        [shaped[128 * m : 128 * m + 128, 128 * c : 128 * c + 128] for m in comps] for c in comps
    ]
    for c in comps:
        jacobian[c][c] = jacobian[c][c] + 1.0
    fields = fluxes(jacobian, wide_weight)
    right = jnp.concatenate(
        [jnp.concatenate([fields[c][m] for c in comps], axis=1) for m in comps], axis=0
    )
    product = dot(whole_back, right)
    last = []
    for k in comps:
        v = product[:, 128 * k : 128 * k + 128]
        v = v + jnp.where((b_of == 0) & (q_of > 0), turn(v, -12, ROW), 0.0)
        v = v + jnp.where((c_of == 3) & (r_of < EZ), turn(v, 3, -1), 0.0)
        v = jnp.concatenate([v[0:48], v[48:64] + turn(v[0:16], 0, 64)], axis=0)
        last.append(moved[64 * k : 64 * k + 64] - relaxed[k] + mesh_step * v)
    last = jnp.concatenate(last, axis=0)
    mesh_velocity = new_velocity - last / step

    out_nodes[192:384, :] = mesh_velocity * owned
    mesh_back = back_to_lattice(out_nodes.at[pl.ds(192, 192)])
    for x in range(3):
        new_vel_out[:, plane * x : plane * (x + 1)] = new_back[8 * x : 8 * x + 3]
        mesh_vel_out[:, plane * x : plane * (x + 1)] = mesh_back[8 * x : 8 * x + 3]


def hand_on(*refs):
    copies = [
        pltpu.make_async_copy(refs[k], refs[3 + k], refs[6].at[k]) for k in range(3)
    ]
    for copy in copies:
        copy.start()
    for copy in copies:
        copy.wait()


def body(n_dom, n_sub, displacement, velocity, energy, mass_density, live_mask, time_step):
    made_tables = tables()
    vmem = pl.BlockSpec(memory_space=pltpu.VMEM)
    anywhere = pl.BlockSpec(memory_space=pl.ANY)
    f32 = jnp.float32
    nodes = displacement.shape[1]
    wide_sum = n_dom * n_sub if n_dom * n_sub <= 64 else n_dom
    made = pl.pallas_call(
        functools.partial(kernel, n_dom, n_sub),
        out_shape=(
            pltpu.VMEM(displacement.shape, f32),
            pltpu.VMEM(energy.shape, f32),
            pltpu.VMEM(displacement.shape, f32),
        ),
        in_specs=[anywhere] * (6 + len(made_tables)),
        out_specs=(vmem, vmem, vmem),
        scratch_shapes=[
            pltpu.VMEM((8, nodes), f32),
            pltpu.VMEM((24, 1024), f32),
            pltpu.VMEM((512, 128), f32),
            pltpu.VMEM((2, 192, 128), f32),
            pltpu.VMEM((192, 128), f32),
            pltpu.VMEM((384, 128), f32),
            pltpu.VMEM((24, 1024), f32),
            pltpu.VMEM((128, 128), f32),
            pltpu.VMEM((32, 128), f32),
            pltpu.VMEM((8, 128), f32),
            pltpu.VMEM((3, 8, 128), f32),
            pltpu.VMEM((3, 2, 16, 128), f32),
            pltpu.VMEM((6, 16, 128), f32),
            pltpu.VMEM((2, 2, 3, 16, 128), f32),
            pltpu.VMEM((3, 2, 16, 128), f32),
            pltpu.VMEM((3, 4, 8, 128), f32),
            pltpu.VMEM((wide_sum, 1, 128), f32),
            pltpu.VMEM((n_sub, 1, 128), f32),
            pltpu.SemaphoreType.DMA((3, 8)),
            pltpu.SemaphoreType.DMA((3, 8)),
            pltpu.SemaphoreType.DMA((wide_sum,)),
            pltpu.SemaphoreType.DMA((wide_sum,)),
            pltpu.SemaphoreType.DMA((n_sub,)),
            pltpu.SemaphoreType.DMA((n_sub,)),
            pltpu.VMEM(displacement.shape, f32),
            pltpu.VMEM(velocity.shape, f32),
            pltpu.VMEM(energy.shape, f32),
            pltpu.VMEM(mass_density.shape[::-1], f32),
            pltpu.VMEM((1, live_mask.shape[0]), jnp.int32),
            pltpu.SMEM((1, 1), f32),
            *[pltpu.VMEM(t.shape, t.dtype) for t in made_tables],
            pltpu.SemaphoreType.DMA((6 + len(made_tables),)),
            pltpu.VMEM((192, 128), f32),
            pltpu.VMEM((96, 128), f32),
            pltpu.VMEM((3, 16, 128), f32),
            pltpu.VMEM((16, 128), f32),
            pltpu.VMEM((2, 24, 128), f32),
            pltpu.VMEM((96, 128), f32),
            pltpu.VMEM((2, 24, 128), f32),
            pltpu.VMEM((2, 16, 128), f32),
            pltpu.VMEM((2, 16, 128), f32),
            pltpu.VMEM((4, 16, 128), f32),
            pltpu.VMEM((192, 128), f32),
            pltpu.SemaphoreType.DMA((len(WIDE_STEPS),)),
            pltpu.SemaphoreType.DMA((len(WIDE_STEPS),)),
            pltpu.SemaphoreType.DMA((3,)),
            pltpu.SemaphoreType.DMA((3,)),
        ],
        compiler_params=pltpu.CompilerParams(collective_id=0, has_side_effects=True),
    )(
        displacement,
        velocity,
        energy,
        mass_density.T,
        live_mask.reshape(1, -1),
        time_step.reshape(1, 1),
        *[jnp.asarray(t) for t in made_tables],
    )
    return pl.pallas_call(
        hand_on,
        out_shape=[jax.ShapeDtypeStruct(m.shape, f32) for m in made],
        in_specs=[vmem] * 3,
        out_specs=[anywhere] * 3,
        scratch_shapes=[pltpu.SemaphoreType.DMA((3,))],
    )(*[pltpu.with_memory_space_constraint(m, pltpu.VMEM) for m in made])


def solution(mesh):
    split = ("dom", "sub")
    return jax.shard_map(
        functools.partial(body, mesh.shape["dom"], mesh.shape["sub"]),
        mesh=mesh,
        in_specs=(
            P(None, split),
            P(None, split),
            P(None, split),
            P(None, split),
            P(split),
            P(),
        ),
        out_specs=(P(None, split), P(None, split), P(None, split)),
        check_vma=False,
    )
```
